32 devices in a mesh: dp: 8 (over y, x, core), tensor: 4 (over z).
Axes of the slice: x: 2, y: 2, z: 4, core: 2. Of those that a mesh axis runs over, the one named last changes fastest.
Arguments:
- tokens: bfloat16 [16384, 1024], P(('dp', 'tensor')), may hold values from -6 to 6
- weight_query: bfloat16 [1024, 1024], P('dp', 'tensor'), may hold values from -0.375 to 0.375
- weight_key: bfloat16 [1024, 1024], P('dp', 'tensor'), may hold values from -0.1875 to 0.1875
- weight_value: bfloat16 [1024, 1024], P('dp', 'tensor'), may hold values from -0.1875 to 0.1875
- weight_out: bfloat16 [1024, 1024], P('tensor', 'dp'), may hold values from -0.5 to 0.5
- bias_query: bfloat16 [1024], P(('tensor', 'dp')), may hold values from -1.796875 to 1.796875
- bias_value: bfloat16 [1024], P(('tensor', 'dp')), may hold values from -0.59765625 to 0.59765625
- bias_out: bfloat16 [1024], P('dp'), may hold values from -1.796875 to 1.796875
- first_scale: bfloat16 [1024], P('dp'), may hold values from 0.5 to 1.5
- first_shift: bfloat16 [1024], P('dp'), may hold values from -1.796875 to 1.796875
- weight_hidden: bfloat16 [1024, 4096], P('dp', 'tensor'), may hold values from -0.1875 to 0.1875
- bias_hidden: bfloat16 [4096], P(('tensor', 'dp')), may hold values from -1.796875 to 1.796875
- weight_down: bfloat16 [4096, 1024], P('tensor', 'dp'), may hold values from -0.125 to 0.125
- bias_down: bfloat16 [1024], P('dp'), may hold values from -1.796875 to 1.796875
- second_scale: bfloat16 [1024], P('dp'), may hold values from 0.5 to 1.5
- second_shift: bfloat16 [1024], P('dp'), may hold values from -1.796875 to 1.796875
- cotangent: bfloat16 [16384, 1024], P(('dp', 'tensor')), may hold values from -6 to 6
Outputs:
- output: bfloat16 [16384, 1024], P(('dp', 'tensor'))
- grad_tokens: bfloat16 [16384, 1024], P(('dp', 'tensor'))
- grad_weight_query: float32 [1024, 1024], P('dp', 'tensor')
- grad_weight_key: float32 [1024, 1024], P('dp', 'tensor')
- grad_weight_value: float32 [1024, 1024], P('dp', 'tensor')
- grad_weight_out: float32 [1024, 1024], P('tensor', 'dp')
- grad_bias_query: float32 [1024], P(('tensor', 'dp'))
- grad_bias_value: float32 [1024], P(('tensor', 'dp'))
- grad_bias_out: float32 [1024], P('dp')
- grad_first_scale: float32 [1024], P('dp')
- grad_first_shift: float32 [1024], P('dp')
- grad_weight_hidden: float32 [1024, 4096], P('dp', 'tensor')
- grad_bias_hidden: float32 [4096], P(('tensor', 'dp'))
- grad_weight_down: float32 [4096, 1024], P('tensor', 'dp')
- grad_bias_down: float32 [1024], P('dp')
- grad_second_scale: float32 [1024], P('dp')
- grad_second_shift: float32 [1024], P('dp')
The draws below stay inside these ranges and needn't reach their ends.
All inputs are finite; a program needn't handle non-finite values.
Results may differ from the reference program's by a relative error of at most 0.02.
Values may be sent and summed in bfloat16 or wider, within the bound.
A program may use at most 128 MiB of HBM per device.

```python
import jax
import jax.numpy as jnp
from jax import lax

D = 1024
HEADS = 16
HD = 64
FF = 4096
LEN = 2048
QB = 512
TOKENS = 16384


def strengthened(array, key, source, target, blocks, factor):
    def block_of(axis_at):
        return (jnp.arange(array.shape[axis_at]) // (array.shape[axis_at] // blocks)).reshape((-1,) + (1,) * (array.ndim - 1 - axis_at))

    one_side = jax.random.permutation(key, blocks)[block_of(target)]
    far = (block_of(target) + blocks // 2) % blocks
    return jnp.where((block_of(source) == one_side) | (block_of(source) == far), factor * array, array)


def block_scale(rng, dims, split, low, high):
    loudness = 1.0
    for position, parts in split:
        steps = jax.random.uniform(jax.random.fold_in(jax.random.fold_in(rng, 6), position), (parts,), jnp.float32, low / len(split), high / len(split))
        loudness = loudness * jnp.repeat(jnp.exp(steps), dims[position] // parts).reshape((-1,) + (1,) * (len(dims) - 1 - position))
    return loudness


def normal_values(rng, dims, scale, bound, pieces=(), kind=jnp.bfloat16):
    gain = block_scale(rng, dims, pieces, -0.22, 0.18) if pieces else 1.0
    entries = jax.random.normal(rng, dims, jnp.float32) * scale * gain
    return jnp.minimum(jnp.maximum(entries, -bound), bound).astype(kind)


def heavy_noise(own_key, dims, deviation, limit, split, heavy, held_as=jnp.bfloat16):
    values = deviation * jax.random.normal(own_key, dims, jnp.float32)
    if split:
        values = values * block_scale(own_key, dims, split, -0.22, 0.18)
    return jnp.clip(strengthened(values, jax.random.fold_in(own_key, 3), *heavy), -limit, limit).astype(held_as)


def setup_inputs(seed: int = 0) -> dict:
    arg_keys = jax.random.split(jax.random.key(seed), 18)
    tokens = normal_values(arg_keys[0], (TOKENS, D), 1.0, 6.0, ((0, 32),))
    weight_query = normal_values(arg_keys[1], (D, D), (D // 4) ** -0.5, 0.375, ((0, 8), (1, 4)))
    weight_key = normal_values(arg_keys[2], (D, D), D ** -0.5, 0.1875, ((0, 8), (1, 4)))
    weight_value = normal_values(arg_keys[3], (D, D), D ** -0.5, 0.1875, ((0, 8), (1, 4)))
    weight_out = normal_values(arg_keys[4], (D, D), (D // 8) ** -0.5, 0.5, ((0, 4), (1, 8)))
    bias_query = normal_values(arg_keys[5], (D,), 0.3, 1.796875, ((0, 32),))
    bias_value = normal_values(arg_keys[6], (D,), 0.1, 0.59765625, ((0, 32),))
    bias_out = normal_values(arg_keys[7], (D,), 0.3, 1.796875, ((0, 8),))
    first_scale = jnp.clip(1.0 + 0.1 * jax.random.normal(arg_keys[8], (D,), jnp.float32), 0.5, 1.5).astype(jnp.bfloat16)
    first_shift = normal_values(arg_keys[9], (D,), 0.3, 1.796875, ((0, 8),))
    weight_hidden = normal_values(arg_keys[10], (D, FF), D ** -0.5, 0.1875, ((0, 8), (1, 4)))
    bias_hidden = normal_values(arg_keys[11], (FF,), 0.3, 1.796875, ((0, 32),))
    weight_down = normal_values(arg_keys[12], (FF, D), (FF // 2) ** -0.5, 0.125, ((0, 4), (1, 8)))
    bias_down = normal_values(arg_keys[13], (D,), 0.3, 1.796875, ((0, 8),))
    second_scale = jnp.clip(1.0 + 0.1 * jax.random.normal(arg_keys[14], (D,), jnp.float32), 0.5, 1.5).astype(jnp.bfloat16)
    second_shift = normal_values(arg_keys[15], (D,), 0.3, 1.796875, ((0, 8),))
    cotangent = heavy_noise(arg_keys[16], (TOKENS, D), 1.0, 6.0, ((0, 32),), (0, 1, 32, 2.75))
    return {"tokens": tokens, "weight_query": weight_query, "weight_key": weight_key, "weight_value": weight_value, "weight_out": weight_out, "bias_query": bias_query, "bias_value": bias_value, "bias_out": bias_out, "first_scale": first_scale, "first_shift": first_shift, "weight_hidden": weight_hidden, "bias_hidden": bias_hidden, "weight_down": weight_down, "bias_down": bias_down, "second_scale": second_scale, "second_shift": second_shift, "cotangent": cotangent}


@jax.custom_vjp
def low(v):
    return lax.optimization_barrier(v.astype(jnp.bfloat16)).astype(jnp.float32)

@jax.custom_vjp
def low_back(v):
    return v

def low_keep(v):
    return (low(v), None)

def low_pass(kept, grad):
    return (grad,)

def back_keep(v):
    return (v, None)

def back_low(kept, grad):
    return (low(grad),)
low.defvjp(low_keep, low_pass)
low_back.defvjp(back_keep, back_low)
PRECISE = lax.Precision.HIGHEST

def rounded(values):
    return low(low_back(values))

def layer_norm(values, scale_vec, shift_vec):
    average = lax.optimization_barrier(jnp.mean(values, axis=-1, keepdims=True))
    centered = values - average
    spread = lax.optimization_barrier(jnp.mean(centered * centered, axis=-1, keepdims=True))
    return centered * lax.rsqrt(spread + 1e-05) * scale_vec + shift_vec

def attend_block(query_block, key_seq, value_seq):
    scores = low_back(jnp.einsum('qhd,khd->hqk', query_block, key_seq, precision=PRECISE)) * 0.125
    highest = lax.optimization_barrier(jnp.max(scores, axis=-1, keepdims=True))
    expons = jnp.exp(scores - highest)
    probs = expons / lax.optimization_barrier(jnp.sum(expons, axis=-1, keepdims=True))
    return jnp.einsum('hqk,khd->qhd', low(probs), value_seq, precision=PRECISE)

def attend_sequence(packed):
    query_seq, key_seq, value_seq = packed
    blocks = query_seq.reshape(LEN // QB, QB, HEADS, HD)

    def block_fn(query_block):
        return attend_block(query_block, key_seq, value_seq)
    outputs = lax.map(jax.checkpoint(block_fn), blocks)
    return outputs.reshape(LEN, HEADS, HD)

def forward(source, weight_query, weight_key, weight_value, weight_out, bias_query, bias_value, bias_out, first_scale, first_shift, weight_hidden, bias_hidden, weight_down, bias_down, second_scale, second_shift):
    seq_count = source.shape[0] // LEN
    queries = rounded(jnp.dot(source, weight_query, precision=PRECISE) + bias_query)
    keys = rounded(jnp.dot(source, weight_key, precision=PRECISE))
    values = rounded(jnp.dot(source, weight_value, precision=PRECISE) + bias_value)
    shaped = (queries.reshape(seq_count, LEN, HEADS, HD), keys.reshape(seq_count, LEN, HEADS, HD), values.reshape(seq_count, LEN, HEADS, HD))
    attended = lax.map(jax.checkpoint(attend_sequence), shaped)
    attended = rounded(attended.reshape(seq_count * LEN, D))
    branch = low_back(jnp.dot(attended, weight_out, precision=PRECISE))
    first = layer_norm(source + branch + bias_out, first_scale, first_shift)
    pre = low_back(jnp.dot(low(first), weight_hidden, precision=PRECISE) + bias_hidden)
    hidden = low(jax.nn.gelu(pre, approximate=False))
    down = low_back(jnp.dot(hidden, weight_down, precision=PRECISE))
    return layer_norm(first + down + bias_down, second_scale, second_shift)

def reference(tokens, weight_query, weight_key, weight_value, weight_out, bias_query, bias_value, bias_out, first_scale, first_shift, weight_hidden, bias_hidden, weight_down, bias_down, second_scale, second_shift, cotangent):
    inputs = tuple((argument.astype(jnp.float32) for argument in (tokens, weight_query, weight_key, weight_value, weight_out, bias_query, bias_value, bias_out, first_scale, first_shift, weight_hidden, bias_hidden, weight_down, bias_down, second_scale, second_shift)))
    result, pullback = jax.vjp(forward, *inputs)
    grads = pullback(cotangent.astype(jnp.float32))
    return (result.astype(jnp.bfloat16), grads[0].astype(jnp.bfloat16), grads[1], grads[2], grads[3], grads[4], grads[5], grads[6], grads[7], grads[8], grads[9], grads[10], grads[11], grads[12], grads[13], grads[14], grads[15])
```

```python
import jax
import jax.numpy as jnp
from jax import lax
from jax.experimental import pallas as pl
from jax.experimental.pallas import tpu as pltpu
from jax.sharding import PartitionSpec as P

HD = 64
LEN = 2048
QB = 256
PAIR = 2 * HD
PAD = 16
F32 = jnp.float32
BF = jnp.bfloat16
BOTH = ("dp", "tensor")


def contract(left, right, left_dim, right_dim):
    return lax.dot_general(
        left, right, (((left_dim,), (right_dim,)), ((), ())), preferred_element_type=F32
    )


def one_head(pair, head):
    lane = lax.broadcasted_iota(jnp.int32, pair.shape, 1)
    keep = lane < HD if head == 0 else lane >= HD
    return jnp.where(keep, pair, jnp.zeros_like(pair))


def attend_forward_kernel(q_ref, k_ref, v_ref, out_ref, logsum_ref):
    query = q_ref[...] * jnp.asarray(0.125, BF)
    key, value = k_ref[...], v_ref[...]
    total, columns = None, []
    for head in range(2):
        scores = contract(query, one_head(key, head), 1, 1)
        highest = jnp.max(scores, axis=1, keepdims=True)
        expons = jnp.exp(scores - highest)
        mass = jnp.sum(expons, axis=1, keepdims=True)
        part = contract(expons.astype(BF), one_head(value, head), 1, 0) / mass
        total = part if total is None else total + part
        columns.append(jnp.broadcast_to(highest + jnp.log(mass), (query.shape[0], PAIR)))
    out_ref[...] = total.astype(BF)
    logsum_ref[0] = jnp.concatenate([jnp.transpose(column)[:4] for column in columns], axis=0)


def attend_forward(qkv):
    width = qkv.shape[1] // 3
    pairs = width // PAIR
    block = pl.BlockSpec((QB, PAIR), lambda i, j: (j, i))
    key_block = pl.BlockSpec((LEN, PAIR), lambda i, j: (0, i + pairs))
    value_block = pl.BlockSpec((LEN, PAIR), lambda i, j: (0, i + 2 * pairs))
    return pl.pallas_call(
        attend_forward_kernel,
        grid=(width // PAIR, LEN // QB),
        in_specs=[block, key_block, value_block],
        out_specs=[block, pl.BlockSpec((1, 8, QB), lambda i, j: (i, 0, j))],
        out_shape=[
            jax.ShapeDtypeStruct((LEN, width), BF),
            jax.ShapeDtypeStruct((width // PAIR, 8, LEN), F32),
        ],
        cost_estimate=pl.CostEstimate(
            flops=20 * LEN * LEN * width, bytes_accessed=12 * LEN * width, transcendentals=0
        ),
        compiler_params=pltpu.CompilerParams(vmem_limit_bytes=40 << 20),
        name="attend_forward",
    )(qkv, qkv, qkv)


def attend_backward_kernel(
    q_ref, k_ref, v_ref, grad_ref, out_ref, logsum_ref, dq_ref, dk_ref, dv_ref, dk_sum, dv_sum
):
    step = pl.program_id(1)
    query = q_ref[...] * jnp.asarray(0.125, BF)
    key, value, grad = k_ref[...], v_ref[...], grad_ref[...]
    products = jnp.transpose(grad.astype(F32) * out_ref[...].astype(F32))

    @pl.when(step == 0)
    def _():
        dk_sum[...] = jnp.zeros_like(dk_sum)
        dv_sum[...] = jnp.zeros_like(dv_sum)

    grad_query = None
    for head in range(2):
        key_head, value_head = one_head(key, head), one_head(value, head)
        inner = jnp.sum(products[HD * head : HD * head + HD], axis=0, keepdims=True)
        logsum = logsum_ref[0, 4 * head : 4 * head + 1, :]
        probs = jnp.exp(contract(key_head, query, 1, 1) - logsum)
        grad_probs = contract(value_head, grad, 1, 1)
        grad_scores = (probs * (grad_probs - inner)).astype(BF)
        dv_sum[...] += contract(probs.astype(BF), one_head(grad, head), 1, 0)
        dk_sum[...] += contract(grad_scores, one_head(query, head), 1, 0)
        part = contract(grad_scores, key_head, 0, 0)
        grad_query = part if grad_query is None else grad_query + part
    dq_ref[...] = (grad_query * 0.125).astype(BF)

    @pl.when(step == pl.num_programs(1) - 1)
    def _():
        dk_ref[...] = dk_sum[...].astype(BF)
        dv_ref[...] = dv_sum[...].astype(BF)


def attend_backward(qkv, grad, out, logsum):
    width = qkv.shape[1] // 3
    pairs = width // PAIR
    block = pl.BlockSpec((QB, PAIR), lambda i, j: (j, i))
    whole = pl.BlockSpec((LEN, PAIR), lambda i, j: (0, i))
    return pl.pallas_call(
        attend_backward_kernel,
        grid=(width // PAIR, LEN // QB),
        in_specs=[
            block,
            pl.BlockSpec((LEN, PAIR), lambda i, j: (0, i + pairs)),
            pl.BlockSpec((LEN, PAIR), lambda i, j: (0, i + 2 * pairs)),
            block,
            block,
            pl.BlockSpec((1, 8, QB), lambda i, j: (i, 0, j)),
        ],
        out_specs=[block, whole, whole],
        out_shape=[jax.ShapeDtypeStruct((LEN, width), BF)] * 3,
        scratch_shapes=[pltpu.VMEM((LEN, PAIR), F32)] * 2,
        cost_estimate=pl.CostEstimate(
            flops=40 * LEN * LEN * width, bytes_accessed=18 * LEN * width, transcendentals=0
        ),
        compiler_params=pltpu.CompilerParams(vmem_limit_bytes=40 << 20),
        name="attend_backward",
    )(qkv, qkv, qkv, grad, out, logsum)


def row_mean(values):
    return jnp.mean(values, axis=1, keepdims=True)


def column_sum(values):
    return jnp.sum(values, axis=0, keepdims=True)


def middle_kernel(
    sizes,
    att_ref,
    tok_ref,
    cot_ref,
    outw_ref,
    vec_ref,
    hid_ref,
    feed_ref,
    out_ref,
    gsum_ref,
    gatt_ref,
    pack_ref,
    first_s,
    norm_s,
    down_s,
    inv_s,
    low_s,
    low_t,
    gdown_s,
    gdown_t,
    hidden_s,
    slope_s,
    stage_s,
    tail_s,
    sems,
):
    dps, tps, piece, chunks = sizes
    step = pl.program_id(0)
    model = tok_ref.shape[1]
    feed_rows = 2 * piece

    def norm_parts(values):
        centered = values - row_mean(values)
        inverse = lax.rsqrt(row_mean(centered * centered) + 1e-05)
        return centered * inverse, inverse

    def norm_back(grad, scale, normed, inverse):
        scaled = grad * scale
        return inverse * (scaled - row_mean(scaled) - normed * row_mean(scaled * normed))

    def send(slot, block):
        return pltpu.make_async_copy(
            stage_s.at[slot], pack_ref.at[:, block, pl.ds(0, feed_rows)], sems.at[slot]
        )

    @pl.when(step == 0)
    def _():
        branch = None
        for t in range(tps):
            weight = outw_ref[:, t, :piece].reshape(model, -1)
            part = contract(att_ref[t], weight, 1, 1)
            branch = part if branch is None else branch + part
        normed, inverse = norm_parts(tok_ref[...].astype(F32) + branch + vec_ref[0:1])
        first = normed * vec_ref[1:2] + vec_ref[2:3]
        norm_s[...] = normed
        inv_s[...] = jnp.broadcast_to(inverse, inv_s.shape)
        first_s[...] = first
        low = first.astype(BF)
        low_s[...] = low
        low_t[...] = jnp.transpose(low)
        down_s[...] = jnp.zeros_like(down_s)

    @pl.when(step < tps)
    def _():
        weight = feed_ref[:, 0, 0].reshape(model, -1)
        pre = contract(low_s[...], weight, 1, 0) + hid_ref[step]
        share = 0.5 + 0.5 * lax.erf(pre * 0.7071067811865476)
        hidden = (pre * share).astype(BF)
        hidden_s[step] = hidden
        slope_s[step] = (share + pre * (0.3989422804014327 * jnp.exp(-0.5 * pre * pre))).astype(BF)
        down_s[...] += contract(hidden, feed_ref[:, 0, 1].reshape(model, -1), 1, 1)

    @pl.when(step == tps)
    def _():
        normed, inverse = norm_parts(first_s[...] + down_s[...] + vec_ref[3:4])
        out_ref[...] = (normed * vec_ref[4:5] + vec_ref[5:6]).astype(BF)
        grad = cot_ref[...].astype(F32)
        tail_s[0:1] = column_sum(grad * normed)
        tail_s[1:2] = column_sum(grad)
        grad_mid = norm_back(grad, vec_ref[4:5], normed, inverse)
        gsum_ref[...] = grad_mid
        tail_s[2:3] = column_sum(grad_mid)
        grad_down = grad_mid.astype(BF)
        gdown_s[...] = grad_down
        gdown_t[...] = jnp.transpose(grad_down)
        down_s[...] = jnp.zeros_like(down_s)

    @pl.when(step >= tps)
    def _():
        block = 2 * tps - 1 - step
        slot = lax.rem(step, 2)

        @pl.when(step >= tps + 2)
        def _():
            send(slot, block + 2).wait()

        grad_hidden = contract(gdown_s[...], feed_ref[:, 0, 1].reshape(model, -1), 1, 0)
        grad_pre = grad_hidden * slope_s[block].astype(F32)
        grad_low = grad_pre.astype(BF)
        tail_s[pl.ds(8 + block, 1)] = column_sum(grad_low.astype(F32))
        down_s[...] += contract(grad_low, feed_ref[:, 0, 0].reshape(model, -1), 1, 1)
        stage_s[slot, :, :piece] = (
            contract(low_t[...], grad_low, 1, 0).astype(BF).reshape(dps, piece, -1)
        )
        stage_s[slot, :, piece:] = (
            contract(gdown_t[...], hidden_s[block], 1, 0).astype(BF).reshape(dps, piece, -1)
        )
        send(slot, block).start()

    @pl.when(step == 2 * tps - 1)
    def _():
        grad = gsum_ref[...] + down_s[...]
        normed = norm_s[...]
        grad_scale, grad_shift = column_sum(grad * normed), column_sum(grad)
        grad_sum = norm_back(grad, vec_ref[1:2], normed, inv_s[:, 0:1])
        gsum_ref[...] = grad_sum
        grad_bias = column_sum(grad_sum)
        low = grad_sum.astype(BF)
        low_t[...] = jnp.transpose(low)
        for t in range(tps):
            gatt_ref[t] = contract(low, outw_ref[:, t, :piece].reshape(model, -1), 1, 0).astype(BF)
        send(lax.rem(step + 1, 2), 1).wait()
        send(lax.rem(step, 2), 0).wait()
        part = piece // chunks
        width = att_ref.shape[2]
        six = jnp.concatenate(
            [grad_bias, grad_scale, grad_shift, tail_s[2:3], tail_s[0:1], tail_s[1:2]], axis=0
        )
        for t in range(tps):
            gout = contract(low_t[...], att_ref[t], 1, 0).reshape(dps, piece, width)
            wide = [gout[:, c * part : (c + 1) * part] for c in range(chunks)]
            if chunks * width < model:
                wide.append(jnp.zeros((dps, part, model - chunks * width), F32))
            stage_s[0, :, :part] = jnp.concatenate(wide, axis=2).astype(BF)
            rows = jnp.concatenate(
                [six, tail_s[8 + t : 9 + t], jnp.zeros((PAD - 7, model), F32)], axis=0
            ).astype(BF)
            stage_s[0, :, part : part + PAD] = jnp.broadcast_to(rows[None], (dps, PAD, model))
            copy = pltpu.make_async_copy(
                stage_s.at[0, :, pl.ds(0, part + PAD)],
                pack_ref.at[:, t, pl.ds(feed_rows, part + PAD)],
                sems.at[0],
            )
            copy.start()
            copy.wait()


def middle(att, tokens, cotangent, outw, vec, hid, feed):
    tps, rows, width = att.shape
    model = tokens.shape[1]
    dps, piece = feed.shape[0], feed.shape[3]
    chunks = min(model // width, piece // PAD)
    pack_rows = 2 * piece + piece // chunks + PAD

    def fixed(array):
        rank = len(array.shape)
        return pl.BlockSpec(
            array.shape, lambda i: (0,) * rank, pipeline_mode=pl.Buffered(buffer_count=1)
        )

    def feed_at(i):
        return (0, jnp.minimum(i, 2 * tps - 1 - i), 0, 0, 0)

    outs = [
        jax.ShapeDtypeStruct((rows, model), BF),
        jax.ShapeDtypeStruct((rows, model), F32),
        jax.ShapeDtypeStruct(att.shape, BF),
        jax.ShapeDtypeStruct((dps, tps, pack_rows, model), BF),
    ]
    return pl.pallas_call(
        lambda *refs: middle_kernel((dps, tps, piece, chunks), *refs),
        grid=(2 * tps,),
        in_specs=[fixed(a) for a in (att, tokens, cotangent, outw, vec, hid)]
        + [pl.BlockSpec((dps, 1, 2, piece, feed.shape[4]), feed_at)],
        out_specs=[fixed(a) for a in outs[:3]] + [pl.BlockSpec(memory_space=pl.ANY)],
        out_shape=outs,
        scratch_shapes=[
            pltpu.VMEM((rows, model), F32),
            pltpu.VMEM((rows, model), F32),
            pltpu.VMEM((rows, model), F32),
            pltpu.VMEM((rows, 128), F32),
            pltpu.VMEM((rows, model), BF),
            pltpu.VMEM((model, rows), BF),
            pltpu.VMEM((rows, model), BF),
            pltpu.VMEM((model, rows), BF),
            pltpu.VMEM((tps, rows, feed.shape[4]), BF),
            pltpu.VMEM((tps, rows, feed.shape[4]), BF),
            pltpu.VMEM((2, dps, 2 * piece, model), BF),
            pltpu.VMEM((16, model), F32),
            pltpu.SemaphoreType.DMA((2,)),
        ],
        cost_estimate=pl.CostEstimate(
            flops=6 * rows * model * model * (2 * tps + 1),
            bytes_accessed=60 << 20,
            transcendentals=0,
        ),
        compiler_params=pltpu.CompilerParams(vmem_limit_bytes=62 << 20),
        name="middle",
    )(att, tokens, cotangent, outw, vec, hid, feed)


def on_device(
    tokens,
    weight_query,
    weight_key,
    weight_value,
    weight_out,
    bias_query,
    bias_value,
    bias_out,
    first_scale,
    first_shift,
    weight_hidden,
    bias_hidden,
    weight_down,
    bias_down,
    second_scale,
    second_shift,
    cotangent,
):
    dps, tps = lax.axis_size("dp"), lax.axis_size("tensor")
    rows, model = tokens.shape
    piece = weight_hidden.shape[0]
    width = weight_query.shape[1]
    hidden_width = weight_hidden.shape[1]
    small = bias_query.shape[0]

    bias_row = jnp.concatenate([bias_query, bias_value])
    attn_bias = jnp.pad(bias_row[None], ((0, PAD - 1), (0, 3 * width - 2 * small)))
    attn_pack = jnp.concatenate(
        [jnp.concatenate([weight_query, weight_key, weight_value], axis=1), attn_bias], axis=0
    )
    attn_all = lax.all_gather(attn_pack, "dp", axis=0, tiled=False)
    rows_full = lax.all_gather(tokens, "tensor", axis=0, tiled=True)
    vec_row = jnp.concatenate(
        [bias_out, first_scale, first_shift, bias_down, second_scale, second_shift, bias_hidden]
    )
    vec_flat = jnp.pad(vec_row, (0, PAD * width - vec_row.shape[0])).reshape(PAD, width)
    out_all = lax.all_gather(
        jnp.concatenate([weight_out.T, vec_flat], axis=0), BOTH, axis=0, tiled=False
    ).reshape(dps, tps, piece + PAD, width)
    feed_all = lax.all_gather(
        jnp.concatenate([weight_hidden, weight_down.T], axis=0), BOTH, axis=0, tiled=False
    ).reshape(dps, tps, 2, piece, hidden_width)

    qkv_weight = attn_all[:, :piece].reshape(model, 3 * width)
    query_bias = attn_all[:, piece, :small].reshape(width).astype(F32)
    value_bias = attn_all[:, piece, small : 2 * small].reshape(width).astype(F32)
    bias_full = jnp.concatenate([query_bias, jnp.zeros_like(query_bias), value_bias])
    qkv = (contract(rows_full, qkv_weight, 1, 0) + bias_full).astype(BF)
    attended, logsum = attend_forward(qkv)
    crossed = lax.all_to_all(attended.reshape(tps, rows, width), "tensor", 0, 0, tiled=False)

    vecs = out_all[:, :, piece:].reshape(dps, tps, PAD * width)
    vec = vecs[:, 0, : 6 * piece].reshape(dps, 6, piece).transpose(1, 0, 2).reshape(6, model)
    vec = jnp.pad(vec.astype(F32), ((0, 2), (0, 0)))
    hid = vecs[:, :, 6 * piece : 6 * piece + bias_hidden.shape[0]].transpose(1, 0, 2)
    hid = hid.reshape(tps, 1, hidden_width).astype(F32)
    output, grad_sum, grad_cross, packed = middle(
        crossed, tokens, cotangent, out_all, vec, hid, feed_all
    )
    grad_attended = lax.all_to_all(grad_cross, "tensor", 0, 0, tiled=False)
    grad_attended = grad_attended.reshape(tps * rows, width)
    packed = lax.psum_scatter(packed, "dp", scatter_dimension=0, tiled=False)
    packed = lax.psum_scatter(packed, "tensor", scatter_dimension=0, tiled=False).astype(F32)

    grads = attend_backward(qkv, grad_attended, attended, logsum)
    grad_rows, weight_grads, sums = None, [], []
    for index, grad in enumerate(grads):
        weight = qkv_weight[:, index * width : (index + 1) * width]
        part = contract(grad, weight, 1, 1)
        grad_rows = part if grad_rows is None else grad_rows + part
        weight_grads.append(contract(rows_full, grad, 0, 0).astype(BF))
        sums.append(jnp.sum(grad, axis=0, dtype=F32).astype(BF))
    grad_tokens = (
        grad_sum
        + lax.psum_scatter(
            grad_rows.astype(BF), "tensor", scatter_dimension=0, tiled=True
        ).astype(F32)
    ).astype(BF)
    tail = jnp.pad(jnp.concatenate(sums)[None], ((0, PAD - 1), (0, 0)))
    attn_grads = jnp.concatenate(
        [
            jnp.concatenate(weight_grads, axis=1).reshape(dps, piece, 3 * width),
            jnp.broadcast_to(tail[None], (dps, PAD, 3 * width)),
        ],
        axis=1,
    )
    attn_grads = lax.psum_scatter(attn_grads, "dp", scatter_dimension=0, tiled=False).astype(F32)

    place = lax.axis_index("dp")

    def share(values, count):
        return lax.dynamic_slice_in_dim(values, place * count, count, 0)

    chunks = min(model // width, piece // PAD)
    part = piece // chunks
    out_grad = packed[2 * piece : 2 * piece + part, : chunks * width]
    out_grad = out_grad.reshape(part, chunks, width).transpose(2, 1, 0).reshape(width, piece)
    vec_grads = [share(packed[2 * piece + part + i], piece) for i in range(6)]
    hidden_grad = share(packed[2 * piece + part + 6], bias_hidden.shape[0])
    return (
        output,
        grad_tokens,
        attn_grads[:piece, :width],
        attn_grads[:piece, width : 2 * width],
        attn_grads[:piece, 2 * width :],
        out_grad,
        share(attn_grads[piece, :width], small),
        share(attn_grads[piece, 2 * width :], small),
        vec_grads[0],
        vec_grads[1],
        vec_grads[2],
        packed[:piece],
        hidden_grad,
        packed[piece : 2 * piece].T,
        vec_grads[3],
        vec_grads[4],
        vec_grads[5],
    )


def solution(mesh):
    placed = (
        P(("dp", "tensor"), None),
        P("dp", "tensor"),
        P("dp", "tensor"),
        P("dp", "tensor"),
        P("tensor", "dp"),
        P(("tensor", "dp")),
        P(("tensor", "dp")),
        P("dp"),
        P("dp"),
        P("dp"),
        P("dp", "tensor"),
        P(("tensor", "dp")),
        P("tensor", "dp"),
        P("dp"),
        P("dp"),
        P("dp"),
        P(("dp", "tensor"), None),
    )
    return jax.shard_map(
        on_device,
        mesh=mesh,
        in_specs=placed,
        out_specs=(
            P(("dp", "tensor"), None),
            P(("dp", "tensor"), None),
            P("dp", "tensor"),
            P("dp", "tensor"),
            P("dp", "tensor"),
            P("tensor", "dp"),
            P(("tensor", "dp")),
            P(("tensor", "dp")),
            P("dp"),
            P("dp"),
            P("dp"),
            P("dp", "tensor"),
            P(("tensor", "dp")),
            P("tensor", "dp"),
            P("dp"),
            P("dp"),
            P("dp"),
        ),
        check_vma=False,
    )
```

```python
import jax
import jax.numpy as jnp
from jax import lax
from jax.experimental import pallas as pl
from jax.experimental.pallas import tpu as pltpu
from jax.sharding import PartitionSpec as P

HD = 64
LEN = 2048
QB = 256
PAIR = 2 * HD
PAD = 16
F32 = jnp.float32
BF = jnp.bfloat16
BOTH = ("dp", "tensor")


def contract(left, right, left_dim, right_dim):
    return lax.dot_general(
        left, right, (((left_dim,), (right_dim,)), ((), ())), preferred_element_type=F32
    )


def one_head(pair, head):
    lane = lax.broadcasted_iota(jnp.int32, pair.shape, 1)
    keep = lane < HD if head == 0 else lane >= HD
    return jnp.where(keep, pair, jnp.zeros_like(pair))


CUTS = 4


def flipped(index, bit):
    size = 1 << bit
    return index + size - 2 * size * lax.rem(index // size, 2)


def bit_order(dps):
    count = dps.bit_length() - 1
    return tuple(range(1, count)) + (0,)


def greet(dps, tps):
    place, level = lax.axis_index("dp"), lax.axis_index("tensor")
    barrier = pltpu.get_barrier_semaphore()
    for bit in bit_order(dps):
        pl.semaphore_signal(barrier, inc=1, device_id={"dp": flipped(place, bit)})
    for step in range(1, tps):
        pl.semaphore_signal(barrier, inc=1, device_id={"tensor": lax.rem(level + step, tps)})
    pl.semaphore_wait(barrier, len(bit_order(dps)) + tps - 1)


def front_kernel(
    dps,
    tps,
    tok_ref,
    pack_ref,
    rows_ref,
    packs_ref,
    qkv_ref,
    weight_s,
    right_sem,
    left_sem,
    land_sem,
    pack_send,
    pack_land,
    local_sem,
):
    place, level = lax.axis_index("dp"), lax.axis_index("tensor")
    rows, model = tok_ref.shape
    piece = model // dps
    cut = rows // CUTS
    own = pltpu.make_async_copy(tok_ref, rows_ref.at[level], local_sem.at[0])
    own_pack = pltpu.make_async_copy(pack_ref, packs_ref.at[place], local_sem.at[1])
    own.start()
    own_pack.start()
    greet(dps, tps)

    def hop(block, chunk, rightward, first=False):
        span = pl.ds(chunk * cut, cut)
        return pltpu.make_async_remote_copy(
            src_ref=tok_ref.at[span] if first else rows_ref.at[block, span],
            dst_ref=rows_ref.at[block, span],
            send_sem=(right_sem if rightward else left_sem).at[block, chunk],
            recv_sem=land_sem.at[block, chunk],
            device_id={"tensor": level + 1 if rightward else level - 1},
        )

    for chunk in range(CUTS):

        @pl.when(level < tps - 1)
        def _():
            hop(level, chunk, True, True).start()

        @pl.when(level > 0)
        def _():
            hop(level, chunk, False, True).start()

    own_pack.wait()
    held = [place]
    for bit in bit_order(dps):
        copies = []
        for block in held:
            copies.append(
                pltpu.make_async_remote_copy(
                    src_ref=packs_ref.at[block],
                    dst_ref=packs_ref.at[block],
                    send_sem=pack_send.at[block],
                    recv_sem=pack_land.at[block],
                    device_id={"dp": flipped(place, bit)},
                )
            )
            copies[-1].start()
        for copy in copies:
            copy.wait_send()
        more = [flipped(block, bit) for block in held]
        for block in more:
            pltpu.make_async_remote_copy(
                src_ref=packs_ref.at[block],
                dst_ref=packs_ref.at[block],
                send_sem=pack_send.at[block],
                recv_sem=pack_land.at[block],
                device_id={"dp": flipped(place, bit)},
            ).wait_recv()
        held = held + more
    weight_s[...] = packs_ref[:, :piece].reshape(weight_s.shape)
    bias = jnp.sum(packs_ref[:, piece : piece + PAD].astype(F32), axis=0)[0:1]

    def project(block):
        qkv_ref[block] = (contract(rows_ref[block], weight_s[...], 1, 0) + bias).astype(BF)

    own.wait()
    project(level)
    for step in range(1, tps):
        for chunk in range(CUTS):

            @pl.when(level - step >= 0)
            def _():
                hop(level - step, chunk, True).wait_recv()

            @pl.when((level - step >= 0) & (level < tps - 1))
            def _():
                hop(level - step, chunk, True).start()

            @pl.when(level + step < tps)
            def _():
                hop(level + step, chunk, False).wait_recv()

            @pl.when((level + step < tps) & (level > 0))
            def _():
                hop(level + step, chunk, False).start()

        @pl.when(level - step >= 0)
        def _():
            project(level - step)

        @pl.when(level + step < tps)
        def _():
            project(level + step)

    for step in range(tps):
        for chunk in range(CUTS):

            @pl.when((level - step >= 0) & (level < tps - 1))
            def _():
                hop(level - step, chunk, True, step == 0).wait_send()

            @pl.when((level + step < tps) & (level > 0))
            def _():
                hop(level + step, chunk, False, step == 0).wait_send()


def front(tokens, pack, dps, tps):
    rows, model = tokens.shape
    columns = pack.shape[1]
    vmem = pl.BlockSpec(memory_space=pltpu.VMEM)
    return pl.pallas_call(
        lambda *refs: front_kernel(dps, tps, *refs),
        in_specs=[vmem] * 2,
        out_specs=[vmem] * 3,
        out_shape=[
            jax.ShapeDtypeStruct((tps, rows, model), BF),
            jax.ShapeDtypeStruct((dps,) + pack.shape, BF),
            jax.ShapeDtypeStruct((tps, rows, columns), BF),
        ],
        scratch_shapes=[
            pltpu.VMEM((model, columns), BF),
            pltpu.SemaphoreType.DMA((tps, CUTS)),
            pltpu.SemaphoreType.DMA((tps, CUTS)),
            pltpu.SemaphoreType.DMA((tps, CUTS)),
            pltpu.SemaphoreType.DMA((dps,)),
            pltpu.SemaphoreType.DMA((dps,)),
            pltpu.SemaphoreType.DMA((2,)),
        ],
        cost_estimate=pl.CostEstimate(
            flops=2 * tps * rows * model * columns, bytes_accessed=200 << 20, transcendentals=0
        ),
        compiler_params=pltpu.CompilerParams(
            vmem_limit_bytes=32 << 20, collective_id=1, has_side_effects=True
        ),
        name="front",
    )(tokens, pack)


def back_kernel(
    dps,
    tps,
    dq_ref,
    dk_ref,
    dv_ref,
    rows_ref,
    packs_ref,
    gsum_ref,
    tok_out,
    pack_out,
    weight_s,
    part_s,
    right_s,
    left_s,
    mine_s,
    theirs_s,
    right_send,
    right_land,
    left_send,
    left_land,
    pack_send,
    pack_land,
):
    place, level = lax.axis_index("dp"), lax.axis_index("tensor")
    rows, model = gsum_ref.shape
    piece = model // dps
    cut = rows // CUTS
    width = dq_ref.shape[1]
    greet(dps, tps)
    weight_s[...] = packs_ref[:, :piece].reshape(weight_s.shape)

    def rows_of(block):
        span = pl.ds(pl.multiple_of(block * rows, rows), rows)
        total = None
        for index, ref in enumerate((dq_ref, dk_ref, dv_ref)):
            weight = weight_s[:, index * width : (index + 1) * width]
            part = contract(ref[span], weight, 1, 1)
            total = part if total is None else total + part
        part_s[block] = total.astype(BF)

    def hop(block, chunk, rightward):
        span = pl.ds(chunk * cut, cut)
        land = right_s if rightward else left_s
        return pltpu.make_async_remote_copy(
            src_ref=part_s.at[block, span],
            dst_ref=land.at[block, span],
            send_sem=(right_send if rightward else left_send).at[block, chunk],
            recv_sem=(right_land if rightward else left_land).at[block, chunk],
            device_id={"tensor": level + 1 if rightward else level - 1},
        )

    def gather_in(block, chunk, rightward):
        hop(block, chunk, rightward).wait_recv()
        span = pl.ds(chunk * cut, cut)
        land = right_s if rightward else left_s
        part_s[block, span] = (
            part_s[block, span].astype(F32) + land[block, span].astype(F32)
        ).astype(BF)

    for step in range(tps - 1, 0, -1):

        @pl.when(level + step < tps)
        def _():
            rows_of(level + step)

        @pl.when((level + step < tps) & (level == 0))
        def _():
            for chunk in range(CUTS):
                hop(level + step, chunk, True).start()

        @pl.when(level - step >= 0)
        def _():
            rows_of(level - step)

        @pl.when((level - step >= 0) & (level == tps - 1))
        def _():
            for chunk in range(CUTS):
                hop(level - step, chunk, False).start()

    rows_of(level)
    model_rows = rows_ref.reshape(tps * rows, model)
    tail = jnp.concatenate(
        [jnp.sum(ref[...].astype(F32), axis=0, keepdims=True) for ref in (dq_ref, dk_ref, dv_ref)],
        axis=1,
    )
    for index, ref in enumerate((dq_ref, dk_ref, dv_ref)):
        grad = contract(model_rows[...], ref[...], 0, 0).astype(BF).reshape(dps, piece, width)
        mine_s[:, :piece, index * width : (index + 1) * width] = grad
    mine_s[:, piece:] = jnp.broadcast_to(tail.astype(BF)[None], (dps, PAD, 3 * width))

    def exchange(index, bit, other):
        return pltpu.make_async_remote_copy(
            src_ref=mine_s.at[other],
            dst_ref=theirs_s.at[index],
            send_sem=pack_send.at[index],
            recv_sem=pack_land.at[index],
            device_id={"dp": flipped(place, bit)},
        )

    order = bit_order(dps)[::-1]

    def kept(done):
        blocks = [place]
        for bit in order[done:][::-1]:
            blocks = blocks + [flipped(block, bit) for block in blocks]
        return blocks

    starts = []
    at = 0
    for done in range(len(order)):
        starts.append(at)
        at += dps >> (done + 1)

    def pack_start(done):
        for index, block in enumerate(kept(done + 1)):
            exchange(starts[done] + index, order[done], flipped(block, order[done])).start()

    def pack_finish(done):
        for index, block in enumerate(kept(done + 1)):
            exchange(starts[done] + index, order[done], block).wait()
            mine_s[block] = (
                mine_s[block].astype(F32) + theirs_s[starts[done] + index].astype(F32)
            ).astype(BF)

    pack_start(0)
    pack_done = 0
    for step in range(tps - 1, 0, -1):
        for chunk in range(CUTS):

            @pl.when((level > 0) & (level + step < tps))
            def _():
                gather_in(level + step, chunk, True)
                hop(level + step, chunk, True).start()

            @pl.when((level < tps - 1) & (level - step >= 0))
            def _():
                gather_in(level - step, chunk, False)
                hop(level - step, chunk, False).start()

        if pack_done < len(order):
            pack_finish(pack_done)
            pack_done += 1
            if pack_done < len(order):
                pack_start(pack_done)
    while pack_done < len(order):
        pack_finish(pack_done)
        pack_done += 1
        if pack_done < len(order):
            pack_start(pack_done)
    pack_out[...] = mine_s[place].astype(F32)
    for chunk in range(CUTS):

        @pl.when(level > 0)
        def _():
            hop(level, chunk, True).wait_recv()

        @pl.when(level < tps - 1)
        def _():
            hop(level, chunk, False).wait_recv()

    total = gsum_ref[...] + part_s[level].astype(F32)
    total = total + jnp.where(level > 0, right_s[level].astype(F32), 0.0)
    total = total + jnp.where(level < tps - 1, left_s[level].astype(F32), 0.0)
    tok_out[...] = total.astype(BF)
    for step in range(1, tps):
        for chunk in range(CUTS):

            @pl.when(level + step < tps)
            def _():
                hop(level + step, chunk, True).wait_send()

            @pl.when(level - step >= 0)
            def _():
                hop(level - step, chunk, False).wait_send()


def back(grads, rows_full, packs, grad_sum):
    rows, model = grad_sum.shape
    tps = rows_full.shape[0]
    dps, pack_rows, columns = packs.shape
    vmem = pl.BlockSpec(memory_space=pltpu.VMEM)
    return pl.pallas_call(
        lambda *refs: back_kernel(dps, tps, *refs),
        in_specs=[vmem] * 6,
        out_specs=[vmem] * 2,
        out_shape=[
            jax.ShapeDtypeStruct((rows, model), BF),
            jax.ShapeDtypeStruct((pack_rows, columns), F32),
        ],
        scratch_shapes=[
            pltpu.VMEM((model, columns), BF),
            pltpu.VMEM((tps, rows, model), BF),
            pltpu.VMEM((tps, rows, model), BF),
            pltpu.VMEM((tps, rows, model), BF),
            pltpu.VMEM(packs.shape, BF),
            pltpu.VMEM(packs.shape, BF),
        ]
        + [pltpu.SemaphoreType.DMA((tps, CUTS))] * 4
        + [pltpu.SemaphoreType.DMA((dps,))] * 2,
        cost_estimate=pl.CostEstimate(
            flops=4 * tps * rows * model * columns, bytes_accessed=200 << 20, transcendentals=0
        ),
        compiler_params=pltpu.CompilerParams(
            vmem_limit_bytes=56 << 20, collective_id=2, has_side_effects=True
        ),
        name="back",
    )(*grads, rows_full, packs, grad_sum)


def pack_kernel(hidden_ref, down_ref, out_ref, vec_ref, packed_ref):
    piece, wide = hidden_ref.shape
    width = out_ref.shape[0]
    chunks = min(wide // width, piece // PAD)
    part = piece // chunks
    packed_ref[:piece] = hidden_ref[...]
    packed_ref[piece : 2 * piece] = jnp.transpose(down_ref[...])
    turned = jnp.transpose(out_ref[...])
    for chunk in range(chunks):
        packed_ref[2 * piece : 2 * piece + part, chunk * width : (chunk + 1) * width] = turned[
            chunk * part : (chunk + 1) * part
        ]
    if chunks * width < wide:
        packed_ref[2 * piece : 2 * piece + part, chunks * width :] = jnp.zeros(
            (part, wide - chunks * width), BF
        )
    packed_ref[2 * piece + part :] = vec_ref[...]


def pack_weights(hidden, down, out, vec):
    piece, wide = hidden.shape
    chunks = min(wide // out.shape[0], piece // PAD)
    return pl.pallas_call(
        pack_kernel,
        out_shape=jax.ShapeDtypeStruct((2 * piece + piece // chunks + PAD, wide), BF),
        name="pack",
    )(hidden, down, out, vec)


def attend_forward_kernel(q_ref, k_ref, v_ref, out_ref, logsum_ref):
    query = q_ref[...] * jnp.asarray(0.125, BF)
    key, value = k_ref[...], v_ref[...]
    total, columns = None, []
    for head in range(2):
        scores = contract(query, one_head(key, head), 1, 1)
        highest = jnp.max(scores, axis=1, keepdims=True)
        expons = jnp.exp(scores - highest)
        mass = jnp.sum(expons, axis=1, keepdims=True)
        part = contract(expons.astype(BF), one_head(value, head), 1, 0) / mass
        total = part if total is None else total + part
        columns.append(jnp.broadcast_to(highest + jnp.log(mass), (query.shape[0], PAIR)))
    out_ref[...] = total.astype(BF)
    logsum_ref[0] = jnp.concatenate([jnp.transpose(column)[:4] for column in columns], axis=0)


def attend_forward(qkv):
    width = qkv.shape[1] // 3
    pairs = width // PAIR
    block = pl.BlockSpec((QB, PAIR), lambda i, j: (j, i))
    key_block = pl.BlockSpec((LEN, PAIR), lambda i, j: (0, i + pairs))
    value_block = pl.BlockSpec((LEN, PAIR), lambda i, j: (0, i + 2 * pairs))
    return pl.pallas_call(
        attend_forward_kernel,
        grid=(width // PAIR, LEN // QB),
        in_specs=[block, key_block, value_block],
        out_specs=[block, pl.BlockSpec((1, 8, QB), lambda i, j: (i, 0, j))],
        out_shape=[
            jax.ShapeDtypeStruct((LEN, width), BF),
            jax.ShapeDtypeStruct((width // PAIR, 8, LEN), F32),
        ],
        cost_estimate=pl.CostEstimate(
            flops=20 * LEN * LEN * width, bytes_accessed=12 * LEN * width, transcendentals=0
        ),
        compiler_params=pltpu.CompilerParams(vmem_limit_bytes=40 << 20),
        name="attend_forward",
    )(qkv, qkv, qkv)


def attend_backward_kernel(
    q_ref, k_ref, v_ref, grad_ref, out_ref, logsum_ref, dq_ref, dk_ref, dv_ref, dk_sum, dv_sum
):
    step = pl.program_id(1)
    query = q_ref[...] * jnp.asarray(0.125, BF)
    key, value, grad = k_ref[...], v_ref[...], grad_ref[...]
    products = jnp.transpose(grad.astype(F32) * out_ref[...].astype(F32))

    @pl.when(step == 0)
    def _():
        dk_sum[...] = jnp.zeros_like(dk_sum)
        dv_sum[...] = jnp.zeros_like(dv_sum)

    grad_query = None
    for head in range(2):
        key_head, value_head = one_head(key, head), one_head(value, head)
        inner = jnp.sum(products[HD * head : HD * head + HD], axis=0, keepdims=True)
        logsum = logsum_ref[0, 4 * head : 4 * head + 1, :]
        probs = jnp.exp(contract(key_head, query, 1, 1) - logsum)
        grad_probs = contract(value_head, grad, 1, 1)
        grad_scores = (probs * (grad_probs - inner)).astype(BF)
        dv_sum[...] += contract(probs.astype(BF), one_head(grad, head), 1, 0)
        dk_sum[...] += contract(grad_scores, one_head(query, head), 1, 0)
        part = contract(grad_scores, key_head, 0, 0)
        grad_query = part if grad_query is None else grad_query + part
    dq_ref[...] = (grad_query * 0.125).astype(BF)

    @pl.when(step == pl.num_programs(1) - 1)
    def _():
        dk_ref[...] = dk_sum[...].astype(BF)
        dv_ref[...] = dv_sum[...].astype(BF)


def attend_backward(qkv, grad, out, logsum):
    width = qkv.shape[1] // 3
    pairs = width // PAIR
    block = pl.BlockSpec((QB, PAIR), lambda i, j: (j, i))
    whole = pl.BlockSpec((LEN, PAIR), lambda i, j: (0, i))
    return pl.pallas_call(
        attend_backward_kernel,
        grid=(width // PAIR, LEN // QB),
        in_specs=[
            block,
            pl.BlockSpec((LEN, PAIR), lambda i, j: (0, i + pairs)),
            pl.BlockSpec((LEN, PAIR), lambda i, j: (0, i + 2 * pairs)),
            block,
            block,
            pl.BlockSpec((1, 8, QB), lambda i, j: (i, 0, j)),
        ],
        out_specs=[block, whole, whole],
        out_shape=[jax.ShapeDtypeStruct((LEN, width), BF)] * 3,
        scratch_shapes=[pltpu.VMEM((LEN, PAIR), F32)] * 2,
        cost_estimate=pl.CostEstimate(
            flops=40 * LEN * LEN * width, bytes_accessed=18 * LEN * width, transcendentals=0
        ),
        compiler_params=pltpu.CompilerParams(vmem_limit_bytes=40 << 20),
        name="attend_backward",
    )(qkv, qkv, qkv, grad, out, logsum)


def row_mean(values):
    return jnp.mean(values, axis=1, keepdims=True)


def column_sum(values):
    return jnp.sum(values, axis=0, keepdims=True)


def middle_kernel(
    sizes,
    att_ref,
    tok_ref,
    cot_ref,
    all_ref,
    feed_ref,
    out_ref,
    gsum_ref,
    gatt_ref,
    pack_ref,
    first_s,
    norm_s,
    down_s,
    inv_s,
    low_s,
    low_t,
    gdown_s,
    gdown_t,
    hidden_s,
    slope_s,
    stage_s,
    tail_s,
    extra_s,
    wout_s,
    vec_s,
    sems,
    extra_sem,
):
    dps, tps, piece, chunks = sizes
    step = pl.program_id(0)
    model = tok_ref.shape[1]
    feed_rows = 2 * piece
    part = piece // chunks
    width = att_ref.shape[2]

    def norm_parts(values):
        centered = values - row_mean(values)
        inverse = lax.rsqrt(row_mean(centered * centered) + 1e-05)
        return centered * inverse, inverse

    def norm_back(grad, scale, normed, inverse):
        scaled = grad * scale
        return inverse * (scaled - row_mean(scaled) - normed * row_mean(scaled * normed))

    def send(slot, block):
        return pltpu.make_async_copy(
            stage_s.at[slot], pack_ref.at[:, block, pl.ds(0, feed_rows)], sems.at[slot]
        )

    @pl.when(step == 0)
    def _():
        def fetch(t):
            return pltpu.make_async_copy(
                all_ref.at[:, t, pl.ds(feed_rows, part + PAD)], extra_s.at[t % 2], extra_sem.at[t % 2]
            )

        fetch(0).start()
        for t in range(tps):
            if t + 1 < tps:
                fetch(t + 1).start()
            fetch(t).wait()
            extra = extra_s.at[t % 2]
            placed = jnp.sum(extra[:, part:].astype(F32), axis=0)
            if t == 0:
                vec_s[0:8] = placed[0:8]
            vec_s[8 + t : 9 + t] = placed[6:7]
            turned = jnp.concatenate(
                [extra[:, :part, c * width : (c + 1) * width] for c in range(chunks)], axis=1
            )
            wout_s[t] = turned.reshape(model, width)
        branch = None
        for t in range(tps):
            term = contract(att_ref[t], wout_s[t], 1, 1)
            branch = term if branch is None else branch + term
        normed, inverse = norm_parts(tok_ref[...].astype(F32) + branch + vec_s[0:1])
        first = normed * vec_s[1:2] + vec_s[2:3]
        norm_s[...] = normed
        inv_s[...] = jnp.broadcast_to(inverse, inv_s.shape)
        first_s[...] = first
        low = first.astype(BF)
        low_s[...] = low
        low_t[...] = jnp.transpose(low)
        down_s[...] = jnp.zeros_like(down_s)

    @pl.when(step < tps)
    def _():
        weight = feed_ref[:, 0, :piece].reshape(model, -1)
        pre = contract(low_s[...], weight, 1, 0) + vec_s[pl.ds(8 + step, 1)]
        share = 0.5 + 0.5 * lax.erf(pre * 0.7071067811865476)
        hidden = (pre * share).astype(BF)
        hidden_s[step] = hidden
        slope_s[step] = (share + pre * (0.3989422804014327 * jnp.exp(-0.5 * pre * pre))).astype(BF)
        down_s[...] += contract(hidden, feed_ref[:, 0, piece:].reshape(model, -1), 1, 1)

    @pl.when(step == tps)
    def _():
        normed, inverse = norm_parts(first_s[...] + down_s[...] + vec_s[3:4])
        out_ref[...] = (normed * vec_s[4:5] + vec_s[5:6]).astype(BF)
        grad = cot_ref[...].astype(F32)
        tail_s[0:1] = column_sum(grad * normed)
        tail_s[1:2] = column_sum(grad)
        grad_mid = norm_back(grad, vec_s[4:5], normed, inverse)
        gsum_ref[...] = grad_mid
        tail_s[2:3] = column_sum(grad_mid)
        grad_down = grad_mid.astype(BF)
        gdown_s[...] = grad_down
        gdown_t[...] = jnp.transpose(grad_down)
        down_s[...] = jnp.zeros_like(down_s)

    @pl.when(step >= tps)
    def _():
        block = 2 * tps - 1 - step
        slot = lax.rem(step, 2)

        @pl.when(step >= tps + 2)
        def _():
            send(slot, block + 2).wait()

        grad_hidden = contract(gdown_s[...], feed_ref[:, 0, piece:].reshape(model, -1), 1, 0)
        grad_pre = grad_hidden * slope_s[block].astype(F32)
        grad_low = grad_pre.astype(BF)
        tail_s[pl.ds(8 + block, 1)] = column_sum(grad_low.astype(F32))
        down_s[...] += contract(grad_low, feed_ref[:, 0, :piece].reshape(model, -1), 1, 1)
        stage_s[slot, :, :piece] = (
            contract(low_t[...], grad_low, 1, 0).astype(BF).reshape(dps, piece, -1)
        )
        stage_s[slot, :, piece:] = (
            contract(gdown_t[...], hidden_s[block], 1, 0).astype(BF).reshape(dps, piece, -1)
        )
        send(slot, block).start()

    @pl.when(step == 2 * tps - 1)
    def _():
        grad = gsum_ref[...] + down_s[...]
        normed = norm_s[...]
        grad_scale, grad_shift = column_sum(grad * normed), column_sum(grad)
        grad_sum = norm_back(grad, vec_s[1:2], normed, inv_s[:, 0:1])
        gsum_ref[...] = grad_sum
        grad_bias = column_sum(grad_sum)
        low = grad_sum.astype(BF)
        low_t[...] = jnp.transpose(low)
        for t in range(tps):
            gatt_ref[t] = contract(low, wout_s[t], 1, 0).astype(BF)
        send(lax.rem(step + 1, 2), 1).wait()
        send(lax.rem(step, 2), 0).wait()
        six = jnp.concatenate(
            [grad_bias, grad_scale, grad_shift, tail_s[2:3], tail_s[0:1], tail_s[1:2]], axis=0
        )
        for t in range(tps):
            gout = contract(low_t[...], att_ref[t], 1, 0).reshape(dps, piece, width)
            wide = [gout[:, c * part : (c + 1) * part] for c in range(chunks)]
            if chunks * width < model:
                wide.append(jnp.zeros((dps, part, model - chunks * width), F32))
            stage_s[0, :, :part] = jnp.concatenate(wide, axis=2).astype(BF)
            rows = jnp.concatenate(
                [six, tail_s[8 + t : 9 + t], jnp.zeros((PAD - 7, model), F32)], axis=0
            ).astype(BF)
            stage_s[0, :, part : part + PAD] = jnp.broadcast_to(rows[None], (dps, PAD, model))
            copy = pltpu.make_async_copy(
                stage_s.at[0, :, pl.ds(0, part + PAD)],
                pack_ref.at[:, t, pl.ds(feed_rows, part + PAD)],
                sems.at[0],
            )
            copy.start()
            copy.wait()


def middle(att, tokens, cotangent, gathered):
    tps, rows, width = att.shape
    model = tokens.shape[1]
    dps, wide = gathered.shape[0], gathered.shape[3]
    piece = model // dps
    chunks = min(model // width, piece // PAD)
    pack_rows = 2 * piece + piece // chunks + PAD

    def fixed(array):
        rank = len(array.shape)
        return pl.BlockSpec(
            array.shape, lambda i: (0,) * rank, pipeline_mode=pl.Buffered(buffer_count=1)
        )

    def feed_at(i):
        return (0, jnp.minimum(i, 2 * tps - 1 - i), 0, 0)

    outs = [
        jax.ShapeDtypeStruct((rows, model), BF),
        jax.ShapeDtypeStruct((rows, model), F32),
        jax.ShapeDtypeStruct(att.shape, BF),
        jax.ShapeDtypeStruct((dps, tps, pack_rows, model), BF),
    ]
    return pl.pallas_call(
        lambda *refs: middle_kernel((dps, tps, piece, chunks), *refs),
        grid=(2 * tps,),
        in_specs=[fixed(a) for a in (att, tokens, cotangent)]
        + [
            pl.BlockSpec(memory_space=pl.ANY),
            pl.BlockSpec((dps, 1, 2 * piece, wide), feed_at),
        ],
        out_specs=[fixed(a) for a in outs[:3]] + [pl.BlockSpec(memory_space=pl.ANY)],
        out_shape=outs,
        scratch_shapes=[
            pltpu.VMEM((rows, model), F32),
            pltpu.VMEM((rows, model), F32),
            pltpu.VMEM((rows, model), F32),
            pltpu.VMEM((rows, 128), F32),
            pltpu.VMEM((rows, model), BF),
            pltpu.VMEM((model, rows), BF),
            pltpu.VMEM((rows, model), BF),
            pltpu.VMEM((model, rows), BF),
            pltpu.VMEM((tps, rows, wide), BF),
            pltpu.VMEM((tps, rows, wide), BF),
            pltpu.VMEM((2, dps, 2 * piece, model), BF),
            pltpu.VMEM((16, model), F32),
            pltpu.VMEM((2, dps, piece // chunks + PAD, wide), BF),
            pltpu.VMEM((tps, model, width), BF),
            pltpu.VMEM((16, model), F32),
            pltpu.SemaphoreType.DMA((2,)),
            pltpu.SemaphoreType.DMA((2,)),
        ],
        cost_estimate=pl.CostEstimate(
            flops=6 * rows * model * model * (2 * tps + 1),
            bytes_accessed=60 << 20,
            transcendentals=0,
        ),
        compiler_params=pltpu.CompilerParams(vmem_limit_bytes=62 << 20),
        name="middle",
    )(att, tokens, cotangent, gathered, gathered)


def on_device(
    tokens,
    weight_query,
    weight_key,
    weight_value,
    weight_out,
    bias_query,
    bias_value,
    bias_out,
    first_scale,
    first_shift,
    weight_hidden,
    bias_hidden,
    weight_down,
    bias_down,
    second_scale,
    second_shift,
    cotangent,
):
    dps, tps = lax.axis_size("dp"), lax.axis_size("tensor")
    rows, model = tokens.shape
    piece = weight_hidden.shape[0]
    width = weight_query.shape[1]
    small = bias_query.shape[0]

    place = lax.axis_index("dp")

    def placed(pieces, length):
        zeros = jnp.zeros((pieces.shape[0], length), BF)
        return lax.dynamic_update_slice_in_dim(zeros, pieces, place * pieces.shape[1], 1)

    vec_rows = placed(
        jnp.stack(
            [bias_out, first_scale, first_shift, bias_down, second_scale, second_shift, bias_hidden]
        ),
        model,
    )
    packed_weights = pack_weights(
        weight_hidden, weight_down, weight_out, jnp.pad(vec_rows, ((0, PAD - 7), (0, 0)))
    )
    gathered = lax.all_gather(packed_weights, BOTH, axis=0, tiled=False)
    gathered = gathered.reshape((dps, tps) + packed_weights.shape)

    bias_rows = placed(jnp.stack([bias_query, bias_value]), width)
    bias_row = jnp.concatenate([bias_rows[0:1], jnp.zeros((1, width), BF), bias_rows[1:2]], axis=1)
    attn_pack = jnp.concatenate(
        [
            jnp.concatenate([weight_query, weight_key, weight_value], axis=1),
            jnp.pad(bias_row, ((0, PAD - 1), (0, 0))),
        ],
        axis=0,
    )
    rows_full, packs, qkv = front(tokens, attn_pack, dps, tps)
    qkv = qkv.reshape(tps * rows, 3 * width)
    attended, logsum = attend_forward(qkv)
    crossed = lax.all_to_all(attended.reshape(tps, rows, width), "tensor", 0, 0, tiled=False)

    output, grad_sum, grad_cross, packed = middle(crossed, tokens, cotangent, gathered)
    grad_attended = lax.all_to_all(grad_cross, "tensor", 0, 0, tiled=False)
    grad_attended = grad_attended.reshape(tps * rows, width)
    packed = lax.psum_scatter(packed, "dp", scatter_dimension=0, tiled=False)
    packed = lax.psum_scatter(packed, "tensor", scatter_dimension=0, tiled=False).astype(F32)

    grads = attend_backward(qkv, grad_attended, attended, logsum)
    grad_tokens, attn_grads = back(grads, rows_full, packs, grad_sum)

    def share(values, count):
        return lax.dynamic_slice_in_dim(values, place * count, count, 0)

    chunks = min(model // width, piece // PAD)
    part = piece // chunks
    out_grad = packed[2 * piece : 2 * piece + part, : chunks * width]
    out_grad = out_grad.reshape(part, chunks, width).transpose(2, 1, 0).reshape(width, piece)
    vec_grads = [share(packed[2 * piece + part + i], piece) for i in range(6)]
    hidden_grad = share(packed[2 * piece + part + 6], bias_hidden.shape[0])
    return (
        output,
        grad_tokens,
        attn_grads[:piece, :width],
        attn_grads[:piece, width : 2 * width],
        attn_grads[:piece, 2 * width :],
        out_grad,
        share(attn_grads[piece, :width], small),
        share(attn_grads[piece, 2 * width :], small),
        vec_grads[0],
        vec_grads[1],
        vec_grads[2],
        packed[:piece],
        hidden_grad,
        packed[piece : 2 * piece].T,
        vec_grads[3],
        vec_grads[4],
        vec_grads[5],
    )


def solution(mesh):
    placed = (
        P(("dp", "tensor"), None),
        P("dp", "tensor"),
        P("dp", "tensor"),
        P("dp", "tensor"),
        P("tensor", "dp"),
        P(("tensor", "dp")),
        P(("tensor", "dp")),
        P("dp"),
        P("dp"),
        P("dp"),
        P("dp", "tensor"),
        P(("tensor", "dp")),
        P("tensor", "dp"),
        P("dp"),
        P("dp"),
        P("dp"),
        P(("dp", "tensor"), None),
    )
    return jax.shard_map(
        on_device,
        mesh=mesh,
        in_specs=placed,
        out_specs=(
            P(("dp", "tensor"), None),
            P(("dp", "tensor"), None),
            P("dp", "tensor"),
            P("dp", "tensor"),
            P("dp", "tensor"),
            P("tensor", "dp"),
            P(("tensor", "dp")),
            P(("tensor", "dp")),
            P("dp"),
            P("dp"),
            P("dp"),
            P("dp", "tensor"),
            P(("tensor", "dp")),
            P("tensor", "dp"),
            P("dp"),
            P("dp"),
            P("dp"),
        ),
        check_vma=False,
    )
```

```python
import jax
import jax.numpy as jnp
from jax import lax
from jax.experimental import pallas as pl
from jax.experimental.pallas import tpu as pltpu
from jax.sharding import PartitionSpec as P

HD = 64
LEN = 2048
QB = 256
PAIR = 2 * HD
PAD = 16
F32 = jnp.float32
BF = jnp.bfloat16


def contract(left, right, left_dim, right_dim):
    return lax.dot_general(
        left, right, (((left_dim,), (right_dim,)), ((), ())), preferred_element_type=F32
    )


def one_head(pair, head):
    lane = lax.broadcasted_iota(jnp.int32, pair.shape, 1)
    keep = lane < HD if head == 0 else lane >= HD
    return jnp.where(keep, pair, jnp.zeros_like(pair))


CUTS = 4


def flipped(index, bit):
    size = 1 << bit
    return index + size - 2 * size * lax.rem(index // size, 2)


def bit_order(dps):
    count = dps.bit_length() - 1
    return tuple(range(1, count)) + (0,)


def greet(dps, tps):
    place, level = lax.axis_index("dp"), lax.axis_index("tensor")
    barrier = pltpu.get_barrier_semaphore()
    for bit in bit_order(dps):
        pl.semaphore_signal(barrier, inc=1, device_id={"dp": flipped(place, bit)})
    for step in range(1, tps):
        pl.semaphore_signal(barrier, inc=1, device_id={"tensor": lax.rem(level + step, tps)})
    pl.semaphore_wait(barrier, len(bit_order(dps)) + tps - 1)


def forward_kernel(
    dps,
    tps,
    tok_ref,
    pack_ref,
    mine_ref,
    rows_ref,
    packs_ref,
    qkv_ref,
    att_ref,
    lse_ref,
    cross_ref,
    gath_ref,
    weight_s,
    right_sem,
    left_sem,
    land_sem,
    pack_send,
    pack_land,
    local_sem,
    level_send,
    level_land,
    plane_send,
    plane_land,
    cross_send,
    cross_land,
):
    place, level = lax.axis_index("dp"), lax.axis_index("tensor")
    rows, model = tok_ref.shape
    piece = model // dps
    width = pack_ref.shape[1] // 3
    pairs = width // PAIR
    cut = rows // CUTS
    count = mine_ref.shape[0]
    middle_row = count // (2 * PAD) * PAD
    spans = (pl.ds(0, middle_row), pl.ds(middle_row, count - middle_row))
    bits = tuple(range(1, dps.bit_length() - 1))
    orders = (bits, bits[::-1])
    own = pltpu.make_async_copy(tok_ref, rows_ref.at[level], local_sem.at[0])
    own_pack = pltpu.make_async_copy(pack_ref, packs_ref.at[place], local_sem.at[1])
    own_block = pltpu.make_async_copy(mine_ref, gath_ref.at[place, level], local_sem.at[2])
    own.start()
    own_pack.start()
    own_block.start()
    greet(dps, tps)

    def hop(block, chunk, rightward, first=False):
        span = pl.ds(chunk * cut, cut)
        return pltpu.make_async_remote_copy(
            src_ref=tok_ref.at[span] if first else rows_ref.at[block, span],
            dst_ref=rows_ref.at[block, span],
            send_sem=(right_sem if rightward else left_sem).at[block, chunk],
            recv_sem=land_sem.at[block, chunk],
            device_id={"tensor": level + 1 if rightward else level - 1},
        )

    def to_level(step, half):
        return pltpu.make_async_remote_copy(
            src_ref=mine_ref.at[spans[half]],
            dst_ref=gath_ref.at[place, level, spans[half]],
            send_sem=level_send.at[step, half],
            recv_sem=level_land.at[step, half],
            device_id={"tensor": lax.rem(level + step, tps)},
        )

    def in_plane(block, step, half, bit, number, mine=False):
        at = lax.rem(level + step, tps)
        return pltpu.make_async_remote_copy(
            src_ref=mine_ref.at[spans[half]] if mine else gath_ref.at[block, at, spans[half]],
            dst_ref=gath_ref.at[block, at, spans[half]],
            send_sem=plane_send.at[number, step, half],
            recv_sem=plane_land.at[block, step, half],
            device_id={"dp": flipped(place, bit)},
        )

    def held(half, stage):
        blocks = [place]
        for bit in orders[half][:stage]:
            blocks = blocks + [flipped(block, bit) for block in blocks]
        return blocks

    def numbered(half):
        found, at = [], 0
        for stage in range(len(bits) + 1):
            for block in held(half, stage)[(1 << stage) // 2 if stage else 0 :]:
                targets = list(orders[half][stage:]) + [0]
                found.append((stage, block, [(bit, at + i) for i, bit in enumerate(targets)]))
                at += len(targets)
        return found

    tables = (numbered(0), numbered(1))

    def pass_on(step, stage):
        for half in range(2):
            for came, block, targets in tables[half]:
                if came != stage:
                    continue
                if stage:
                    in_plane(block, step, half, 0, 0).wait_recv()
                for bit, number in targets:
                    in_plane(block, step, half, bit, number, step == 0 and stage == 0).start()

    def level_in(step):
        back = tps - step
        for half in range(2):
            pltpu.make_async_remote_copy(
                src_ref=mine_ref.at[spans[half]],
                dst_ref=gath_ref.at[place, lax.rem(level + step, tps), spans[half]],
                send_sem=level_send.at[back, half],
                recv_sem=level_land.at[back, half],
                device_id={"tensor": lax.rem(level + back, tps)},
            ).wait_recv()

    for chunk in range(CUTS):

        @pl.when(level < tps - 1)
        def _():
            hop(level, chunk, True, True).start()

        @pl.when(level > 0)
        def _():
            hop(level, chunk, False, True).start()

    own_pack.wait()
    known = [place]
    for bit in bit_order(dps):
        copies = []
        for block in known:
            copies.append(
                pltpu.make_async_remote_copy(
                    src_ref=packs_ref.at[block],
                    dst_ref=packs_ref.at[block],
                    send_sem=pack_send.at[block],
                    recv_sem=pack_land.at[block],
                    device_id={"dp": flipped(place, bit)},
                )
            )
            copies[-1].start()
        for copy in copies:
            copy.wait_send()
        more = [flipped(block, bit) for block in known]
        for block in more:
            pltpu.make_async_remote_copy(
                src_ref=packs_ref.at[block],
                dst_ref=packs_ref.at[block],
                send_sem=pack_send.at[block],
                recv_sem=pack_land.at[block],
                device_id={"dp": flipped(place, bit)},
            ).wait_recv()
        known = known + more
    pass_on(0, 0)
    weight_s[...] = packs_ref[:, :piece].reshape(weight_s.shape)
    bias = jnp.sum(packs_ref[:, piece : piece + PAD].astype(F32), axis=0)[0:1]

    def project(block):
        qkv_ref[block] = (contract(rows_ref[block], weight_s[...], 1, 0) + bias).astype(BF)

    own.wait()
    project(level)
    for step in range(1, tps):
        for chunk in range(CUTS):

            @pl.when(level - step >= 0)
            def _():
                hop(level - step, chunk, True).wait_recv()

            @pl.when((level - step >= 0) & (level < tps - 1))
            def _():
                hop(level - step, chunk, True).start()

            @pl.when(level + step < tps)
            def _():
                hop(level + step, chunk, False).wait_recv()

            @pl.when((level + step < tps) & (level > 0))
            def _():
                hop(level + step, chunk, False).start()

        @pl.when(level - step >= 0)
        def _():
            project(level - step)

        @pl.when(level + step < tps)
        def _():
            project(level + step)

        if step == min(2, tps - 1):
            for other in range(1, tps):
                for half in range(2):
                    to_level(other, half).start()
        if step <= len(bits):
            pass_on(0, step)
    for stage in range(tps, len(bits) + 1):
        pass_on(0, stage)

    half_rows = rows // 2

    def cross(target, half):
        span = pl.ds(half * half_rows, half_rows)
        return pltpu.make_async_remote_copy(
            src_ref=att_ref.at[target, span],
            dst_ref=cross_ref.at[level, span],
            send_sem=cross_send.at[target, half],
            recv_sem=cross_land.at[level, half],
            device_id={"tensor": target},
        )

    turns = 2 * pairs * tps

    def attend(turn, carry):
        pair = lax.rem(turn, pairs)
        half = lax.rem(turn // pairs, 2)
        target = lax.rem(level + 1 + turn // (2 * pairs), tps)
        span = pl.ds(pl.multiple_of(half * half_rows, half_rows), half_rows)
        lanes = pl.ds(pl.multiple_of(pair * PAIR, PAIR), PAIR)
        query = qkv_ref[target, span, lanes] * jnp.asarray(0.125, BF)
        key = qkv_ref[:, :, pl.ds(pl.multiple_of(width + pair * PAIR, PAIR), PAIR)]
        value = qkv_ref[:, :, pl.ds(pl.multiple_of(2 * width + pair * PAIR, PAIR), PAIR)]
        key, value = key.reshape(tps * rows, PAIR), value.reshape(tps * rows, PAIR)
        total, columns = None, []
        for head in range(2):
            scores = contract(query, one_head(key, head), 1, 1)
            highest = jnp.max(scores, axis=1, keepdims=True)
            expons = jnp.exp(scores - highest)
            mass = jnp.sum(expons, axis=1, keepdims=True)
            part = contract(expons.astype(BF), one_head(value, head), 1, 0) / mass
            total = part if total is None else total + part
            columns.append(jnp.broadcast_to(highest + jnp.log(mass), (half_rows, PAIR)))
        att_ref[target, span, lanes] = total.astype(BF)
        where = pl.ds(pl.multiple_of(target * rows + half * half_rows, half_rows), half_rows)
        lse_ref[pair, :, where] = jnp.concatenate(
            [jnp.transpose(column)[:4] for column in columns], axis=0
        )

        @pl.when((pair == pairs - 1) & (turn < 2 * pairs * (tps - 1)))
        def _():
            cross(target, half).start()

        @pl.when(turn == turns // 2)
        def _():
            level_in(1)
            pass_on(1, 0)

        return carry

    lax.fori_loop(0, turns, attend, 0)
    own_cross = pltpu.make_async_copy(att_ref.at[level], cross_ref.at[level], local_sem.at[3])
    own_cross.start()
    for step in range(2, tps):
        level_in(step)
        pass_on(step, 0)
        for stage in range(1, len(bits) + 1):
            pass_on(step - 1, stage)
    for stage in range(1, len(bits) + 1):
        pass_on(tps - 1, stage)
    for step in range(1, tps):
        other = lax.rem(level + step, tps)
        for half in range(2):
            pltpu.make_async_remote_copy(
                src_ref=att_ref.at[level, pl.ds(half * half_rows, half_rows)],
                dst_ref=cross_ref.at[other, pl.ds(half * half_rows, half_rows)],
                send_sem=cross_send.at[other, half],
                recv_sem=cross_land.at[other, half],
                device_id={"tensor": other},
            ).wait_recv()
            cross(other, half).wait_send()
            to_level(step, half).wait_send()
    for step in range(tps):
        for half in range(2):
            for stage, block, targets in tables[half]:
                in_plane(flipped(block, 0), step, half, 0, 0).wait_recv()
                for bit, number in targets:
                    in_plane(block, step, half, bit, number).wait_send()
    own_block.wait()
    own_cross.wait()
    for step in range(tps):
        for chunk in range(CUTS):

            @pl.when((level - step >= 0) & (level < tps - 1))
            def _():
                hop(level - step, chunk, True, step == 0).wait_send()

            @pl.when((level + step < tps) & (level > 0))
            def _():
                hop(level + step, chunk, False, step == 0).wait_send()


def forward(tokens, pack, mine, dps, tps):
    rows, model = tokens.shape
    columns = pack.shape[1]
    width = columns // 3
    vmem = pl.BlockSpec(memory_space=pltpu.VMEM)
    hbm = pl.BlockSpec(memory_space=pl.ANY)
    dma = pltpu.SemaphoreType.DMA
    return pl.pallas_call(
        lambda *refs: forward_kernel(dps, tps, *refs),
        in_specs=[vmem, vmem, hbm],
        out_specs=[vmem] * 5 + [hbm] * 2,
        out_shape=[
            jax.ShapeDtypeStruct((tps, rows, model), BF),
            jax.ShapeDtypeStruct((dps,) + pack.shape, BF),
            jax.ShapeDtypeStruct((tps, rows, columns), BF),
            jax.ShapeDtypeStruct((tps, rows, width), BF),
            jax.ShapeDtypeStruct((width // PAIR, 8, tps * rows), F32),
            jax.ShapeDtypeStruct((tps, rows, width), BF),
            jax.ShapeDtypeStruct((dps, tps) + mine.shape, BF),
        ],
        scratch_shapes=[
            pltpu.VMEM((model, columns), BF),
            dma((tps, CUTS)),
            dma((tps, CUTS)),
            dma((tps, CUTS)),
            dma((dps,)),
            dma((dps,)),
            dma((4,)),
            dma((tps, 2)),
            dma((tps, 2)),
            dma((dps - 1, tps, 2)),
            dma((dps, tps, 2)),
            dma((tps, 2)),
            dma((tps, 2)),
        ],
        cost_estimate=pl.CostEstimate(
            flops=2 * tps * rows * model * columns, bytes_accessed=200 << 20, transcendentals=0
        ),
        compiler_params=pltpu.CompilerParams(
            vmem_limit_bytes=50 << 20, collective_id=1, has_side_effects=True
        ),
        name="forward",
    )(tokens, pack, mine)


def back_kernel(
    dps,
    tps,
    dq_ref,
    dk_ref,
    dv_ref,
    rows_ref,
    packs_ref,
    gsum_ref,
    tok_out,
    pack_out,
    weight_s,
    part_s,
    right_s,
    left_s,
    mine_s,
    theirs_s,
    right_send,
    right_land,
    left_send,
    left_land,
    pack_send,
    pack_land,
):
    place, level = lax.axis_index("dp"), lax.axis_index("tensor")
    rows, model = gsum_ref.shape
    piece = model // dps
    cut = rows // CUTS
    width = dq_ref.shape[1]
    greet(dps, tps)
    weight_s[...] = packs_ref[:, :piece].reshape(weight_s.shape)

    def rows_of(block):
        span = pl.ds(pl.multiple_of(block * rows, rows), rows)
        total = None
        for index, ref in enumerate((dq_ref, dk_ref, dv_ref)):
            weight = weight_s[:, index * width : (index + 1) * width]
            part = contract(ref[span], weight, 1, 1)
            total = part if total is None else total + part
        part_s[block] = total.astype(BF)

    def hop(block, chunk, rightward):
        span = pl.ds(chunk * cut, cut)
        land = right_s if rightward else left_s
        return pltpu.make_async_remote_copy(
            src_ref=part_s.at[block, span],
            dst_ref=land.at[block, span],
            send_sem=(right_send if rightward else left_send).at[block, chunk],
            recv_sem=(right_land if rightward else left_land).at[block, chunk],
            device_id={"tensor": level + 1 if rightward else level - 1},
        )

    def gather_in(block, chunk, rightward):
        hop(block, chunk, rightward).wait_recv()
        span = pl.ds(chunk * cut, cut)
        land = right_s if rightward else left_s
        part_s[block, span] = (
            part_s[block, span].astype(F32) + land[block, span].astype(F32)
        ).astype(BF)

    for step in range(tps - 1, 0, -1):

        @pl.when(level + step < tps)
        def _():
            rows_of(level + step)

        @pl.when((level + step < tps) & (level == 0))
        def _():
            for chunk in range(CUTS):
                hop(level + step, chunk, True).start()

        @pl.when(level - step >= 0)
        def _():
            rows_of(level - step)

        @pl.when((level - step >= 0) & (level == tps - 1))
        def _():
            for chunk in range(CUTS):
                hop(level - step, chunk, False).start()

    rows_of(level)
    model_rows = rows_ref.reshape(tps * rows, model)
    tail = jnp.concatenate(
        [jnp.sum(ref[...].astype(F32), axis=0, keepdims=True) for ref in (dq_ref, dk_ref, dv_ref)],
        axis=1,
    )
    for index, ref in enumerate((dq_ref, dk_ref, dv_ref)):
        grad = contract(model_rows[...], ref[...], 0, 0).astype(BF).reshape(dps, piece, width)
        mine_s[:, :piece, index * width : (index + 1) * width] = grad
    mine_s[:, piece:] = jnp.broadcast_to(tail.astype(BF)[None], (dps, PAD, 3 * width))

    def exchange(index, bit, other):
        return pltpu.make_async_remote_copy(
            src_ref=mine_s.at[other],
            dst_ref=theirs_s.at[index],
            send_sem=pack_send.at[index],
            recv_sem=pack_land.at[index],
            device_id={"dp": flipped(place, bit)},
        )

    order = bit_order(dps)[::-1]

    def kept(done):
        blocks = [place]
        for bit in order[done:][::-1]:
            blocks = blocks + [flipped(block, bit) for block in blocks]
        return blocks

    starts = []
    at = 0
    for done in range(len(order)):
        starts.append(at)
        at += dps >> (done + 1)

    def pack_start(done):
        for index, block in enumerate(kept(done + 1)):
            exchange(starts[done] + index, order[done], flipped(block, order[done])).start()

    def pack_finish(done):
        for index, block in enumerate(kept(done + 1)):
            exchange(starts[done] + index, order[done], block).wait()
            mine_s[block] = (
                mine_s[block].astype(F32) + theirs_s[starts[done] + index].astype(F32)
            ).astype(BF)

    pack_start(0)
    pack_done = 0
    for step in range(tps - 1, 0, -1):
        for chunk in range(CUTS):

            @pl.when((level > 0) & (level + step < tps))
            def _():
                gather_in(level + step, chunk, True)
                hop(level + step, chunk, True).start()

            @pl.when((level < tps - 1) & (level - step >= 0))
            def _():
                gather_in(level - step, chunk, False)
                hop(level - step, chunk, False).start()

        if pack_done < len(order):
            pack_finish(pack_done)
            pack_done += 1
            if pack_done < len(order):
                pack_start(pack_done)
    while pack_done < len(order):
        pack_finish(pack_done)
        pack_done += 1
        if pack_done < len(order):
            pack_start(pack_done)
    pack_out[...] = mine_s[place].astype(F32)
    for chunk in range(CUTS):

        @pl.when(level > 0)
        def _():
            hop(level, chunk, True).wait_recv()

        @pl.when(level < tps - 1)
        def _():
            hop(level, chunk, False).wait_recv()

    total = gsum_ref[...] + part_s[level].astype(F32)
    total = total + jnp.where(level > 0, right_s[level].astype(F32), 0.0)
    total = total + jnp.where(level < tps - 1, left_s[level].astype(F32), 0.0)
    tok_out[...] = total.astype(BF)
    for step in range(1, tps):
        for chunk in range(CUTS):

            @pl.when(level + step < tps)
            def _():
                hop(level + step, chunk, True).wait_send()

            @pl.when(level - step >= 0)
            def _():
                hop(level - step, chunk, False).wait_send()


def back(grads, rows_full, packs, grad_sum):
    rows, model = grad_sum.shape
    tps = rows_full.shape[0]
    dps, pack_rows, columns = packs.shape
    vmem = pl.BlockSpec(memory_space=pltpu.VMEM)
    return pl.pallas_call(
        lambda *refs: back_kernel(dps, tps, *refs),
        in_specs=[vmem] * 6,
        out_specs=[vmem] * 2,
        out_shape=[
            jax.ShapeDtypeStruct((rows, model), BF),
            jax.ShapeDtypeStruct((pack_rows, columns), F32),
        ],
        scratch_shapes=[
            pltpu.VMEM((model, columns), BF),
            pltpu.VMEM((tps, rows, model), BF),
            pltpu.VMEM((tps, rows, model), BF),
            pltpu.VMEM((tps, rows, model), BF),
            pltpu.VMEM(packs.shape, BF),
            pltpu.VMEM(packs.shape, BF),
        ]
        + [pltpu.SemaphoreType.DMA((tps, CUTS))] * 4
        + [pltpu.SemaphoreType.DMA((dps,))] * 2,
        cost_estimate=pl.CostEstimate(
            flops=4 * tps * rows * model * columns, bytes_accessed=200 << 20, transcendentals=0
        ),
        compiler_params=pltpu.CompilerParams(
            vmem_limit_bytes=56 << 20, collective_id=2, has_side_effects=True
        ),
        name="back",
    )(*grads, rows_full, packs, grad_sum)


def pack_kernel(hidden_ref, down_ref, out_ref, vec_ref, packed_ref):
    piece, wide = hidden_ref.shape
    width = out_ref.shape[0]
    chunks = min(wide // width, piece // PAD)
    part = piece // chunks
    packed_ref[:piece] = hidden_ref[...]
    packed_ref[piece : 2 * piece] = jnp.transpose(down_ref[...])
    turned = jnp.transpose(out_ref[...])
    for chunk in range(chunks):
        packed_ref[2 * piece : 2 * piece + part, chunk * width : (chunk + 1) * width] = turned[
            chunk * part : (chunk + 1) * part
        ]
    if chunks * width < wide:
        packed_ref[2 * piece : 2 * piece + part, chunks * width :] = jnp.zeros(
            (part, wide - chunks * width), BF
        )
    packed_ref[2 * piece + part :] = vec_ref[...]


def pack_weights(hidden, down, out, vec):
    piece, wide = hidden.shape
    chunks = min(wide // out.shape[0], piece // PAD)
    return pl.pallas_call(
        pack_kernel,
        out_shape=jax.ShapeDtypeStruct((2 * piece + piece // chunks + PAD, wide), BF),
        name="pack",
    )(hidden, down, out, vec)


def attend_backward_kernel(
    q_ref, k_ref, v_ref, grad_ref, out_ref, logsum_ref, dq_ref, dk_ref, dv_ref, dk_sum, dv_sum
):
    step = pl.program_id(1)
    query = q_ref[...] * jnp.asarray(0.125, BF)
    key, value, grad = k_ref[...], v_ref[...], grad_ref[...]
    products = jnp.transpose(grad.astype(F32) * out_ref[...].astype(F32))

    @pl.when(step == 0)
    def _():
        dk_sum[...] = jnp.zeros_like(dk_sum)
        dv_sum[...] = jnp.zeros_like(dv_sum)

    grad_query = None
    for head in range(2):
        key_head, value_head = one_head(key, head), one_head(value, head)
        inner = jnp.sum(products[HD * head : HD * head + HD], axis=0, keepdims=True)
        logsum = logsum_ref[0, 4 * head : 4 * head + 1, :]
        probs = jnp.exp(contract(key_head, query, 1, 1) - logsum)
        grad_probs = contract(value_head, grad, 1, 1)
        grad_scores = (probs * (grad_probs - inner)).astype(BF)
        dv_sum[...] += contract(probs.astype(BF), one_head(grad, head), 1, 0)
        dk_sum[...] += contract(grad_scores, one_head(query, head), 1, 0)
        part = contract(grad_scores, key_head, 0, 0)
        grad_query = part if grad_query is None else grad_query + part
    dq_ref[...] = (grad_query * 0.125).astype(BF)

    @pl.when(step == pl.num_programs(1) - 1)
    def _():
        dk_ref[...] = dk_sum[...].astype(BF)
        dv_ref[...] = dv_sum[...].astype(BF)


def attend_backward(qkv, grad, out, logsum):
    width = qkv.shape[1] // 3
    pairs = width // PAIR
    block = pl.BlockSpec((QB, PAIR), lambda i, j: (j, i))
    whole = pl.BlockSpec((LEN, PAIR), lambda i, j: (0, i))
    return pl.pallas_call(
        attend_backward_kernel,
        grid=(width // PAIR, LEN // QB),
        in_specs=[
            block,
            pl.BlockSpec((LEN, PAIR), lambda i, j: (0, i + pairs)),
            pl.BlockSpec((LEN, PAIR), lambda i, j: (0, i + 2 * pairs)),
            block,
            block,
            pl.BlockSpec((1, 8, QB), lambda i, j: (i, 0, j)),
        ],
        out_specs=[block, whole, whole],
        out_shape=[jax.ShapeDtypeStruct((LEN, width), BF)] * 3,
        scratch_shapes=[pltpu.VMEM((LEN, PAIR), F32)] * 2,
        cost_estimate=pl.CostEstimate(
            flops=40 * LEN * LEN * width, bytes_accessed=18 * LEN * width, transcendentals=0
        ),
        compiler_params=pltpu.CompilerParams(vmem_limit_bytes=40 << 20),
        name="attend_backward",
    )(qkv, qkv, qkv, grad, out, logsum)


def row_mean(values):
    return jnp.mean(values, axis=1, keepdims=True)


def column_sum(values):
    return jnp.sum(values, axis=0, keepdims=True)


def middle_kernel(
    sizes,
    att_ref,
    tok_ref,
    cot_ref,
    all_ref,
    feed_ref,
    out_ref,
    gsum_ref,
    gatt_ref,
    pack_ref,
    first_s,
    norm_s,
    down_s,
    inv_s,
    low_s,
    low_t,
    gdown_s,
    gdown_t,
    hidden_s,
    slope_s,
    stage_s,
    tail_s,
    extra_s,
    wout_s,
    vec_s,
    sems,
    extra_sem,
):
    dps, tps, piece, chunks = sizes
    step = pl.program_id(0)
    model = tok_ref.shape[1]
    feed_rows = 2 * piece
    part = piece // chunks
    width = att_ref.shape[2]

    def norm_parts(values):
        centered = values - row_mean(values)
        inverse = lax.rsqrt(row_mean(centered * centered) + 1e-05)
        return centered * inverse, inverse

    def norm_back(grad, scale, normed, inverse):
        scaled = grad * scale
        return inverse * (scaled - row_mean(scaled) - normed * row_mean(scaled * normed))

    def send(slot, block):
        return pltpu.make_async_copy(
            stage_s.at[slot], pack_ref.at[:, block, pl.ds(0, feed_rows)], sems.at[slot]
        )

    @pl.when(step == 0)
    def _():
        def fetch(t):
            return pltpu.make_async_copy(
                all_ref.at[:, t, pl.ds(feed_rows, part + PAD)], extra_s.at[t % 2], extra_sem.at[t % 2]
            )

        fetch(0).start()
        for t in range(tps):
            if t + 1 < tps:
                fetch(t + 1).start()
            fetch(t).wait()
            extra = extra_s.at[t % 2]
            placed = jnp.sum(extra[:, part:].astype(F32), axis=0)
            if t == 0:
                vec_s[0:8] = placed[0:8]
            vec_s[8 + t : 9 + t] = placed[6:7]
            turned = jnp.concatenate(
                [extra[:, :part, c * width : (c + 1) * width] for c in range(chunks)], axis=1
            )
            wout_s[t] = turned.reshape(model, width)
        branch = None
        for t in range(tps):
            term = contract(att_ref[t], wout_s[t], 1, 1)
            branch = term if branch is None else branch + term
        normed, inverse = norm_parts(tok_ref[...].astype(F32) + branch + vec_s[0:1])
        first = normed * vec_s[1:2] + vec_s[2:3]
        norm_s[...] = normed
        inv_s[...] = jnp.broadcast_to(inverse, inv_s.shape)
        first_s[...] = first
        low = first.astype(BF)
        low_s[...] = low
        low_t[...] = jnp.transpose(low)
        down_s[...] = jnp.zeros_like(down_s)

    @pl.when(step < tps)
    def _():
        weight = feed_ref[:, 0, :piece].reshape(model, -1)
        pre = contract(low_s[...], weight, 1, 0) + vec_s[pl.ds(8 + step, 1)]
        share = 0.5 + 0.5 * lax.erf(pre * 0.7071067811865476)
        hidden = (pre * share).astype(BF)
        hidden_s[step] = hidden
        slope_s[step] = (share + pre * (0.3989422804014327 * jnp.exp(-0.5 * pre * pre))).astype(BF)
        down_s[...] += contract(hidden, feed_ref[:, 0, piece:].reshape(model, -1), 1, 1)

    @pl.when(step == tps)
    def _():
        normed, inverse = norm_parts(first_s[...] + down_s[...] + vec_s[3:4])
        out_ref[...] = (normed * vec_s[4:5] + vec_s[5:6]).astype(BF)
        grad = cot_ref[...].astype(F32)
        tail_s[0:1] = column_sum(grad * normed)
        tail_s[1:2] = column_sum(grad)
        grad_mid = norm_back(grad, vec_s[4:5], normed, inverse)
        gsum_ref[...] = grad_mid
        tail_s[2:3] = column_sum(grad_mid)
        grad_down = grad_mid.astype(BF)
        gdown_s[...] = grad_down
        gdown_t[...] = jnp.transpose(grad_down)
        down_s[...] = jnp.zeros_like(down_s)

    @pl.when(step >= tps)
    def _():
        block = 2 * tps - 1 - step
        slot = lax.rem(step, 2)

        @pl.when(step >= tps + 2)
        def _():
            send(slot, block + 2).wait()

        grad_hidden = contract(gdown_s[...], feed_ref[:, 0, piece:].reshape(model, -1), 1, 0)
        grad_pre = grad_hidden * slope_s[block].astype(F32)
        grad_low = grad_pre.astype(BF)
        tail_s[pl.ds(8 + block, 1)] = column_sum(grad_low.astype(F32))
        down_s[...] += contract(grad_low, feed_ref[:, 0, :piece].reshape(model, -1), 1, 1)
        stage_s[slot, :, :piece] = (
            contract(low_t[...], grad_low, 1, 0).astype(BF).reshape(dps, piece, -1)
        )
        stage_s[slot, :, piece:] = (
            contract(gdown_t[...], hidden_s[block], 1, 0).astype(BF).reshape(dps, piece, -1)
        )
        send(slot, block).start()

    @pl.when(step == 2 * tps - 1)
    def _():
        grad = gsum_ref[...] + down_s[...]
        normed = norm_s[...]
        grad_scale, grad_shift = column_sum(grad * normed), column_sum(grad)
        grad_sum = norm_back(grad, vec_s[1:2], normed, inv_s[:, 0:1])
        gsum_ref[...] = grad_sum
        grad_bias = column_sum(grad_sum)
        low = grad_sum.astype(BF)
        low_t[...] = jnp.transpose(low)
        for t in range(tps):
            gatt_ref[t] = contract(low, wout_s[t], 1, 0).astype(BF)
        send(lax.rem(step + 1, 2), 1).wait()
        send(lax.rem(step, 2), 0).wait()
        six = jnp.concatenate(
            [grad_bias, grad_scale, grad_shift, tail_s[2:3], tail_s[0:1], tail_s[1:2]], axis=0
        )
        for t in range(tps):
            gout = contract(low_t[...], att_ref[t], 1, 0).reshape(dps, piece, width)
            wide = [gout[:, c * part : (c + 1) * part] for c in range(chunks)]
            if chunks * width < model:
                wide.append(jnp.zeros((dps, part, model - chunks * width), F32))
            stage_s[0, :, :part] = jnp.concatenate(wide, axis=2).astype(BF)
            rows = jnp.concatenate(
                [six, tail_s[8 + t : 9 + t], jnp.zeros((PAD - 7, model), F32)], axis=0
            ).astype(BF)
            stage_s[0, :, part : part + PAD] = jnp.broadcast_to(rows[None], (dps, PAD, model))
            copy = pltpu.make_async_copy(
                stage_s.at[0, :, pl.ds(0, part + PAD)],
                pack_ref.at[:, t, pl.ds(feed_rows, part + PAD)],
                sems.at[0],
            )
            copy.start()
            copy.wait()


def middle(att, tokens, cotangent, gathered):
    tps, rows, width = att.shape
    model = tokens.shape[1]
    dps, wide = gathered.shape[0], gathered.shape[3]
    piece = model // dps
    chunks = min(model // width, piece // PAD)
    pack_rows = 2 * piece + piece // chunks + PAD

    def fixed(array):
        rank = len(array.shape)
        return pl.BlockSpec(
            array.shape, lambda i: (0,) * rank, pipeline_mode=pl.Buffered(buffer_count=1)
        )

    def feed_at(i):
        return (0, jnp.minimum(i, 2 * tps - 1 - i), 0, 0)

    outs = [
        jax.ShapeDtypeStruct((rows, model), BF),
        jax.ShapeDtypeStruct((rows, model), F32),
        jax.ShapeDtypeStruct(att.shape, BF),
        jax.ShapeDtypeStruct((dps, tps, pack_rows, model), BF),
    ]
    return pl.pallas_call(
        lambda *refs: middle_kernel((dps, tps, piece, chunks), *refs),
        grid=(2 * tps,),
        in_specs=[fixed(a) for a in (att, tokens, cotangent)]
        + [
            pl.BlockSpec(memory_space=pl.ANY),
            pl.BlockSpec((dps, 1, 2 * piece, wide), feed_at),
        ],
        out_specs=[fixed(a) for a in outs[:3]] + [pl.BlockSpec(memory_space=pl.ANY)],
        out_shape=outs,
        scratch_shapes=[
            pltpu.VMEM((rows, model), F32),
            pltpu.VMEM((rows, model), F32),
            pltpu.VMEM((rows, model), F32),
            pltpu.VMEM((rows, 128), F32),
            pltpu.VMEM((rows, model), BF),
            pltpu.VMEM((model, rows), BF),
            pltpu.VMEM((rows, model), BF),
            pltpu.VMEM((model, rows), BF),
            pltpu.VMEM((tps, rows, wide), BF),
            pltpu.VMEM((tps, rows, wide), BF),
            pltpu.VMEM((2, dps, 2 * piece, model), BF),
            pltpu.VMEM((16, model), F32),
            pltpu.VMEM((2, dps, piece // chunks + PAD, wide), BF),
            pltpu.VMEM((tps, model, width), BF),
            pltpu.VMEM((16, model), F32),
            pltpu.SemaphoreType.DMA((2,)),
            pltpu.SemaphoreType.DMA((2,)),
        ],
        cost_estimate=pl.CostEstimate(
            flops=6 * rows * model * model * (2 * tps + 1),
            bytes_accessed=60 << 20,
            transcendentals=0,
        ),
        compiler_params=pltpu.CompilerParams(vmem_limit_bytes=62 << 20),
        name="middle",
    )(att, tokens, cotangent, gathered, gathered)


def on_device(
    tokens,
    weight_query,
    weight_key,
    weight_value,
    weight_out,
    bias_query,
    bias_value,
    bias_out,
    first_scale,
    first_shift,
    weight_hidden,
    bias_hidden,
    weight_down,
    bias_down,
    second_scale,
    second_shift,
    cotangent,
):
    dps, tps = lax.axis_size("dp"), lax.axis_size("tensor")
    rows, model = tokens.shape
    piece = weight_hidden.shape[0]
    width = weight_query.shape[1]
    small = bias_query.shape[0]

    place = lax.axis_index("dp")

    def placed(pieces, length):
        zeros = jnp.zeros((pieces.shape[0], length), BF)
        return lax.dynamic_update_slice_in_dim(zeros, pieces, place * pieces.shape[1], 1)

    vec_rows = placed(
        jnp.stack(
            [bias_out, first_scale, first_shift, bias_down, second_scale, second_shift, bias_hidden]
        ),
        model,
    )
    packed_weights = pack_weights(
        weight_hidden, weight_down, weight_out, jnp.pad(vec_rows, ((0, PAD - 7), (0, 0)))
    )
    bias_rows = placed(jnp.stack([bias_query, bias_value]), width)
    bias_row = jnp.concatenate([bias_rows[0:1], jnp.zeros((1, width), BF), bias_rows[1:2]], axis=1)
    attn_pack = jnp.concatenate(
        [
            jnp.concatenate([weight_query, weight_key, weight_value], axis=1),
            jnp.pad(bias_row, ((0, PAD - 1), (0, 0))),
        ],
        axis=0,
    )
    rows_full, packs, qkv, attended, logsum, crossed, gathered = forward(
        tokens, attn_pack, packed_weights, dps, tps
    )
    qkv = qkv.reshape(tps * rows, 3 * width)
    attended = attended.reshape(tps * rows, width)
    output, grad_sum, grad_cross, packed = middle(crossed, tokens, cotangent, gathered)
    grad_attended = lax.all_to_all(grad_cross, "tensor", 0, 0, tiled=False)
    grad_attended = grad_attended.reshape(tps * rows, width)
    packed = lax.psum_scatter(packed, "dp", scatter_dimension=0, tiled=False)
    grads = attend_backward(qkv, grad_attended, attended, logsum)
    packed, grads = lax.optimization_barrier((packed, grads))
    packed = lax.psum_scatter(packed, "tensor", scatter_dimension=0, tiled=False).astype(F32)
    grad_tokens, attn_grads = back(grads, rows_full, packs, grad_sum)

    def share(values, count):
        return lax.dynamic_slice_in_dim(values, place * count, count, 0)

    chunks = min(model // width, piece // PAD)
    part = piece // chunks
    out_grad = packed[2 * piece : 2 * piece + part, : chunks * width]
    out_grad = out_grad.reshape(part, chunks, width).transpose(2, 1, 0).reshape(width, piece)
    vec_grads = [share(packed[2 * piece + part + i], piece) for i in range(6)]
    hidden_grad = share(packed[2 * piece + part + 6], bias_hidden.shape[0])
    return (
        output,
        grad_tokens,
        attn_grads[:piece, :width],
        attn_grads[:piece, width : 2 * width],
        attn_grads[:piece, 2 * width :],
        out_grad,
        share(attn_grads[piece, :width], small),
        share(attn_grads[piece, 2 * width :], small),
        vec_grads[0],
        vec_grads[1],
        vec_grads[2],
        packed[:piece],
        hidden_grad,
        packed[piece : 2 * piece].T,
        vec_grads[3],
        vec_grads[4],
        vec_grads[5],
    )


def solution(mesh):
    placed = (
        P(("dp", "tensor"), None),
        P("dp", "tensor"),
        P("dp", "tensor"),
        P("dp", "tensor"),
        P("tensor", "dp"),
        P(("tensor", "dp")),
        P(("tensor", "dp")),
        P("dp"),
        P("dp"),
        P("dp"),
        P("dp", "tensor"),
        P(("tensor", "dp")),
        P("tensor", "dp"),
        P("dp"),
        P("dp"),
        P("dp"),
        P(("dp", "tensor"), None),
    )
    return jax.shard_map(
        on_device,
        mesh=mesh,
        in_specs=placed,
        out_specs=(
            P(("dp", "tensor"), None),
            P(("dp", "tensor"), None),
            P("dp", "tensor"),
            P("dp", "tensor"),
            P("dp", "tensor"),
            P("tensor", "dp"),
            P(("tensor", "dp")),
            P(("tensor", "dp")),
            P("dp"),
            P("dp"),
            P("dp"),
            P("dp", "tensor"),
            P(("tensor", "dp")),
            P("tensor", "dp"),
            P("dp"),
            P("dp"),
            P("dp"),
        ),
        check_vma=False,
    )
```

```python
import jax
import jax.numpy as jnp
from jax import lax
from jax.experimental import pallas as pl
from jax.experimental.pallas import tpu as pltpu
from jax.sharding import PartitionSpec as P

HD = 64
PAIR = 2 * HD
PAD = 16
F32 = jnp.float32
BF = jnp.bfloat16


def contract(left, right, left_dim, right_dim):
    return lax.dot_general(
        left, right, (((left_dim,), (right_dim,)), ((), ())), preferred_element_type=F32
    )


def one_head(pair, head):
    lane = lax.broadcasted_iota(jnp.int32, pair.shape, 1)
    keep = lane < HD if head == 0 else lane >= HD
    return jnp.where(keep, pair, jnp.zeros_like(pair))


CUTS = 4


def flipped(index, bit):
    size = 1 << bit
    return index + size - 2 * size * lax.rem(index // size, 2)


def bit_order(dps):
    count = dps.bit_length() - 1
    return tuple(range(1, count)) + (0,)


def greet(dps, tps):
    place, level = lax.axis_index("dp"), lax.axis_index("tensor")
    barrier = pltpu.get_barrier_semaphore()
    for bit in bit_order(dps):
        pl.semaphore_signal(barrier, inc=1, device_id={"dp": flipped(place, bit)})
    for step in range(1, tps):
        pl.semaphore_signal(barrier, inc=1, device_id={"tensor": lax.rem(level + step, tps)})
    pl.semaphore_wait(barrier, len(bit_order(dps)) + tps - 1)


def forward_kernel(
    dps,
    tps,
    tok_ref,
    pack_ref,
    mine_ref,
    rows_ref,
    packs_ref,
    qkv_ref,
    att_ref,
    lse_ref,
    cross_ref,
    gath_ref,
    weight_s,
    right_sem,
    left_sem,
    land_sem,
    pack_send,
    pack_land,
    local_sem,
    level_send,
    level_land,
    plane_send,
    plane_land,
    cross_send,
    cross_land,
):
    place, level = lax.axis_index("dp"), lax.axis_index("tensor")
    rows, model = tok_ref.shape
    piece = model // dps
    width = pack_ref.shape[1] // 3
    pairs = width // PAIR
    cut = rows // CUTS
    count = mine_ref.shape[0]
    middle_row = count // (2 * PAD) * PAD
    spans = (pl.ds(0, middle_row), pl.ds(middle_row, count - middle_row))
    bits = tuple(range(1, dps.bit_length() - 1))
    orders = (bits, bits[::-1])
    own = pltpu.make_async_copy(tok_ref, rows_ref.at[level], local_sem.at[0])
    own_pack = pltpu.make_async_copy(pack_ref, packs_ref.at[place], local_sem.at[1])
    own_block = pltpu.make_async_copy(mine_ref, gath_ref.at[place, level], local_sem.at[2])
    own.start()
    own_pack.start()
    own_block.start()
    greet(dps, tps)

    def hop(block, chunk, rightward, first=False):
        span = pl.ds(chunk * cut, cut)
        return pltpu.make_async_remote_copy(
            src_ref=tok_ref.at[span] if first else rows_ref.at[block, span],
            dst_ref=rows_ref.at[block, span],
            send_sem=(right_sem if rightward else left_sem).at[block, chunk],
            recv_sem=land_sem.at[block, chunk],
            device_id={"tensor": level + 1 if rightward else level - 1},
        )

    def to_level(step, half):
        return pltpu.make_async_remote_copy(
            src_ref=mine_ref.at[spans[half]],
            dst_ref=gath_ref.at[place, level, spans[half]],
            send_sem=level_send.at[step, half],
            recv_sem=level_land.at[step, half],
            device_id={"tensor": lax.rem(level + step, tps)},
        )

    def in_plane(block, step, half, bit, number, mine=False):
        at = lax.rem(level + step, tps)
        return pltpu.make_async_remote_copy(
            src_ref=mine_ref.at[spans[half]] if mine else gath_ref.at[block, at, spans[half]],
            dst_ref=gath_ref.at[block, at, spans[half]],
            send_sem=plane_send.at[number, step, half],
            recv_sem=plane_land.at[block, step, half],
            device_id={"dp": flipped(place, bit)},
        )

    def held(half, stage):
        blocks = [place]
        for bit in orders[half][:stage]:
            blocks = blocks + [flipped(block, bit) for block in blocks]
        return blocks

    def numbered(half):
        found, at = [], 0
        for stage in range(len(bits) + 1):
            for block in held(half, stage)[(1 << stage) // 2 if stage else 0 :]:
                targets = list(orders[half][stage:]) + [0]
                found.append((stage, block, [(bit, at + i) for i, bit in enumerate(targets)]))
                at += len(targets)
        return found

    tables = (numbered(0), numbered(1))

    def pass_on(step, stage):
        for half in range(2):
            for came, block, targets in tables[half]:
                if came != stage:
                    continue
                if stage:
                    in_plane(block, step, half, 0, 0).wait_recv()
                for bit, number in targets:
                    in_plane(block, step, half, bit, number, step == 0 and stage == 0).start()

    def level_in(step):
        back = tps - step
        for half in range(2):
            pltpu.make_async_remote_copy(
                src_ref=mine_ref.at[spans[half]],
                dst_ref=gath_ref.at[place, lax.rem(level + step, tps), spans[half]],
                send_sem=level_send.at[back, half],
                recv_sem=level_land.at[back, half],
                device_id={"tensor": lax.rem(level + back, tps)},
            ).wait_recv()

    for chunk in range(CUTS):

        @pl.when(level < tps - 1)
        def _():
            hop(level, chunk, True, True).start()

        @pl.when(level > 0)
        def _():
            hop(level, chunk, False, True).start()

    own_pack.wait()
    known = [place]
    for bit in bit_order(dps):
        copies = []
        for block in known:
            copies.append(
                pltpu.make_async_remote_copy(
                    src_ref=packs_ref.at[block],
                    dst_ref=packs_ref.at[block],
                    send_sem=pack_send.at[block],
                    recv_sem=pack_land.at[block],
                    device_id={"dp": flipped(place, bit)},
                )
            )
            copies[-1].start()
        for copy in copies:
            copy.wait_send()
        more = [flipped(block, bit) for block in known]
        for block in more:
            pltpu.make_async_remote_copy(
                src_ref=packs_ref.at[block],
                dst_ref=packs_ref.at[block],
                send_sem=pack_send.at[block],
                recv_sem=pack_land.at[block],
                device_id={"dp": flipped(place, bit)},
            ).wait_recv()
        known = known + more
    pass_on(0, 0)
    weight_s[...] = packs_ref[:, :piece].reshape(weight_s.shape)
    bias = jnp.sum(packs_ref[:, piece : piece + PAD].astype(F32), axis=0)[0:1]

    def project(block):
        qkv_ref[block] = (contract(rows_ref[block], weight_s[...], 1, 0) + bias).astype(BF)

    own.wait()
    project(level)
    for step in range(1, tps):
        for chunk in range(CUTS):

            @pl.when(level - step >= 0)
            def _():
                hop(level - step, chunk, True).wait_recv()

            @pl.when((level - step >= 0) & (level < tps - 1))
            def _():
                hop(level - step, chunk, True).start()

            @pl.when(level + step < tps)
            def _():
                hop(level + step, chunk, False).wait_recv()

            @pl.when((level + step < tps) & (level > 0))
            def _():
                hop(level + step, chunk, False).start()

        @pl.when(level - step >= 0)
        def _():
            project(level - step)

        @pl.when(level + step < tps)
        def _():
            project(level + step)

        if step == min(2, tps - 1):
            for other in range(1, tps):
                for half in range(2):
                    to_level(other, half).start()
        if step <= len(bits):
            pass_on(0, step)
    for stage in range(tps, len(bits) + 1):
        pass_on(0, stage)

    half_rows = rows // 2

    def cross(target, half):
        span = pl.ds(half * half_rows, half_rows)
        return pltpu.make_async_remote_copy(
            src_ref=att_ref.at[target, span],
            dst_ref=cross_ref.at[level, span],
            send_sem=cross_send.at[target, half],
            recv_sem=cross_land.at[level, half],
            device_id={"tensor": target},
        )

    turns = 2 * pairs * tps

    def attend(turn, carry):
        pair = lax.rem(turn, pairs)
        half = lax.rem(turn // pairs, 2)
        target = lax.rem(level + 1 + turn // (2 * pairs), tps)
        span = pl.ds(pl.multiple_of(half * half_rows, half_rows), half_rows)
        lanes = pl.ds(pl.multiple_of(pair * PAIR, PAIR), PAIR)
        query = qkv_ref[target, span, lanes] * jnp.asarray(0.125, BF)
        key = qkv_ref[:, :, pl.ds(pl.multiple_of(width + pair * PAIR, PAIR), PAIR)]
        value = qkv_ref[:, :, pl.ds(pl.multiple_of(2 * width + pair * PAIR, PAIR), PAIR)]
        key, value = key.reshape(tps * rows, PAIR), value.reshape(tps * rows, PAIR)
        total, columns = None, []
        for head in range(2):
            scores = contract(query, one_head(key, head), 1, 1)
            highest = jnp.max(scores, axis=1, keepdims=True)
            expons = jnp.exp(scores - highest)
            mass = jnp.sum(expons, axis=1, keepdims=True)
            part = contract(expons.astype(BF), one_head(value, head), 1, 0) / mass
            total = part if total is None else total + part
            columns.append(jnp.broadcast_to(highest + jnp.log(mass), (half_rows, PAIR)))
        att_ref[target, span, lanes] = total.astype(BF)
        where = pl.ds(pl.multiple_of(target * rows + half * half_rows, half_rows), half_rows)
        lse_ref[pair, :, where] = jnp.concatenate(
            [jnp.transpose(column)[:4] for column in columns], axis=0
        )

        @pl.when((pair == pairs - 1) & (turn < 2 * pairs * (tps - 1)))
        def _():
            cross(target, half).start()

        @pl.when(turn == turns // 2)
        def _():
            level_in(1)
            pass_on(1, 0)

        return carry

    lax.fori_loop(0, turns, attend, 0)
    own_cross = pltpu.make_async_copy(att_ref.at[level], cross_ref.at[level], local_sem.at[3])
    own_cross.start()
    for step in range(2, tps):
        level_in(step)
        pass_on(step, 0)
        for stage in range(1, len(bits) + 1):
            pass_on(step - 1, stage)
    for stage in range(1, len(bits) + 1):
        pass_on(tps - 1, stage)
    for step in range(1, tps):
        other = lax.rem(level + step, tps)
        for half in range(2):
            pltpu.make_async_remote_copy(
                src_ref=att_ref.at[level, pl.ds(half * half_rows, half_rows)],
                dst_ref=cross_ref.at[other, pl.ds(half * half_rows, half_rows)],
                send_sem=cross_send.at[other, half],
                recv_sem=cross_land.at[other, half],
                device_id={"tensor": other},
            ).wait_recv()
            cross(other, half).wait_send()
            to_level(step, half).wait_send()
    for step in range(tps):
        for half in range(2):
            for stage, block, targets in tables[half]:
                in_plane(flipped(block, 0), step, half, 0, 0).wait_recv()
                for bit, number in targets:
                    in_plane(block, step, half, bit, number).wait_send()
    own_block.wait()
    own_cross.wait()
    for step in range(tps):
        for chunk in range(CUTS):

            @pl.when((level - step >= 0) & (level < tps - 1))
            def _():
                hop(level - step, chunk, True, step == 0).wait_send()

            @pl.when((level + step < tps) & (level > 0))
            def _():
                hop(level + step, chunk, False, step == 0).wait_send()


def forward(tokens, pack, mine, dps, tps):
    rows, model = tokens.shape
    columns = pack.shape[1]
    width = columns // 3
    vmem = pl.BlockSpec(memory_space=pltpu.VMEM)
    hbm = pl.BlockSpec(memory_space=pl.ANY)
    dma = pltpu.SemaphoreType.DMA
    return pl.pallas_call(
        lambda *refs: forward_kernel(dps, tps, *refs),
        in_specs=[vmem, vmem, hbm],
        out_specs=[vmem] * 5 + [hbm] * 2,
        out_shape=[
            jax.ShapeDtypeStruct((tps, rows, model), BF),
            jax.ShapeDtypeStruct((dps,) + pack.shape, BF),
            jax.ShapeDtypeStruct((tps, rows, columns), BF),
            jax.ShapeDtypeStruct((tps, rows, width), BF),
            jax.ShapeDtypeStruct((width // PAIR, 8, tps * rows), F32),
            jax.ShapeDtypeStruct((tps, rows, width), BF),
            jax.ShapeDtypeStruct((dps, tps) + mine.shape, BF),
        ],
        scratch_shapes=[
            pltpu.VMEM((model, columns), BF),
            dma((tps, CUTS)),
            dma((tps, CUTS)),
            dma((tps, CUTS)),
            dma((dps,)),
            dma((dps,)),
            dma((4,)),
            dma((tps, 2)),
            dma((tps, 2)),
            dma((dps - 1, tps, 2)),
            dma((dps, tps, 2)),
            dma((tps, 2)),
            dma((tps, 2)),
        ],
        cost_estimate=pl.CostEstimate(
            flops=2 * tps * rows * model * columns, bytes_accessed=200 << 20, transcendentals=0
        ),
        compiler_params=pltpu.CompilerParams(
            vmem_limit_bytes=50 << 20, collective_id=1, has_side_effects=True
        ),
        name="forward",
    )(tokens, pack, mine)


def backward_kernel(
    dps,
    tps,
    scatter,
    cross_ref,
    packed_ref,
    qkv_ref,
    att_ref,
    lse_ref,
    rows_ref,
    packs_ref,
    gsum_ref,
    tok_out,
    pack_out,
    feed_out,
    grad_s,
    weight_s,
    dq_s,
    dk_s,
    dv_s,
    land_s,
    mine_s,
    theirs_s,
    gsum_s,
    kept_s,
    stage_s,
    one_a,
    one_b,
    two_a,
    two_b,
    level_s,
    local_sem,
    grad_send,
    grad_land,
    hop_send,
    hop_land,
    pack_send,
    pack_land,
    chip_send,
    chip_land,
    stage_sem,
    one_send,
    one_land,
    two_send,
    two_land,
    level_send,
    level_land,
):
    place, level = lax.axis_index("dp"), lax.axis_index("tensor")
    rows, model = gsum_ref.shape
    piece = model // dps
    width = att_ref.shape[2]
    pairs = width // PAIR
    cut = rows // CUTS
    half_rows = rows // 2
    count = packed_ref.shape[2]
    middle_row = count // (2 * PAD) * PAD
    spans = (pl.ds(0, middle_row), pl.ds(middle_row, count - middle_row))

    load_weight = pltpu.make_async_copy(
        packs_ref.at[:, pl.ds(0, piece)], weight_s, local_sem.at[0]
    )
    load_sum = pltpu.make_async_copy(gsum_ref, gsum_s, local_sem.at[1])
    own_grad = pltpu.make_async_copy(cross_ref.at[level], grad_s.at[level], local_sem.at[2])
    load_weight.start()
    load_sum.start()
    own_grad.start()
    greet(dps, tps)

    def cross(step):
        other = lax.rem(level + step, tps)
        return pltpu.make_async_remote_copy(
            src_ref=cross_ref.at[other],
            dst_ref=grad_s.at[level],
            send_sem=grad_send.at[other],
            recv_sem=grad_land.at[level],
            device_id={"tensor": other},
        )

    def crossed(other):
        return pltpu.make_async_remote_copy(
            src_ref=cross_ref.at[other],
            dst_ref=grad_s.at[other],
            send_sem=grad_send.at[other],
            recv_sem=grad_land.at[other],
            device_id={"tensor": other},
        )

    for step in range(1, tps):
        cross(step).start()

    def block_of(kind):
        block = place
        if kind in (0, 2):
            block = flipped(block, 1)
        if kind in (0, 1):
            block = flipped(block, 2)
        return block

    def level_of(turn):
        return lax.rem(level + 1 + turn, tps)

    def chip(kind, turn):
        return pltpu.make_async_remote_copy(
            src_ref=packed_ref.at[flipped(block_of(kind), 0), level_of(turn)],
            dst_ref=kept_s.at[turn * 4 + kind],
            send_sem=chip_send.at[turn * 4 + kind],
            recv_sem=chip_land.at[turn * 4 + kind],
            device_id={"dp": flipped(place, 0)},
        )

    def load(kind, turn, slot):
        return pltpu.make_async_copy(
            packed_ref.at[block_of(kind), level_of(turn)], stage_s.at[slot], stage_sem.at[slot]
        )

    def plane_one(kind, turn, half):
        bit = 2 - half
        target = one_b if half else one_a
        at = turn * 2 + (0 if kind == 0 else 1)
        return pltpu.make_async_remote_copy(
            src_ref=kept_s.at[turn * 4 + kind, spans[half]],
            dst_ref=target.at[at],
            send_sem=one_send.at[at, half],
            recv_sem=one_land.at[at, half],
            device_id={"dp": flipped(place, bit)},
        )

    def plane_two(turn, half):
        bit = 1 + half
        target = two_b if half else two_a
        return pltpu.make_async_remote_copy(
            src_ref=kept_s.at[turn * 4 + 2 - half, spans[half]],
            dst_ref=target.at[turn],
            send_sem=two_send.at[turn, half],
            recv_sem=two_land.at[turn, half],
            device_id={"dp": flipped(place, bit)},
        )

    def over_z(turn):
        return pltpu.make_async_remote_copy(
            src_ref=kept_s.at[turn * 4 + 3],
            dst_ref=level_s.at[turn],
            send_sem=level_send.at[turn],
            recv_sem=level_land.at[turn],
            device_id={"tensor": level_of(turn)},
        )

    def add_to(slot, half, source):
        kept_s[slot, spans[half]] = (
            kept_s[slot, spans[half]].astype(F32) + source.astype(F32)
        ).astype(BF)

    def chip_in(kind, turn):
        slot = kind % 2
        load(kind, turn, slot).wait()
        chip(kind, turn).wait_recv()
        at = turn * 4 + kind
        kept_s[at] = (kept_s[at].astype(F32) + stage_s[slot].astype(F32)).astype(BF)
        if kind in (0, 1):
            plane_one(kind, turn, 0).start()
        if kind in (0, 2):
            plane_one(kind, turn, 1).start()

    def one_in(turn):
        plane_one(0, turn, 0).wait_recv()
        add_to(turn * 4 + 2, 0, one_a[turn * 2])
        plane_two(turn, 0).start()
        plane_one(0, turn, 1).wait_recv()
        add_to(turn * 4 + 1, 1, one_b[turn * 2])
        plane_two(turn, 1).start()
        plane_one(1, turn, 0).wait_recv()
        add_to(turn * 4 + 3, 0, one_a[turn * 2 + 1])
        plane_one(2, turn, 1).wait_recv()
        add_to(turn * 4 + 3, 1, one_b[turn * 2 + 1])

    def two_in(turn):
        plane_two(turn, 0).wait_recv()
        add_to(turn * 4 + 3, 0, two_a[turn])
        plane_two(turn, 1).wait_recv()
        add_to(turn * 4 + 3, 1, two_b[turn])
        if turn < tps - 1:
            over_z(turn).start()

    if scatter:
        load(0, 0, 0).start()
        for turn in range(tps):
            for kind in range(4):
                chip(kind, turn).start()

    dk_s[...] = jnp.zeros_like(dk_s)
    dv_s[...] = jnp.zeros_like(dv_s)
    own_grad.wait()

    def attend(turn, carry):
        pair = lax.rem(turn, pairs)
        half = lax.rem(turn // pairs, 2)
        step = turn // (2 * pairs)
        target = lax.rem(level + step, tps)

        @pl.when((lax.rem(turn, 2 * pairs) == 0) & (step > 0))
        def _():
            crossed(target).wait_recv()

        span = pl.ds(pl.multiple_of(half * half_rows, half_rows), half_rows)
        lanes = pl.ds(pl.multiple_of(pair * PAIR, PAIR), PAIR)
        query = qkv_ref[target, span, lanes] * jnp.asarray(0.125, BF)
        key = qkv_ref[:, :, pl.ds(pl.multiple_of(width + pair * PAIR, PAIR), PAIR)]
        value = qkv_ref[:, :, pl.ds(pl.multiple_of(2 * width + pair * PAIR, PAIR), PAIR)]
        key, value = key.reshape(tps * rows, PAIR), value.reshape(tps * rows, PAIR)
        grad = grad_s[target, span, lanes]
        products = jnp.transpose(grad.astype(F32) * att_ref[target, span, lanes].astype(F32))
        where = pl.ds(pl.multiple_of(target * rows + half * half_rows, half_rows), half_rows)
        logsums = lse_ref[pair, :, where]
        grad_query = None
        for head in range(2):
            key_head, value_head = one_head(key, head), one_head(value, head)
            inner = jnp.sum(products[HD * head : HD * head + HD], axis=0, keepdims=True)
            logsum = logsums[4 * head : 4 * head + 1]
            probs = jnp.exp(contract(key_head, query, 1, 1) - logsum)
            grad_probs = contract(value_head, grad, 1, 1)
            grad_scores = (probs * (grad_probs - inner)).astype(BF)
            dv_s[:, lanes] += contract(probs.astype(BF), one_head(grad, head), 1, 0)
            dk_s[:, lanes] += contract(grad_scores, one_head(query, head), 1, 0)
            part = contract(grad_scores, key_head, 0, 0)
            grad_query = part if grad_query is None else grad_query + part
        dq_s[where, lanes] = (grad_query * 0.125).astype(BF)

        if scatter:
            for kind in range(4):

                @pl.when(lax.rem(turn, 4) == kind)
                def _():
                    if kind < 3:
                        load(kind + 1, turn // 4, (kind + 1) % 2).start()
                    else:

                        @pl.when(turn // 4 < tps - 1)
                        def _():
                            load(0, turn // 4 + 1, 0).start()

                    chip_in(kind, turn // 4)

            @pl.when(turn == 9)
            def _():
                one_in(0)

            @pl.when(turn == 13)
            def _():
                two_in(0)

            @pl.when(turn == 15)
            def _():
                one_in(1)

        return carry

    lax.fori_loop(0, 2 * pairs * tps, attend, 0)
    load_weight.wait()
    refs = (dq_s, dk_s, dv_s)

    def rows_of(block):
        span = pl.ds(pl.multiple_of(block * rows, rows), rows)
        total = None
        for index, ref in enumerate(refs):
            weight = weight_s[:, :, index * width : (index + 1) * width].reshape(model, width)
            part = contract(ref[span].astype(BF), weight, 1, 1)
            total = part if total is None else total + part
        return total

    def hop(block, chunk, rightward):
        slot = block + 1 if rightward else block
        span = pl.ds(chunk * cut, cut)
        return pltpu.make_async_remote_copy(
            src_ref=land_s.at[slot, span],
            dst_ref=land_s.at[slot, span],
            send_sem=hop_send.at[slot, chunk],
            recv_sem=hop_land.at[slot, chunk],
            device_id={"tensor": level + 1 if rightward else level - 1},
        )

    def begin(block, rightward):
        land_s[block + 1 if rightward else block] = rows_of(block).astype(BF)
        for chunk in range(CUTS):
            hop(block, chunk, rightward).start()

    def carry_on(block, rightward):
        slot = block + 1 if rightward else block
        own = rows_of(block)
        for chunk in range(CUTS):
            span = pl.ds(chunk * cut, cut)
            hop(block, chunk, rightward).wait_recv()
            land_s[slot, span] = (
                land_s[slot, span].astype(F32) + own[chunk * cut : (chunk + 1) * cut]
            ).astype(BF)
            hop(block, chunk, rightward).start()

    for step in range(tps - 1, 0, -1):

        @pl.when((level + step < tps) & (level == 0))
        def _():
            begin(level + step, True)

        @pl.when((level - step >= 0) & (level == tps - 1))
        def _():
            begin(level - step, False)

    if scatter:
        two_in(1)
    tail = jnp.concatenate(
        [jnp.sum(ref[...].astype(BF).astype(F32), axis=0, keepdims=True) for ref in refs], axis=1
    )
    tokens = rows_ref.reshape(tps * rows, model)
    for index, ref in enumerate(refs):
        grad = contract(tokens[...], ref[...].astype(BF), 0, 0).astype(BF)
        mine_s[:, :piece, index * width : (index + 1) * width] = grad.reshape(dps, piece, width)
    mine_s[:, piece:] = jnp.broadcast_to(tail.astype(BF)[None], (dps, PAD, 3 * width))

    def exchange(index, bit, other):
        return pltpu.make_async_remote_copy(
            src_ref=mine_s.at[other],
            dst_ref=theirs_s.at[index],
            send_sem=pack_send.at[index],
            recv_sem=pack_land.at[index],
            device_id={"dp": flipped(place, bit)},
        )

    order = bit_order(dps)[::-1]

    def kept(done):
        blocks = [place]
        for bit in order[done:][::-1]:
            blocks = blocks + [flipped(block, bit) for block in blocks]
        return blocks

    starts, at = [], 0
    for done in range(len(order)):
        starts.append(at)
        at += dps >> (done + 1)

    def pack_start(done):
        for index, block in enumerate(kept(done + 1)):
            exchange(starts[done] + index, order[done], flipped(block, order[done])).start()

    def pack_finish(done):
        for index, block in enumerate(kept(done + 1)):
            exchange(starts[done] + index, order[done], block).wait()
            mine_s[block] = (
                mine_s[block].astype(F32) + theirs_s[starts[done] + index].astype(F32)
            ).astype(BF)

    pack_start(0)
    for turn in range(max(tps - 1, len(order))):
        step = tps - 1 - turn
        if scatter and turn == 0:
            one_in(2)
        if step > 0:

            @pl.when((level > 0) & (level + step < tps))
            def _():
                carry_on(level + step, True)

            @pl.when((level < tps - 1) & (level - step >= 0))
            def _():
                carry_on(level - step, False)

        if turn < len(order):
            pack_finish(turn)
            if turn + 1 < len(order):
                pack_start(turn + 1)
        if scatter and turn == 0:
            two_in(2)
            one_in(3)
        if scatter and turn == 1:
            two_in(3)
    pack_out[...] = mine_s[place].astype(F32)
    own = rows_of(level)
    load_sum.wait()
    if scatter:
        total = kept_s[(tps - 1) * 4 + 3].astype(F32)
        for turn in range(tps - 1):
            over_z(turn).wait_recv()
            total = total + level_s[turn].astype(F32)
        feed_out[...] = total
    for chunk in range(CUTS):

        @pl.when(level > 0)
        def _():
            hop(level, chunk, True).wait_recv()

        @pl.when(level < tps - 1)
        def _():
            hop(level, chunk, False).wait_recv()

    total = gsum_s[...] + own
    total = total + jnp.where(level > 0, land_s[level + 1].astype(F32), 0.0)
    total = total + jnp.where(level < tps - 1, land_s[level].astype(F32), 0.0)
    tok_out[...] = total.astype(BF)
    for step in range(1, tps):
        cross(step).wait_send()
        for chunk in range(CUTS):

            @pl.when(level + step < tps)
            def _():
                hop(level + step, chunk, True).wait_send()

            @pl.when(level - step >= 0)
            def _():
                hop(level - step, chunk, False).wait_send()

    if scatter:
        for turn in range(tps):
            for kind in range(4):
                chip(kind, turn).wait_send()
            plane_one(0, turn, 0).wait_send()
            plane_one(1, turn, 0).wait_send()
            plane_one(0, turn, 1).wait_send()
            plane_one(2, turn, 1).wait_send()
            plane_two(turn, 0).wait_send()
            plane_two(turn, 1).wait_send()
            if turn < tps - 1:
                over_z(turn).wait_send()
    else:
        feed_out[...] = jnp.zeros_like(feed_out)


def backward(grad_cross, packed, qkv, attended, logsum, rows_full, packs, grad_sum, scatter):
    rows, model = grad_sum.shape
    tps = rows_full.shape[0]
    dps, pack_rows, columns = packs.shape
    width = columns // 3
    count = packed.shape[2]
    middle_row = count // (2 * PAD) * PAD
    vmem = pl.BlockSpec(memory_space=pltpu.VMEM)
    hbm = pl.BlockSpec(memory_space=pl.ANY)
    dma = pltpu.SemaphoreType.DMA
    slots = 4 * tps if scatter else 1

    def buffer(*shape):
        return pltpu.VMEM(shape if scatter else (1, 16, model), BF)

    return pl.pallas_call(
        lambda *refs: backward_kernel(dps, tps, scatter, *refs),
        in_specs=[hbm, hbm, vmem, vmem, vmem, vmem, hbm, hbm],
        out_specs=[vmem] * 3,
        out_shape=[
            jax.ShapeDtypeStruct((rows, model), BF),
            jax.ShapeDtypeStruct((pack_rows, columns), F32),
            jax.ShapeDtypeStruct((count, model), F32),
        ],
        scratch_shapes=[
            pltpu.VMEM((tps, rows, width), BF),
            pltpu.VMEM((dps, model // dps, columns), BF),
            pltpu.VMEM((tps * rows, width), BF),
            pltpu.VMEM((tps * rows, width), F32),
            pltpu.VMEM((tps * rows, width), F32),
            pltpu.VMEM((tps + 1, rows, model), BF),
            pltpu.VMEM(packs.shape, BF),
            pltpu.VMEM(packs.shape, BF),
            pltpu.VMEM((rows, model), F32),
            buffer(slots, count, model),
            buffer(2, count, model),
            buffer(2 * tps, middle_row, model),
            buffer(2 * tps, count - middle_row, model),
            buffer(tps, middle_row, model),
            buffer(tps, count - middle_row, model),
            buffer(tps - 1, count, model),
            dma((3,)),
            dma((tps,)),
            dma((tps,)),
            dma((tps + 1, CUTS)),
            dma((tps + 1, CUTS)),
            dma((dps,)),
            dma((dps,)),
            dma((slots,)),
            dma((slots,)),
            dma((2,)),
            dma((2 * tps, 2)),
            dma((2 * tps, 2)),
            dma((tps, 2)),
            dma((tps, 2)),
            dma((tps - 1,)),
            dma((tps - 1,)),
        ],
        cost_estimate=pl.CostEstimate(
            flops=4 * tps * rows * model * columns, bytes_accessed=200 << 20, transcendentals=0
        ),
        compiler_params=pltpu.CompilerParams(
            vmem_limit_bytes=63 << 20, collective_id=2, has_side_effects=True
        ),
        name="backward",
    )(grad_cross, packed, qkv, attended, logsum, rows_full, packs, grad_sum)


def pack_kernel(hidden_ref, down_ref, out_ref, vec_ref, packed_ref):
    piece, wide = hidden_ref.shape
    width = out_ref.shape[0]
    chunks = min(wide // width, piece // PAD)
    part = piece // chunks
    packed_ref[:piece] = hidden_ref[...]
    packed_ref[piece : 2 * piece] = jnp.transpose(down_ref[...])
    turned = jnp.transpose(out_ref[...])
    for chunk in range(chunks):
        packed_ref[2 * piece : 2 * piece + part, chunk * width : (chunk + 1) * width] = turned[
            chunk * part : (chunk + 1) * part
        ]
    if chunks * width < wide:
        packed_ref[2 * piece : 2 * piece + part, chunks * width :] = jnp.zeros(
            (part, wide - chunks * width), BF
        )
    packed_ref[2 * piece + part :] = vec_ref[...]


def pack_weights(hidden, down, out, vec):
    piece, wide = hidden.shape
    chunks = min(wide // out.shape[0], piece // PAD)
    return pl.pallas_call(
        pack_kernel,
        out_shape=jax.ShapeDtypeStruct((2 * piece + piece // chunks + PAD, wide), BF),
        name="pack",
    )(hidden, down, out, vec)


def row_mean(values):
    return jnp.mean(values, axis=1, keepdims=True)


def column_sum(values):
    return jnp.sum(values, axis=0, keepdims=True)


def middle_kernel(
    sizes,
    att_ref,
    tok_ref,
    cot_ref,
    all_ref,
    feed_ref,
    out_ref,
    gsum_ref,
    gatt_ref,
    pack_ref,
    first_s,
    norm_s,
    down_s,
    inv_s,
    low_s,
    low_t,
    gdown_s,
    gdown_t,
    hidden_s,
    slope_s,
    stage_s,
    tail_s,
    extra_s,
    wout_s,
    vec_s,
    sems,
    extra_sem,
):
    dps, tps, piece, chunks = sizes
    step = pl.program_id(0)
    model = tok_ref.shape[1]
    feed_rows = 2 * piece
    part = piece // chunks
    width = att_ref.shape[2]

    def norm_parts(values):
        centered = values - row_mean(values)
        inverse = lax.rsqrt(row_mean(centered * centered) + 1e-05)
        return centered * inverse, inverse

    def norm_back(grad, scale, normed, inverse):
        scaled = grad * scale
        return inverse * (scaled - row_mean(scaled) - normed * row_mean(scaled * normed))

    def send(slot, block):
        return pltpu.make_async_copy(
            stage_s.at[slot], pack_ref.at[:, block, pl.ds(0, feed_rows)], sems.at[slot]
        )

    @pl.when(step == 0)
    def _():
        def fetch(t):
            return pltpu.make_async_copy(
                all_ref.at[:, t, pl.ds(feed_rows, part + PAD)], extra_s.at[t % 2], extra_sem.at[t % 2]
            )

        fetch(0).start()
        for t in range(tps):
            if t + 1 < tps:
                fetch(t + 1).start()
            fetch(t).wait()
            extra = extra_s.at[t % 2]
            placed = jnp.sum(extra[:, part:].astype(F32), axis=0)
            if t == 0:
                vec_s[0:8] = placed[0:8]
            vec_s[8 + t : 9 + t] = placed[6:7]
            turned = jnp.concatenate(
                [extra[:, :part, c * width : (c + 1) * width] for c in range(chunks)], axis=1
            )
            wout_s[t] = turned.reshape(model, width)
        branch = None
        for t in range(tps):
            term = contract(att_ref[t], wout_s[t], 1, 1)
            branch = term if branch is None else branch + term
        normed, inverse = norm_parts(tok_ref[...].astype(F32) + branch + vec_s[0:1])
        first = normed * vec_s[1:2] + vec_s[2:3]
        norm_s[...] = normed
        inv_s[...] = jnp.broadcast_to(inverse, inv_s.shape)
        first_s[...] = first
        low = first.astype(BF)
        low_s[...] = low
        low_t[...] = jnp.transpose(low)
        down_s[...] = jnp.zeros_like(down_s)

    @pl.when(step < tps)
    def _():
        weight = feed_ref[:, 0, :piece].reshape(model, -1)
        pre = contract(low_s[...], weight, 1, 0) + vec_s[pl.ds(8 + step, 1)]
        share = 0.5 + 0.5 * lax.erf(pre * 0.7071067811865476)
        hidden = (pre * share).astype(BF)
        hidden_s[step] = hidden
        slope_s[step] = (share + pre * (0.3989422804014327 * jnp.exp(-0.5 * pre * pre))).astype(BF)
        down_s[...] += contract(hidden, feed_ref[:, 0, piece:].reshape(model, -1), 1, 1)

    @pl.when(step == tps)
    def _():
        normed, inverse = norm_parts(first_s[...] + down_s[...] + vec_s[3:4])
        out_ref[...] = (normed * vec_s[4:5] + vec_s[5:6]).astype(BF)
        grad = cot_ref[...].astype(F32)
        tail_s[0:1] = column_sum(grad * normed)
        tail_s[1:2] = column_sum(grad)
        grad_mid = norm_back(grad, vec_s[4:5], normed, inverse)
        gsum_ref[...] = grad_mid
        tail_s[2:3] = column_sum(grad_mid)
        grad_down = grad_mid.astype(BF)
        gdown_s[...] = grad_down
        gdown_t[...] = jnp.transpose(grad_down)
        down_s[...] = jnp.zeros_like(down_s)

    @pl.when(step >= tps)
    def _():
        block = 2 * tps - 1 - step
        slot = lax.rem(step, 2)

        @pl.when(step >= tps + 2)
        def _():
            send(slot, block + 2).wait()

        grad_hidden = contract(gdown_s[...], feed_ref[:, 0, piece:].reshape(model, -1), 1, 0)
        grad_pre = grad_hidden * slope_s[block].astype(F32)
        grad_low = grad_pre.astype(BF)
        tail_s[pl.ds(8 + block, 1)] = column_sum(grad_low.astype(F32))
        down_s[...] += contract(grad_low, feed_ref[:, 0, :piece].reshape(model, -1), 1, 1)
        stage_s[slot, :, :piece] = (
            contract(low_t[...], grad_low, 1, 0).astype(BF).reshape(dps, piece, -1)
        )
        stage_s[slot, :, piece:] = (
            contract(gdown_t[...], hidden_s[block], 1, 0).astype(BF).reshape(dps, piece, -1)
        )
        send(slot, block).start()

    @pl.when(step == 2 * tps - 1)
    def _():
        grad = gsum_ref[...] + down_s[...]
        normed = norm_s[...]
        grad_scale, grad_shift = column_sum(grad * normed), column_sum(grad)
        grad_sum = norm_back(grad, vec_s[1:2], normed, inv_s[:, 0:1])
        gsum_ref[...] = grad_sum
        grad_bias = column_sum(grad_sum)
        low = grad_sum.astype(BF)
        low_t[...] = jnp.transpose(low)
        for t in range(tps):
            gatt_ref[t] = contract(low, wout_s[t], 1, 0).astype(BF)
        send(lax.rem(step + 1, 2), 1).wait()
        send(lax.rem(step, 2), 0).wait()
        six = jnp.concatenate(
            [grad_bias, grad_scale, grad_shift, tail_s[2:3], tail_s[0:1], tail_s[1:2]], axis=0
        )
        for t in range(tps):
            gout = contract(low_t[...], att_ref[t], 1, 0).reshape(dps, piece, width)
            wide = [gout[:, c * part : (c + 1) * part] for c in range(chunks)]
            if chunks * width < model:
                wide.append(jnp.zeros((dps, part, model - chunks * width), F32))
            stage_s[0, :, :part] = jnp.concatenate(wide, axis=2).astype(BF)
            rows = jnp.concatenate(
                [six, tail_s[8 + t : 9 + t], jnp.zeros((PAD - 7, model), F32)], axis=0
            ).astype(BF)
            stage_s[0, :, part : part + PAD] = jnp.broadcast_to(rows[None], (dps, PAD, model))
            copy = pltpu.make_async_copy(
                stage_s.at[0, :, pl.ds(0, part + PAD)],
                pack_ref.at[:, t, pl.ds(feed_rows, part + PAD)],
                sems.at[0],
            )
            copy.start()
            copy.wait()


def middle(att, tokens, cotangent, gathered):
    tps, rows, width = att.shape
    model = tokens.shape[1]
    dps, wide = gathered.shape[0], gathered.shape[3]
    piece = model // dps
    chunks = min(model // width, piece // PAD)
    pack_rows = 2 * piece + piece // chunks + PAD

    def fixed(array):
        rank = len(array.shape)
        return pl.BlockSpec(
            array.shape, lambda i: (0,) * rank, pipeline_mode=pl.Buffered(buffer_count=1)
        )

    def feed_at(i):
        return (0, jnp.minimum(i, 2 * tps - 1 - i), 0, 0)

    outs = [
        jax.ShapeDtypeStruct((rows, model), BF),
        jax.ShapeDtypeStruct((rows, model), F32),
        jax.ShapeDtypeStruct(att.shape, BF),
        jax.ShapeDtypeStruct((dps, tps, pack_rows, model), BF),
    ]
    return pl.pallas_call(
        lambda *refs: middle_kernel((dps, tps, piece, chunks), *refs),
        grid=(2 * tps,),
        in_specs=[fixed(a) for a in (att, tokens, cotangent)]
        + [
            pl.BlockSpec(memory_space=pl.ANY),
            pl.BlockSpec((dps, 1, 2 * piece, wide), feed_at),
        ],
        out_specs=[fixed(a) for a in outs[:3]] + [pl.BlockSpec(memory_space=pl.ANY)],
        out_shape=outs,
        scratch_shapes=[
            pltpu.VMEM((rows, model), F32),
            pltpu.VMEM((rows, model), F32),
            pltpu.VMEM((rows, model), F32),
            pltpu.VMEM((rows, 128), F32),
            pltpu.VMEM((rows, model), BF),
            pltpu.VMEM((model, rows), BF),
            pltpu.VMEM((rows, model), BF),
            pltpu.VMEM((model, rows), BF),
            pltpu.VMEM((tps, rows, wide), BF),
            pltpu.VMEM((tps, rows, wide), BF),
            pltpu.VMEM((2, dps, 2 * piece, model), BF),
            pltpu.VMEM((16, model), F32),
            pltpu.VMEM((2, dps, piece // chunks + PAD, wide), BF),
            pltpu.VMEM((tps, model, width), BF),
            pltpu.VMEM((16, model), F32),
            pltpu.SemaphoreType.DMA((2,)),
            pltpu.SemaphoreType.DMA((2,)),
        ],
        cost_estimate=pl.CostEstimate(
            flops=6 * rows * model * model * (2 * tps + 1),
            bytes_accessed=60 << 20,
            transcendentals=0,
        ),
        compiler_params=pltpu.CompilerParams(vmem_limit_bytes=62 << 20),
        name="middle",
    )(att, tokens, cotangent, gathered, gathered)


def on_device(
    tokens,
    weight_query,
    weight_key,
    weight_value,
    weight_out,
    bias_query,
    bias_value,
    bias_out,
    first_scale,
    first_shift,
    weight_hidden,
    bias_hidden,
    weight_down,
    bias_down,
    second_scale,
    second_shift,
    cotangent,
):
    dps, tps = lax.axis_size("dp"), lax.axis_size("tensor")
    rows, model = tokens.shape
    piece = weight_hidden.shape[0]
    width = weight_query.shape[1]
    small = bias_query.shape[0]

    place = lax.axis_index("dp")

    def placed(pieces, length):
        zeros = jnp.zeros((pieces.shape[0], length), BF)
        return lax.dynamic_update_slice_in_dim(zeros, pieces, place * pieces.shape[1], 1)

    vec_rows = placed(
        jnp.stack(
            [bias_out, first_scale, first_shift, bias_down, second_scale, second_shift, bias_hidden]
        ),
        model,
    )
    packed_weights = pack_weights(
        weight_hidden, weight_down, weight_out, jnp.pad(vec_rows, ((0, PAD - 7), (0, 0)))
    )
    bias_rows = placed(jnp.stack([bias_query, bias_value]), width)
    bias_row = jnp.concatenate([bias_rows[0:1], jnp.zeros((1, width), BF), bias_rows[1:2]], axis=1)
    attn_pack = jnp.concatenate(
        [
            jnp.concatenate([weight_query, weight_key, weight_value], axis=1),
            jnp.pad(bias_row, ((0, PAD - 1), (0, 0))),
        ],
        axis=0,
    )
    rows_full, packs, qkv, attended, logsum, crossed, gathered = forward(
        tokens, attn_pack, packed_weights, dps, tps
    )
    output, grad_sum, grad_cross, packed = middle(crossed, tokens, cotangent, gathered)
    scatter = dps == 8 and tps == 4 and width == 2 * PAIR
    grad_tokens, attn_grads, summed = backward(
        grad_cross, packed, qkv, attended, logsum, rows_full, packs, grad_sum, scatter
    )
    if scatter:
        packed = summed
    else:
        packed = lax.psum_scatter(packed, "dp", scatter_dimension=0, tiled=False)
        packed = lax.psum_scatter(packed, "tensor", scatter_dimension=0, tiled=False).astype(F32)

    def share(values, count):
        return lax.dynamic_slice_in_dim(values, place * count, count, 0)

    chunks = min(model // width, piece // PAD)
    part = piece // chunks
    out_grad = packed[2 * piece : 2 * piece + part, : chunks * width]
    out_grad = out_grad.reshape(part, chunks, width).transpose(2, 1, 0).reshape(width, piece)
    vec_grads = [share(packed[2 * piece + part + i], piece) for i in range(6)]
    hidden_grad = share(packed[2 * piece + part + 6], bias_hidden.shape[0])
    return (
        output,
        grad_tokens,
        attn_grads[:piece, :width],
        attn_grads[:piece, width : 2 * width],
        attn_grads[:piece, 2 * width :],
        out_grad,
        share(attn_grads[piece, :width], small),
        share(attn_grads[piece, 2 * width :], small),
        vec_grads[0],
        vec_grads[1],
        vec_grads[2],
        packed[:piece],
        hidden_grad,
        packed[piece : 2 * piece].T,
        vec_grads[3],
        vec_grads[4],
        vec_grads[5],
    )


def solution(mesh):
    placed = (
        P(("dp", "tensor"), None),
        P("dp", "tensor"),
        P("dp", "tensor"),
        P("dp", "tensor"),
        P("tensor", "dp"),
        P(("tensor", "dp")),
        P(("tensor", "dp")),
        P("dp"),
        P("dp"),
        P("dp"),
        P("dp", "tensor"),
        P(("tensor", "dp")),
        P("tensor", "dp"),
        P("dp"),
        P("dp"),
        P("dp"),
        P(("dp", "tensor"), None),
    )
    return jax.shard_map(
        on_device,
        mesh=mesh,
        in_specs=placed,
        out_specs=(
            P(("dp", "tensor"), None),
            P(("dp", "tensor"), None),
            P("dp", "tensor"),
            P("dp", "tensor"),
            P("dp", "tensor"),
            P("tensor", "dp"),
            P(("tensor", "dp")),
            P(("tensor", "dp")),
            P("dp"),
            P("dp"),
            P("dp"),
            P("dp", "tensor"),
            P(("tensor", "dp")),
            P("tensor", "dp"),
            P("dp"),
            P("dp"),
            P("dp"),
        ),
        check_vma=False,
    )
```

```python
import jax
import jax.numpy as jnp
from jax import lax
from jax.experimental import pallas as pl
from jax.experimental.pallas import tpu as pltpu
from jax.sharding import PartitionSpec as P

HD = 64
PAIR = 2 * HD
PAD = 16
F32 = jnp.float32
BF = jnp.bfloat16


def contract(left, right, left_dim, right_dim):
    return lax.dot_general(
        left, right, (((left_dim,), (right_dim,)), ((), ())), preferred_element_type=F32
    )


def one_head(pair, head):
    lane = lax.broadcasted_iota(jnp.int32, pair.shape, 1)
    keep = lane < HD if head == 0 else lane >= HD
    return jnp.where(keep, pair, jnp.zeros_like(pair))


CUTS = 4


def flipped(index, bit):
    size = 1 << bit
    return index + size - 2 * size * lax.rem(index // size, 2)


def greet(dps, tps):
    place, level = lax.axis_index("dp"), lax.axis_index("tensor")
    barrier = pltpu.get_barrier_semaphore()
    bits = range(1, dps.bit_length() - 1)
    for bit in bits:
        pl.semaphore_signal(barrier, inc=1, device_id={"dp": flipped(place, bit)})
    pl.semaphore_signal(barrier, inc=1, device_id={"dp": flipped(place, 0)})
    for step in range(1, tps):
        other = lax.rem(level + step, tps)
        pl.semaphore_signal(barrier, inc=1, device_id={"tensor": other})
        pl.semaphore_signal(barrier, inc=1, device_id={"dp": flipped(place, 0), "tensor": other})
    pl.semaphore_wait(barrier, len(bits) + 2 * tps - 1)


def seat(place, level):
    core = lax.rem(place, 2)
    group = level // 2
    gate = lax.rem((level + 1) // 2, 2)
    mate = level + 1 - 2 * lax.rem(level, 2)
    near, far = 2 - group, 3 - 3 * group
    heads = lax.rem(level + 2 * core, 4)
    return core, group, gate, mate, near, far, heads


def ordered(level, step):
    group = level // 2
    gate = lax.rem((level + 1) // 2, 2)
    turned = step + gate * (step // 2) * (5 - 2 * step)
    return (1 - group) * (3 - turned) + group * turned


def forward_kernel(
    dps,
    tps,
    tok_ref,
    pack_ref,
    mine_ref,
    rows_ref,
    packs_ref,
    qkv_ref,
    att_ref,
    lse_ref,
    cross_ref,
    gath_ref,
    weight_s,
    away_sem,
    mate_sem,
    core_sem,
    land_sem,
    pack_send,
    pack_land,
    local_sem,
    level_send,
    level_land,
    plane_send,
    plane_land,
    cross_send,
    cross_land,
):
    place, level = lax.axis_index("dp"), lax.axis_index("tensor")
    rows, model = tok_ref.shape
    piece = model // dps
    width = pack_ref.shape[1] // 3
    pairs = width // PAIR
    cut = rows // CUTS
    count = mine_ref.shape[0]
    middle_row = count // (2 * PAD) * PAD
    spans = (pl.ds(0, middle_row), pl.ds(middle_row, count - middle_row))
    bits = tuple(range(1, dps.bit_length() - 1))
    orders = (bits, bits[::-1])
    core, group, gate, mate, near, far, heads = seat(place, level)
    lead = core == group
    partner = flipped(place, 0)
    own = pltpu.make_async_copy(tok_ref, rows_ref.at[level], local_sem.at[0])
    own_pack = pltpu.make_async_copy(pack_ref, packs_ref.at[place], local_sem.at[1])
    own_block = pltpu.make_async_copy(mine_ref, gath_ref.at[place, level], local_sem.at[2])
    own_block.start()

    @pl.when(lead)
    def _():
        own.start()

    @pl.when(core == 0)
    def _():
        own_pack.start()

    greet(dps, tps)

    def away(chunk):
        span = pl.ds(chunk * cut, cut)
        return pltpu.make_async_remote_copy(
            src_ref=tok_ref.at[span],
            dst_ref=rows_ref.at[level, span],
            send_sem=away_sem.at[chunk],
            recv_sem=land_sem.at[level, chunk],
            device_id={"tensor": near},
        )

    def to_mate(block, chunk, first=False):
        span = pl.ds(chunk * cut, cut)
        return pltpu.make_async_remote_copy(
            src_ref=tok_ref.at[span] if first else rows_ref.at[block, span],
            dst_ref=rows_ref.at[block, span],
            send_sem=mate_sem.at[block, chunk],
            recv_sem=land_sem.at[block, chunk],
            device_id={"tensor": mate},
        )

    def to_core(block, chunk, first=False):
        span = pl.ds(chunk * cut, cut)
        return pltpu.make_async_remote_copy(
            src_ref=tok_ref.at[span] if first else rows_ref.at[block, span],
            dst_ref=rows_ref.at[block, span],
            send_sem=core_sem.at[block, chunk],
            recv_sem=land_sem.at[block, chunk],
            device_id={"dp": partner},
        )

    def to_level(step, half):
        return pltpu.make_async_remote_copy(
            src_ref=mine_ref.at[spans[half]],
            dst_ref=gath_ref.at[place, level, spans[half]],
            send_sem=level_send.at[step, half],
            recv_sem=level_land.at[step, half],
            device_id={"tensor": lax.rem(level + step, tps)},
        )

    def in_plane(block, step, half, bit, number, mine=False):
        at = lax.rem(level + step, tps)
        return pltpu.make_async_remote_copy(
            src_ref=mine_ref.at[spans[half]] if mine else gath_ref.at[block, at, spans[half]],
            dst_ref=gath_ref.at[block, at, spans[half]],
            send_sem=plane_send.at[number, step, half],
            recv_sem=plane_land.at[block, step, half],
            device_id={"dp": flipped(place, bit)},
        )

    def held(half, stage):
        blocks = [place]
        for bit in orders[half][:stage]:
            blocks = blocks + [flipped(block, bit) for block in blocks]
        return blocks

    def numbered(half):
        found, at = [], 0
        for stage in range(len(bits) + 1):
            for block in held(half, stage)[(1 << stage) // 2 if stage else 0 :]:
                targets = list(orders[half][stage:]) + [0]
                found.append((stage, block, [(bit, at + i) for i, bit in enumerate(targets)]))
                at += len(targets)
        return found

    tables = (numbered(0), numbered(1))

    def pass_on(step, stage):
        for half in range(2):
            for came, block, targets in tables[half]:
                if came != stage:
                    continue
                if stage:
                    in_plane(block, step, half, 0, 0).wait_recv()
                for bit, number in targets:
                    in_plane(block, step, half, bit, number, step == 0 and stage == 0).start()

    def level_in(step):
        back = tps - step
        for half in range(2):
            pltpu.make_async_remote_copy(
                src_ref=mine_ref.at[spans[half]],
                dst_ref=gath_ref.at[place, lax.rem(level + step, tps), spans[half]],
                send_sem=level_send.at[back, half],
                recv_sem=level_land.at[back, half],
                device_id={"tensor": lax.rem(level + back, tps)},
            ).wait_recv()

    even = place - core
    opposite = lax.rem(level + 2, tps)

    def pack_to(index, block, device):
        return pltpu.make_async_remote_copy(
            src_ref=pack_ref,
            dst_ref=packs_ref.at[block],
            send_sem=pack_send.at[index],
            recv_sem=pack_land.at[block],
            device_id=device,
        )

    pack_to(0, place, {"dp": even + 1, "tensor": opposite}).start()
    for half in range(2):
        to_level(1, half).start()
    for half in range(2):
        to_level(3, half).start()
    for chunk in range(CUTS):

        @pl.when(lead)
        def _():
            to_mate(level, chunk, True).start()
            to_core(level, chunk, True).start()

        @pl.when(core != group)
        def _():
            away(chunk).start()

    pass_on(0, 0)

    @pl.when(core == 1)
    def _():
        pack_to(1, place, {"dp": even}).start()
        pack_to(0, even, {"dp": even}).wait_recv()

    @pl.when(core == 0)
    def _():
        own_pack.wait()

    pack_to(0, even + 1, {"dp": even}).wait_recv()

    def pack_on(block, index, bit):
        return pltpu.make_async_remote_copy(
            src_ref=packs_ref.at[block],
            dst_ref=packs_ref.at[block],
            send_sem=pack_send.at[index],
            recv_sem=pack_land.at[block],
            device_id={"dp": flipped(place, bit)},
        )

    known = [even, even + 1]
    sent = 2
    pack_sends = []
    for bit in bits:
        for block in known:
            pack_on(block, sent, bit).start()
            pack_sends.append((block, sent, bit))
            sent += 1
        more = [flipped(block, bit) for block in known]
        for block in more:
            pack_on(block, 0, bit).wait_recv()
        known = known + more
    weight_s[...] = packs_ref[:, :piece].reshape(weight_s.shape)
    bias = jnp.sum(packs_ref[:, piece : piece + PAD].astype(F32), axis=0)[0:1]

    def project(block):
        qkv_ref[block] = (contract(rows_ref[block], weight_s[...], 1, 0) + bias).astype(BF)

    def advance(step, stage):
        if step and stage == 0:
            level_in(step)
        pass_on(step, stage)

    @pl.when(lead)
    def _():
        own.wait()

    for index, block in enumerate((level, mate, near, far)):
        for chunk in range(CUTS):
            if index:

                @pl.when(lead)
                def _():
                    to_core(block, chunk).wait_recv()

                if index > 1:

                    @pl.when(lead & (gate == 1))
                    def _():
                        to_mate(block, chunk).start()

                @pl.when(lead)
                def _():
                    to_core(block, chunk).start()

            @pl.when(core != group)
            def _():
                to_core(block, chunk).wait_recv()

        project(block)
        for other, when in ((2, 1),):
            if when == index:
                for half in range(2):
                    to_level(other, half).start()
        for step, stage in (((0, 1),), ((1, 0),), ((0, 2), (3, 0)), ((1, 1),))[index]:
            advance(step, stage)
    for stage in range(3, len(bits) + 1):
        pass_on(0, stage)

    half_rows = rows // 2

    def cross(target, half):
        span = pl.ds(half * half_rows, half_rows)
        return pltpu.make_async_remote_copy(
            src_ref=att_ref.at[target, span],
            dst_ref=cross_ref.at[heads, span],
            send_sem=cross_send.at[target, half],
            recv_sem=cross_land.at[heads, half],
            device_id={"dp": even + group, "tensor": target},
        )

    turns = 2 * pairs * tps

    def attend(turn, carry):
        pair = lax.rem(turn, pairs)
        half = lax.rem(turn // pairs, 2)
        target = ordered(level, turn // (2 * pairs))
        span = pl.ds(pl.multiple_of(half * half_rows, half_rows), half_rows)
        lanes = pl.ds(pl.multiple_of(pair * PAIR, PAIR), PAIR)
        query = qkv_ref[target, span, lanes] * jnp.asarray(0.125, BF)
        key = qkv_ref[:, :, pl.ds(pl.multiple_of(width + pair * PAIR, PAIR), PAIR)]
        value = qkv_ref[:, :, pl.ds(pl.multiple_of(2 * width + pair * PAIR, PAIR), PAIR)]
        key, value = key.reshape(tps * rows, PAIR), value.reshape(tps * rows, PAIR)
        total, columns = None, []
        for head in range(2):
            scores = contract(query, one_head(key, head), 1, 1)
            highest = jnp.max(scores, axis=1, keepdims=True)
            expons = jnp.exp(scores - highest)
            mass = jnp.sum(expons, axis=1, keepdims=True)
            part = contract(expons.astype(BF), one_head(value, head), 1, 0) / mass
            total = part if total is None else total + part
            columns.append(jnp.broadcast_to(highest + jnp.log(mass), (half_rows, PAIR)))
        att_ref[target, span, lanes] = total.astype(BF)
        where = pl.ds(pl.multiple_of(target * rows + half * half_rows, half_rows), half_rows)
        lse_ref[pair, :, where] = jnp.concatenate(
            [jnp.transpose(column)[:4] for column in columns], axis=0
        )

        @pl.when((pair == pairs - 1) & ((turn < 2 * pairs * (tps - 1)) | (core != group)))
        def _():
            cross(target, half).start()

        for at, batch in events.items():

            @pl.when(turn == at)
            def _():
                for step, stage in batch:
                    advance(step, stage)

        return carry

    events = {1: [(3, 1)], turns // 4: [(1, 2), (2, 0)], turns // 2: [(3, 2)], turns - 4: [(2, 1)], turns - 1: [(2, 2)]}
    early = [item for batch in events.values() for item in batch]
    early = early + [item for batch in (((0, 1),), ((1, 0),), ((0, 2), (3, 0)), ((1, 1),)) for item in batch]
    late = [
        (step, stage)
        for step in range(1, tps)
        for stage in range(len(bits) + 1)
        if (step, stage) not in early
    ]
    lax.fori_loop(0, turns, attend, 0)
    own_cross = pltpu.make_async_copy(att_ref.at[level], cross_ref.at[heads], local_sem.at[3])

    @pl.when(lead)
    def _():
        own_cross.start()

    for step, stage in sorted(late, key=lambda item: (item[0] + item[1], item[0])):
        advance(step, stage)
    for index in range(tps):
        for half in range(2):

            @pl.when((core != group) | (index != heads))
            def _():
                pltpu.make_async_remote_copy(
                    src_ref=att_ref.at[level, pl.ds(half * half_rows, half_rows)],
                    dst_ref=cross_ref.at[index, pl.ds(half * half_rows, half_rows)],
                    send_sem=cross_send.at[index, half],
                    recv_sem=cross_land.at[index, half],
                    device_id={"tensor": mate},
                ).wait_recv()

            @pl.when((core != group) | (index != level))
            def _():
                cross(index, half).wait_send()

            if index:
                to_level(index, half).wait_send()
    for step in range(tps):
        for half in range(2):
            for stage, block, targets in tables[half]:
                in_plane(flipped(block, 0), step, half, 0, 0).wait_recv()
                for bit, number in targets:
                    in_plane(block, step, half, bit, number).wait_send()
    own_block.wait()
    pack_to(0, place, {"dp": even + 1, "tensor": opposite}).wait_send()

    @pl.when(core == 1)
    def _():
        pack_to(1, place, {"dp": even}).wait_send()

    for block, index, bit in pack_sends:
        pack_on(block, index, bit).wait_send()

    @pl.when(lead)
    def _():
        own_cross.wait()

    for chunk in range(CUTS):

        @pl.when(core != group)
        def _():
            away(chunk).wait_send()

        for index, block in enumerate((level, mate, near, far)):

            @pl.when(lead)
            def _():
                to_core(block, chunk).wait_send()

            if index == 0:

                @pl.when(lead)
                def _():
                    to_mate(block, chunk).wait_send()

            if index > 1:

                @pl.when(lead & (gate == 1))
                def _():
                    to_mate(block, chunk).wait_send()


def forward(tokens, pack, mine, dps, tps):
    rows, model = tokens.shape
    columns = pack.shape[1]
    width = columns // 3
    vmem = pl.BlockSpec(memory_space=pltpu.VMEM)
    hbm = pl.BlockSpec(memory_space=pl.ANY)
    dma = pltpu.SemaphoreType.DMA
    return pl.pallas_call(
        lambda *refs: forward_kernel(dps, tps, *refs),
        in_specs=[vmem, vmem, hbm],
        out_specs=[vmem] * 5 + [hbm] * 2,
        out_shape=[
            jax.ShapeDtypeStruct((tps, rows, model), BF),
            jax.ShapeDtypeStruct((dps,) + pack.shape, BF),
            jax.ShapeDtypeStruct((tps, rows, columns), BF),
            jax.ShapeDtypeStruct((tps, rows, width), BF),
            jax.ShapeDtypeStruct((width // PAIR, 8, tps * rows), F32),
            jax.ShapeDtypeStruct((tps, rows, width), BF),
            jax.ShapeDtypeStruct((dps, tps) + mine.shape, BF),
        ],
        scratch_shapes=[
            pltpu.VMEM((model, columns), BF),
            dma((CUTS,)),
            dma((tps, CUTS)),
            dma((tps, CUTS)),
            dma((tps, CUTS)),
            dma((dps,)),
            dma((dps,)),
            dma((4,)),
            dma((tps, 2)),
            dma((tps, 2)),
            dma((dps - 1, tps, 2)),
            dma((dps, tps, 2)),
            dma((tps, 2)),
            dma((tps, 2)),
        ],
        cost_estimate=pl.CostEstimate(
            flops=2 * tps * rows * model * columns, bytes_accessed=200 << 20, transcendentals=0
        ),
        compiler_params=pltpu.CompilerParams(
            vmem_limit_bytes=50 << 20, collective_id=1, has_side_effects=True
        ),
        name="forward",
    )(tokens, pack, mine)


def backward_kernel(
    dps,
    tps,
    scatter,
    cross_ref,
    packed_ref,
    qkv_ref,
    att_ref,
    lse_ref,
    rows_ref,
    packs_ref,
    gsum_ref,
    tok_out,
    pack_out,
    feed_out,
    grad_s,
    weight_s,
    dq_s,
    dk_s,
    dv_s,
    land_s,
    other_s,
    mine_s,
    theirs_s,
    gsum_s,
    kept_s,
    stage_s,
    one_a,
    one_b,
    two_a,
    two_b,
    level_s,
    local_sem,
    grad_send,
    grad_land,
    core_send,
    core_land,
    hop_send,
    hop_land,
    pack_send,
    pack_land,
    chip_send,
    chip_land,
    stage_sem,
    one_send,
    one_land,
    two_send,
    two_land,
    level_send,
    level_land,
):
    place, level = lax.axis_index("dp"), lax.axis_index("tensor")
    rows, model = gsum_ref.shape
    piece = model // dps
    width = att_ref.shape[2]
    pairs = width // PAIR
    cut = rows // CUTS
    half_rows = rows // 2
    count = packed_ref.shape[2]
    middle_row = count // (2 * PAD) * PAD
    spans = (pl.ds(0, middle_row), pl.ds(middle_row, count - middle_row))

    load_weight = pltpu.make_async_copy(
        packs_ref.at[:, pl.ds(0, piece)], weight_s, local_sem.at[0]
    )
    load_sum = pltpu.make_async_copy(gsum_ref, gsum_s, local_sem.at[1])
    core, group, gate, mate, near, far, heads = seat(place, level)
    lead = core == group
    even = place - core
    opposite = lax.rem(level + 2, tps)
    own_grad = pltpu.make_async_copy(cross_ref.at[heads], grad_s.at[level], local_sem.at[2])
    load_weight.start()
    load_sum.start()

    @pl.when(lead)
    def _():
        own_grad.start()

    greet(dps, tps)

    def cross(index):
        other = lax.rem(index // 2 + core, 2)
        return pltpu.make_async_remote_copy(
            src_ref=cross_ref.at[index],
            dst_ref=grad_s.at[level],
            send_sem=grad_send.at[index],
            recv_sem=grad_land.at[level],
            device_id={"dp": even + other, "tensor": lax.rem(index + 2 * other, tps)},
        )

    def crossed(block):
        return pltpu.make_async_remote_copy(
            src_ref=cross_ref.at[block],
            dst_ref=grad_s.at[block],
            send_sem=grad_send.at[block],
            recv_sem=grad_land.at[block],
            device_id={"tensor": mate},
        )

    for index in range(tps):

        @pl.when((core != group) | (index != heads))
        def _():
            cross(index).start()

    def block_of(kind):
        block = place
        if kind in (0, 2):
            block = flipped(block, 1)
        if kind in (0, 1):
            block = flipped(block, 2)
        return block

    def level_of(turn):
        return lax.rem(level + 1 + turn, tps)

    def chip(kind, turn):
        return pltpu.make_async_remote_copy(
            src_ref=packed_ref.at[flipped(block_of(kind), 0), level_of(turn)],
            dst_ref=kept_s.at[turn * 4 + kind],
            send_sem=chip_send.at[turn * 4 + kind],
            recv_sem=chip_land.at[turn * 4 + kind],
            device_id={"dp": flipped(place, 0)},
        )

    def load(kind, turn, slot):
        return pltpu.make_async_copy(
            packed_ref.at[block_of(kind), level_of(turn)], stage_s.at[slot], stage_sem.at[slot]
        )

    def plane_one(kind, turn, half):
        bit = 2 - half
        target = one_b if half else one_a
        at = turn * 2 + (0 if kind == 0 else 1)
        return pltpu.make_async_remote_copy(
            src_ref=kept_s.at[turn * 4 + kind, spans[half]],
            dst_ref=target.at[at],
            send_sem=one_send.at[at, half],
            recv_sem=one_land.at[at, half],
            device_id={"dp": flipped(place, bit)},
        )

    def plane_two(turn, half):
        bit = 1 + half
        target = two_b if half else two_a
        return pltpu.make_async_remote_copy(
            src_ref=kept_s.at[turn * 4 + 2 - half, spans[half]],
            dst_ref=target.at[turn],
            send_sem=two_send.at[turn, half],
            recv_sem=two_land.at[turn, half],
            device_id={"dp": flipped(place, bit)},
        )

    def over_z(turn):
        return pltpu.make_async_remote_copy(
            src_ref=kept_s.at[turn * 4 + 3],
            dst_ref=level_s.at[turn],
            send_sem=level_send.at[turn],
            recv_sem=level_land.at[turn],
            device_id={"tensor": level_of(turn)},
        )

    def add_to(slot, half, source):
        kept_s[slot, spans[half]] = (
            kept_s[slot, spans[half]].astype(F32) + source.astype(F32)
        ).astype(BF)

    def chip_in(kind, turn):
        slot = kind % 2
        load(kind, turn, slot).wait()
        chip(kind, turn).wait_recv()
        at = turn * 4 + kind
        kept_s[at] = (kept_s[at].astype(F32) + stage_s[slot].astype(F32)).astype(BF)
        if kind in (0, 1):
            plane_one(kind, turn, 0).start()
        if kind in (0, 2):
            plane_one(kind, turn, 1).start()

    def one_in(turn):
        plane_one(0, turn, 0).wait_recv()
        add_to(turn * 4 + 2, 0, one_a[turn * 2])
        plane_two(turn, 0).start()
        plane_one(0, turn, 1).wait_recv()
        add_to(turn * 4 + 1, 1, one_b[turn * 2])
        plane_two(turn, 1).start()
        plane_one(1, turn, 0).wait_recv()
        add_to(turn * 4 + 3, 0, one_a[turn * 2 + 1])
        plane_one(2, turn, 1).wait_recv()
        add_to(turn * 4 + 3, 1, one_b[turn * 2 + 1])

    def two_in(turn):
        plane_two(turn, 0).wait_recv()
        add_to(turn * 4 + 3, 0, two_a[turn])
        plane_two(turn, 1).wait_recv()
        add_to(turn * 4 + 3, 1, two_b[turn])
        if turn < tps - 1:
            over_z(turn).start()

    if scatter:
        load(0, 0, 0).start()
        for turn in range(tps):
            for kind in range(4):
                chip(kind, turn).start()

    dk_s[...] = jnp.zeros_like(dk_s)
    dv_s[...] = jnp.zeros_like(dv_s)

    @pl.when(lead)
    def _():
        own_grad.wait()

    def attend(turn, carry):
        pair = lax.rem(turn, pairs)
        half = lax.rem(turn // pairs, 2)
        step = turn // (2 * pairs)
        target = ordered(level, tps - 1 - step)

        @pl.when((lax.rem(turn, 2 * pairs) == 0) & ((step > 0) | (core != group)))
        def _():
            crossed(target).wait_recv()

        span = pl.ds(pl.multiple_of(half * half_rows, half_rows), half_rows)
        lanes = pl.ds(pl.multiple_of(pair * PAIR, PAIR), PAIR)
        query = qkv_ref[target, span, lanes] * jnp.asarray(0.125, BF)
        key = qkv_ref[:, :, pl.ds(pl.multiple_of(width + pair * PAIR, PAIR), PAIR)]
        value = qkv_ref[:, :, pl.ds(pl.multiple_of(2 * width + pair * PAIR, PAIR), PAIR)]
        key, value = key.reshape(tps * rows, PAIR), value.reshape(tps * rows, PAIR)
        grad = grad_s[target, span, lanes]
        products = jnp.transpose(grad.astype(F32) * att_ref[target, span, lanes].astype(F32))
        where = pl.ds(pl.multiple_of(target * rows + half * half_rows, half_rows), half_rows)
        logsums = lse_ref[pair, :, where]
        grad_query = None
        for head in range(2):
            key_head, value_head = one_head(key, head), one_head(value, head)
            inner = jnp.sum(products[HD * head : HD * head + HD], axis=0, keepdims=True)
            logsum = logsums[4 * head : 4 * head + 1]
            probs = jnp.exp(contract(key_head, query, 1, 1) - logsum)
            grad_probs = contract(value_head, grad, 1, 1)
            grad_scores = (probs * (grad_probs - inner)).astype(BF)
            dv_s[:, lanes] += contract(probs.astype(BF), one_head(grad, head), 1, 0)
            dk_s[:, lanes] += contract(grad_scores, one_head(query, head), 1, 0)
            part = contract(grad_scores, key_head, 0, 0)
            grad_query = part if grad_query is None else grad_query + part
        dq_s[where, lanes] = (grad_query * 0.125).astype(BF)

        if scatter:
            for kind in range(4):

                @pl.when(lax.rem(turn, 4) == kind)
                def _():
                    if kind < 3:
                        load(kind + 1, turn // 4, (kind + 1) % 2).start()
                    else:

                        @pl.when(turn // 4 < tps - 1)
                        def _():
                            load(0, turn // 4 + 1, 0).start()

                    chip_in(kind, turn // 4)

            @pl.when(turn == 9)
            def _():
                one_in(0)

            @pl.when(turn == 13)
            def _():
                two_in(0)

            @pl.when(turn == 15)
            def _():
                one_in(1)

        return carry

    lax.fori_loop(0, 2 * pairs * tps, attend, 0)
    load_weight.wait()
    refs = (dq_s, dk_s, dv_s)

    def rows_of(block):
        span = pl.ds(pl.multiple_of(block * rows, rows), rows)
        total = None
        for index, ref in enumerate(refs):
            weight = weight_s[:, :, index * width : (index + 1) * width].reshape(model, width)
            part = contract(ref[span].astype(BF), weight, 1, 1)
            total = part if total is None else total + part
        return total

    def to_core(block, chunk):
        span = pl.ds(chunk * cut, cut)
        return pltpu.make_async_remote_copy(
            src_ref=land_s.at[block, span],
            dst_ref=land_s.at[block, span],
            send_sem=core_send.at[block, chunk],
            recv_sem=core_land.at[block, chunk],
            device_id={"dp": flipped(place, 0)},
        )

    def onward(block, chunk, slot, device):
        span = pl.ds(chunk * cut, cut)
        return pltpu.make_async_remote_copy(
            src_ref=land_s.at[block, span],
            dst_ref=other_s.at[slot, span],
            send_sem=hop_send.at[block, chunk],
            recv_sem=hop_land.at[slot, chunk],
            device_id={"tensor": device},
        )

    order_of = (far, near, mate, level)

    def part_out(index):
        block = order_of[index]
        land_s[block] = rows_of(block).astype(BF)
        for chunk in range(CUTS):
            to_core(block, chunk).start()

    def chip_total(block, chunk, own):
        to_core(block, chunk).wait_recv()
        span = pl.ds(chunk * cut, cut)
        return land_s[block, span].astype(F32) + own[chunk * cut : (chunk + 1) * cut]

    def part_on(index):
        block = order_of[index]
        own = rows_of(block)
        for chunk in range(CUTS):
            land_s[block, pl.ds(chunk * cut, cut)] = chip_total(block, chunk, own).astype(BF)
            onward(block, chunk, index, mate).start()

    def part_through(index):
        block = order_of[index]
        own = rows_of(block)
        for chunk in range(CUTS):
            span = pl.ds(chunk * cut, cut)
            total = chip_total(block, chunk, own)
            onward(block, chunk, index, block).wait_recv()
            land_s[block, span] = (total + other_s[index, span].astype(F32)).astype(BF)
            onward(block, chunk, 2, block).start()

    def part_own():
        own = rows_of(level)
        for chunk in range(CUTS):
            land_s[level, pl.ds(chunk * cut, cut)] = chip_total(level, chunk, own).astype(BF)

    for index in range(tps):

        @pl.when(core != group)
        def _():
            part_out(index)

    outer = lead & (gate == 0)
    inner = lead & (gate == 1)
    for index in (0, 1):

        @pl.when(outer)
        def _():
            part_on(index)

    @pl.when(lead)
    def _():
        part_on(2)

    tail = jnp.concatenate(
        [jnp.sum(ref[...].astype(BF).astype(F32), axis=0, keepdims=True) for ref in refs], axis=1
    )
    tokens = rows_ref.reshape(tps * rows, model)
    for index, ref in enumerate(refs):
        grad = contract(tokens[...], ref[...].astype(BF), 0, 0).astype(BF)
        mine_s[:, :piece, index * width : (index + 1) * width] = grad.reshape(dps, piece, width)
    mine_s[:, piece:] = jnp.broadcast_to(tail.astype(BF)[None], (dps, PAD, 3 * width))

    def exchange(index, bit, other):
        return pltpu.make_async_remote_copy(
            src_ref=mine_s.at[other],
            dst_ref=theirs_s.at[index],
            send_sem=pack_send.at[index],
            recv_sem=pack_land.at[index],
            device_id={"dp": flipped(place, bit)},
        )

    plane = tuple(range(1, dps.bit_length() - 1))[::-1]

    def kept(done):
        blocks = [even, even + 1]
        for bit in plane[done:][::-1]:
            blocks = blocks + [flipped(block, bit) for block in blocks]
        return blocks

    starts, at = [], 0
    for done in range(len(plane)):
        starts.append(at)
        at += dps >> (done + 1)

    def pack_start(done):
        for index, block in enumerate(kept(done + 1)):
            exchange(starts[done] + index, plane[done], flipped(block, plane[done])).start()

    def pack_finish(done):
        for index, block in enumerate(kept(done + 1)):
            exchange(starts[done] + index, plane[done], block).wait()
            mine_s[block] = (
                mine_s[block].astype(F32) + theirs_s[starts[done] + index].astype(F32)
            ).astype(BF)

    def pack_home(block, slot, device):
        return pltpu.make_async_remote_copy(
            src_ref=mine_s.at[block],
            dst_ref=theirs_s.at[slot],
            send_sem=pack_send.at[lax.rem(block, 2) + dps - 2],
            recv_sem=pack_land.at[slot],
            device_id=device,
        )

    def homeward():
        @pl.when(core == 0)
        def _():
            pack_home(even + 1, dps - 1, {"dp": even + 1}).start()

        @pl.when(core == 1)
        def _():
            pack_home(even, dps - 2, {"dp": even, "tensor": opposite}).start()
            pack_home(even + 1, dps - 2, {"tensor": opposite}).start()

    pack_start(0)
    if scatter:
        two_in(1)
        one_in(2)
    for index in (0, 1):

        @pl.when(inner)
        def _():
            part_through(index)

    @pl.when(lead)
    def _():
        part_own()

    stages = len(plane)
    for turn in range(stages):
        pack_finish(turn)
        if turn + 1 < stages:
            pack_start(turn + 1)
        else:
            homeward()
        if scatter and turn == 0:
            one_in(3)
            two_in(2)
    if scatter:
        two_in(3)
    pack_home(even, dps - 2, {"dp": even}).wait_recv()

    @pl.when(core == 0)
    def _():
        pack_out[...] = mine_s[even].astype(F32) + theirs_s[dps - 2].astype(F32)
        pack_home(even + 1, dps - 1, {"dp": even + 1}).wait_send()

    @pl.when(core == 1)
    def _():
        pack_home(even, dps - 1, {"dp": even}).wait_recv()
        pack_out[...] = theirs_s[dps - 1].astype(F32) + theirs_s[dps - 2].astype(F32)
        pack_home(even, dps - 2, {"dp": even, "tensor": opposite}).wait_send()
        pack_home(even + 1, dps - 2, {"tensor": opposite}).wait_send()

    load_sum.wait()
    if scatter:
        total = kept_s[(tps - 1) * 4 + 3].astype(F32)
        for turn in range(tps - 1):
            over_z(turn).wait_recv()
            total = total + level_s[turn].astype(F32)
        feed_out[...] = total
    for chunk in range(CUTS):
        onward(level, chunk, 2, mate).wait_recv()
    total = gsum_s[...] + other_s[2].astype(F32)
    tok_out[...] = (total + jnp.where(lead, land_s[level].astype(F32), 0.0)).astype(BF)
    for index, block in enumerate(order_of):

        @pl.when((core != group) | (index != heads))
        def _():
            cross(index).wait_send()

        for chunk in range(CUTS):

            @pl.when(core != group)
            def _():
                to_core(block, chunk).wait_send()

            if index < 3:

                @pl.when(lead)
                def _():
                    onward(block, chunk, 2, mate).wait_send()

    if scatter:
        for turn in range(tps):
            for kind in range(4):
                chip(kind, turn).wait_send()
            plane_one(0, turn, 0).wait_send()
            plane_one(1, turn, 0).wait_send()
            plane_one(0, turn, 1).wait_send()
            plane_one(2, turn, 1).wait_send()
            plane_two(turn, 0).wait_send()
            plane_two(turn, 1).wait_send()
            if turn < tps - 1:
                over_z(turn).wait_send()
    else:
        feed_out[...] = jnp.zeros_like(feed_out)


def backward(grad_cross, packed, qkv, attended, logsum, rows_full, packs, grad_sum, scatter):
    rows, model = grad_sum.shape
    tps = rows_full.shape[0]
    dps, pack_rows, columns = packs.shape
    width = columns // 3
    count = packed.shape[2]
    middle_row = count // (2 * PAD) * PAD
    vmem = pl.BlockSpec(memory_space=pltpu.VMEM)
    hbm = pl.BlockSpec(memory_space=pl.ANY)
    dma = pltpu.SemaphoreType.DMA
    slots = 4 * tps if scatter else 1

    def buffer(*shape):
        return pltpu.VMEM(shape if scatter else (1, 16, model), BF)

    return pl.pallas_call(
        lambda *refs: backward_kernel(dps, tps, scatter, *refs),
        in_specs=[hbm, hbm, vmem, vmem, vmem, vmem, hbm, hbm],
        out_specs=[vmem] * 3,
        out_shape=[
            jax.ShapeDtypeStruct((rows, model), BF),
            jax.ShapeDtypeStruct((pack_rows, columns), F32),
            jax.ShapeDtypeStruct((count, model), F32),
        ],
        scratch_shapes=[
            pltpu.VMEM((tps, rows, width), BF),
            pltpu.VMEM((dps, model // dps, columns), BF),
            pltpu.VMEM((tps * rows, width), BF),
            pltpu.VMEM((tps * rows, width), F32),
            pltpu.VMEM((tps * rows, width), F32),
            pltpu.VMEM((tps, rows, model), BF),
            pltpu.VMEM((3, rows, model), BF),
            pltpu.VMEM(packs.shape, BF),
            pltpu.VMEM(packs.shape, BF),
            pltpu.VMEM((rows, model), F32),
            buffer(slots, count, model),
            buffer(2, count, model),
            buffer(2 * tps, middle_row, model),
            buffer(2 * tps, count - middle_row, model),
            buffer(tps, middle_row, model),
            buffer(tps, count - middle_row, model),
            buffer(tps - 1, count, model),
            dma((3,)),
            dma((tps,)),
            dma((tps,)),
            dma((tps, CUTS)),
            dma((tps, CUTS)),
            dma((tps, CUTS)),
            dma((3, CUTS)),
            dma((dps,)),
            dma((dps,)),
            dma((slots,)),
            dma((slots,)),
            dma((2,)),
            dma((2 * tps, 2)),
            dma((2 * tps, 2)),
            dma((tps, 2)),
            dma((tps, 2)),
            dma((tps - 1,)),
            dma((tps - 1,)),
        ],
        cost_estimate=pl.CostEstimate(
            flops=4 * tps * rows * model * columns, bytes_accessed=200 << 20, transcendentals=0
        ),
        compiler_params=pltpu.CompilerParams(
            vmem_limit_bytes=63 << 20, collective_id=2, has_side_effects=True
        ),
        name="backward",
    )(grad_cross, packed, qkv, attended, logsum, rows_full, packs, grad_sum)


def pack_kernel(hidden_ref, down_ref, out_ref, vec_ref, packed_ref):
    piece, wide = hidden_ref.shape
    width = out_ref.shape[0]
    chunks = min(wide // width, piece // PAD)
    part = piece // chunks
    packed_ref[:piece] = hidden_ref[...]
    packed_ref[piece : 2 * piece] = jnp.transpose(down_ref[...])
    turned = jnp.transpose(out_ref[...])
    for chunk in range(chunks):
        packed_ref[2 * piece : 2 * piece + part, chunk * width : (chunk + 1) * width] = turned[
            chunk * part : (chunk + 1) * part
        ]
    if chunks * width < wide:
        packed_ref[2 * piece : 2 * piece + part, chunks * width :] = jnp.zeros(
            (part, wide - chunks * width), BF
        )
    packed_ref[2 * piece + part :] = vec_ref[...]


def pack_weights(hidden, down, out, vec):
    piece, wide = hidden.shape
    chunks = min(wide // out.shape[0], piece // PAD)
    return pl.pallas_call(
        pack_kernel,
        out_shape=jax.ShapeDtypeStruct((2 * piece + piece // chunks + PAD, wide), BF),
        name="pack",
    )(hidden, down, out, vec)


def row_mean(values):
    return jnp.mean(values, axis=1, keepdims=True)


def column_sum(values):
    return jnp.sum(values, axis=0, keepdims=True)


def middle_kernel(
    sizes,
    att_ref,
    tok_ref,
    cot_ref,
    all_ref,
    feed_ref,
    out_ref,
    gsum_ref,
    gatt_ref,
    pack_ref,
    first_s,
    norm_s,
    down_s,
    inv_s,
    low_s,
    low_t,
    gdown_s,
    gdown_t,
    hidden_s,
    slope_s,
    stage_s,
    tail_s,
    extra_s,
    wout_s,
    vec_s,
    sems,
    extra_sem,
):
    dps, tps, piece, chunks = sizes
    step = pl.program_id(0)
    model = tok_ref.shape[1]
    feed_rows = 2 * piece
    part = piece // chunks
    width = att_ref.shape[2]

    def norm_parts(values):
        centered = values - row_mean(values)
        inverse = lax.rsqrt(row_mean(centered * centered) + 1e-05)
        return centered * inverse, inverse

    def norm_back(grad, scale, normed, inverse):
        scaled = grad * scale
        return inverse * (scaled - row_mean(scaled) - normed * row_mean(scaled * normed))

    def send(slot, block):
        return pltpu.make_async_copy(
            stage_s.at[slot], pack_ref.at[:, block, pl.ds(0, feed_rows)], sems.at[slot]
        )

    @pl.when(step == 0)
    def _():
        def fetch(t):
            return pltpu.make_async_copy(
                all_ref.at[:, t, pl.ds(feed_rows, part + PAD)], extra_s.at[t % 2], extra_sem.at[t % 2]
            )

        fetch(0).start()
        for t in range(tps):
            if t + 1 < tps:
                fetch(t + 1).start()
            fetch(t).wait()
            extra = extra_s.at[t % 2]
            placed = jnp.sum(extra[:, part:].astype(F32), axis=0)
            if t == 0:
                vec_s[0:8] = placed[0:8]
            vec_s[8 + t : 9 + t] = placed[6:7]
            turned = jnp.concatenate(
                [extra[:, :part, c * width : (c + 1) * width] for c in range(chunks)], axis=1
            )
            wout_s[t] = turned.reshape(model, width)
        branch = None
        for t in range(tps):
            term = contract(att_ref[t], wout_s[t], 1, 1)
            branch = term if branch is None else branch + term
        normed, inverse = norm_parts(tok_ref[...].astype(F32) + branch + vec_s[0:1])
        first = normed * vec_s[1:2] + vec_s[2:3]
        norm_s[...] = normed
        inv_s[...] = jnp.broadcast_to(inverse, inv_s.shape)
        first_s[...] = first
        low = first.astype(BF)
        low_s[...] = low
        low_t[...] = jnp.transpose(low)
        down_s[...] = jnp.zeros_like(down_s)

    @pl.when(step < tps)
    def _():
        weight = feed_ref[:, 0, :piece].reshape(model, -1)
        pre = contract(low_s[...], weight, 1, 0) + vec_s[pl.ds(8 + step, 1)]
        share = 0.5 + 0.5 * lax.erf(pre * 0.7071067811865476)
        hidden = (pre * share).astype(BF)
        hidden_s[step] = hidden
        slope_s[step] = (share + pre * (0.3989422804014327 * jnp.exp(-0.5 * pre * pre))).astype(BF)
        down_s[...] += contract(hidden, feed_ref[:, 0, piece:].reshape(model, -1), 1, 1)

    @pl.when(step == tps)
    def _():
        normed, inverse = norm_parts(first_s[...] + down_s[...] + vec_s[3:4])
        out_ref[...] = (normed * vec_s[4:5] + vec_s[5:6]).astype(BF)
        grad = cot_ref[...].astype(F32)
        tail_s[0:1] = column_sum(grad * normed)
        tail_s[1:2] = column_sum(grad)
        grad_mid = norm_back(grad, vec_s[4:5], normed, inverse)
        gsum_ref[...] = grad_mid
        tail_s[2:3] = column_sum(grad_mid)
        grad_down = grad_mid.astype(BF)
        gdown_s[...] = grad_down
        gdown_t[...] = jnp.transpose(grad_down)
        down_s[...] = jnp.zeros_like(down_s)

    @pl.when(step >= tps)
    def _():
        block = 2 * tps - 1 - step
        slot = lax.rem(step, 2)

        @pl.when(step >= tps + 2)
        def _():
            send(slot, block + 2).wait()

        grad_hidden = contract(gdown_s[...], feed_ref[:, 0, piece:].reshape(model, -1), 1, 0)
        grad_pre = grad_hidden * slope_s[block].astype(F32)
        grad_low = grad_pre.astype(BF)
        tail_s[pl.ds(8 + block, 1)] = column_sum(grad_low.astype(F32))
        down_s[...] += contract(grad_low, feed_ref[:, 0, :piece].reshape(model, -1), 1, 1)
        stage_s[slot, :, :piece] = (
            contract(low_t[...], grad_low, 1, 0).astype(BF).reshape(dps, piece, -1)
        )
        stage_s[slot, :, piece:] = (
            contract(gdown_t[...], hidden_s[block], 1, 0).astype(BF).reshape(dps, piece, -1)
        )
        send(slot, block).start()

    @pl.when(step == 2 * tps - 1)
    def _():
        grad = gsum_ref[...] + down_s[...]
        normed = norm_s[...]
        grad_scale, grad_shift = column_sum(grad * normed), column_sum(grad)
        grad_sum = norm_back(grad, vec_s[1:2], normed, inv_s[:, 0:1])
        gsum_ref[...] = grad_sum
        grad_bias = column_sum(grad_sum)
        low = grad_sum.astype(BF)
        low_t[...] = jnp.transpose(low)
        for t in range(tps):
            gatt_ref[t] = contract(low, wout_s[t], 1, 0).astype(BF)
        send(lax.rem(step + 1, 2), 1).wait()
        send(lax.rem(step, 2), 0).wait()
        six = jnp.concatenate(
            [grad_bias, grad_scale, grad_shift, tail_s[2:3], tail_s[0:1], tail_s[1:2]], axis=0
        )
        for t in range(tps):
            gout = contract(low_t[...], att_ref[t], 1, 0).reshape(dps, piece, width)
            wide = [gout[:, c * part : (c + 1) * part] for c in range(chunks)]
            if chunks * width < model:
                wide.append(jnp.zeros((dps, part, model - chunks * width), F32))
            stage_s[0, :, :part] = jnp.concatenate(wide, axis=2).astype(BF)
            rows = jnp.concatenate(
                [six, tail_s[8 + t : 9 + t], jnp.zeros((PAD - 7, model), F32)], axis=0
            ).astype(BF)
            stage_s[0, :, part : part + PAD] = jnp.broadcast_to(rows[None], (dps, PAD, model))
            copy = pltpu.make_async_copy(
                stage_s.at[0, :, pl.ds(0, part + PAD)],
                pack_ref.at[:, t, pl.ds(feed_rows, part + PAD)],
                sems.at[0],
            )
            copy.start()
            copy.wait()


def middle(att, tokens, cotangent, gathered):
    tps, rows, width = att.shape
    model = tokens.shape[1]
    dps, wide = gathered.shape[0], gathered.shape[3]
    piece = model // dps
    chunks = min(model // width, piece // PAD)
    pack_rows = 2 * piece + piece // chunks + PAD

    def fixed(array):
        rank = len(array.shape)
        return pl.BlockSpec(
            array.shape, lambda i: (0,) * rank, pipeline_mode=pl.Buffered(buffer_count=1)
        )

    def feed_at(i):
        return (0, jnp.minimum(i, 2 * tps - 1 - i), 0, 0)

    outs = [
        jax.ShapeDtypeStruct((rows, model), BF),
        jax.ShapeDtypeStruct((rows, model), F32),
        jax.ShapeDtypeStruct(att.shape, BF),
        jax.ShapeDtypeStruct((dps, tps, pack_rows, model), BF),
    ]
    return pl.pallas_call(
        lambda *refs: middle_kernel((dps, tps, piece, chunks), *refs),
        grid=(2 * tps,),
        in_specs=[fixed(a) for a in (att, tokens, cotangent)]
        + [
            pl.BlockSpec(memory_space=pl.ANY),
            pl.BlockSpec((dps, 1, 2 * piece, wide), feed_at),
        ],
        out_specs=[fixed(a) for a in outs[:3]] + [pl.BlockSpec(memory_space=pl.ANY)],
        out_shape=outs,
        scratch_shapes=[
            pltpu.VMEM((rows, model), F32),
            pltpu.VMEM((rows, model), F32),
            pltpu.VMEM((rows, model), F32),
            pltpu.VMEM((rows, 128), F32),
            pltpu.VMEM((rows, model), BF),
            pltpu.VMEM((model, rows), BF),
            pltpu.VMEM((rows, model), BF),
            pltpu.VMEM((model, rows), BF),
            pltpu.VMEM((tps, rows, wide), BF),
            pltpu.VMEM((tps, rows, wide), BF),
            pltpu.VMEM((2, dps, 2 * piece, model), BF),
            pltpu.VMEM((16, model), F32),
            pltpu.VMEM((2, dps, piece // chunks + PAD, wide), BF),
            pltpu.VMEM((tps, model, width), BF),
            pltpu.VMEM((16, model), F32),
            pltpu.SemaphoreType.DMA((2,)),
            pltpu.SemaphoreType.DMA((2,)),
        ],
        cost_estimate=pl.CostEstimate(
            flops=6 * rows * model * model * (2 * tps + 1),
            bytes_accessed=60 << 20,
            transcendentals=0,
        ),
        compiler_params=pltpu.CompilerParams(vmem_limit_bytes=62 << 20),
        name="middle",
    )(att, tokens, cotangent, gathered, gathered)


def on_device(
    tokens,
    weight_query,
    weight_key,
    weight_value,
    weight_out,
    bias_query,
    bias_value,
    bias_out,
    first_scale,
    first_shift,
    weight_hidden,
    bias_hidden,
    weight_down,
    bias_down,
    second_scale,
    second_shift,
    cotangent,
):
    dps, tps = lax.axis_size("dp"), lax.axis_size("tensor")
    rows, model = tokens.shape
    piece = weight_hidden.shape[0]
    width = weight_query.shape[1]
    small = bias_query.shape[0]

    place = lax.axis_index("dp")

    def placed(pieces, length):
        zeros = jnp.zeros((pieces.shape[0], length), BF)
        return lax.dynamic_update_slice_in_dim(zeros, pieces, place * pieces.shape[1], 1)

    vec_rows = placed(
        jnp.stack(
            [bias_out, first_scale, first_shift, bias_down, second_scale, second_shift, bias_hidden]
        ),
        model,
    )
    packed_weights = pack_weights(
        weight_hidden, weight_down, weight_out, jnp.pad(vec_rows, ((0, PAD - 7), (0, 0)))
    )
    bias_rows = placed(jnp.stack([bias_query, bias_value]), width)
    bias_row = jnp.concatenate([bias_rows[0:1], jnp.zeros((1, width), BF), bias_rows[1:2]], axis=1)
    attn_pack = jnp.concatenate(
        [
            jnp.concatenate([weight_query, weight_key, weight_value], axis=1),
            jnp.pad(bias_row, ((0, PAD - 1), (0, 0))),
        ],
        axis=0,
    )
    rows_full, packs, qkv, attended, logsum, crossed, gathered = forward(
        tokens, attn_pack, packed_weights, dps, tps
    )
    output, grad_sum, grad_cross, packed = middle(crossed, tokens, cotangent, gathered)
    scatter = dps == 8 and tps == 4 and width == 2 * PAIR
    grad_tokens, attn_grads, summed = backward(
        grad_cross, packed, qkv, attended, logsum, rows_full, packs, grad_sum, scatter
    )
    if scatter:
        packed = summed
    else:
        packed = lax.psum_scatter(packed, "dp", scatter_dimension=0, tiled=False)
        packed = lax.psum_scatter(packed, "tensor", scatter_dimension=0, tiled=False).astype(F32)

    def share(values, count):
        return lax.dynamic_slice_in_dim(values, place * count, count, 0)

    chunks = min(model // width, piece // PAD)
    part = piece // chunks
    out_grad = packed[2 * piece : 2 * piece + part, : chunks * width]
    out_grad = out_grad.reshape(part, chunks, width).transpose(2, 1, 0).reshape(width, piece)
    vec_grads = [share(packed[2 * piece + part + i], piece) for i in range(6)]
    hidden_grad = share(packed[2 * piece + part + 6], bias_hidden.shape[0])
    return (
        output,
        grad_tokens,
        attn_grads[:piece, :width],
        attn_grads[:piece, width : 2 * width],
        attn_grads[:piece, 2 * width :],
        out_grad,
        share(attn_grads[piece, :width], small),
        share(attn_grads[piece, 2 * width :], small),
        vec_grads[0],
        vec_grads[1],
        vec_grads[2],
        packed[:piece],
        hidden_grad,
        packed[piece : 2 * piece].T,
        vec_grads[3],
        vec_grads[4],
        vec_grads[5],
    )


def solution(mesh):
    placed = (
        P(("dp", "tensor"), None),
        P("dp", "tensor"),
        P("dp", "tensor"),
        P("dp", "tensor"),
        P("tensor", "dp"),
        P(("tensor", "dp")),
        P(("tensor", "dp")),
        P("dp"),
        P("dp"),
        P("dp"),
        P("dp", "tensor"),
        P(("tensor", "dp")),
        P("tensor", "dp"),
        P("dp"),
        P("dp"),
        P("dp"),
        P(("dp", "tensor"), None),
    )
    return jax.shard_map(
        on_device,
        mesh=mesh,
        in_specs=placed,
        out_specs=(
            P(("dp", "tensor"), None),
            P(("dp", "tensor"), None),
            P("dp", "tensor"),
            P("dp", "tensor"),
            P("dp", "tensor"),
            P("tensor", "dp"),
            P(("tensor", "dp")),
            P(("tensor", "dp")),
            P("dp"),
            P("dp"),
            P("dp"),
            P("dp", "tensor"),
            P(("tensor", "dp")),
            P("tensor", "dp"),
            P("dp"),
            P("dp"),
            P("dp"),
        ),
        check_vma=False,
    )
```

```python
import jax
import jax.numpy as jnp
from jax import lax
from jax.experimental import pallas as pl
from jax.experimental.pallas import tpu as pltpu
from jax.sharding import PartitionSpec as P

HD = 64
PAIR = 2 * HD
PAD = 16
F32 = jnp.float32
BF = jnp.bfloat16


def contract(left, right, left_dim, right_dim):
    return lax.dot_general(
        left, right, (((left_dim,), (right_dim,)), ((), ())), preferred_element_type=F32
    )


def one_head(pair, head):
    lane = lax.broadcasted_iota(jnp.int32, pair.shape, 1)
    keep = lane < HD if head == 0 else lane >= HD
    return jnp.where(keep, pair, jnp.zeros_like(pair))


CUTS = 4


def flipped(index, bit):
    size = 1 << bit
    return index + size - 2 * size * lax.rem(index // size, 2)


def greet(dps, tps):
    place, level = lax.axis_index("dp"), lax.axis_index("tensor")
    barrier = pltpu.get_barrier_semaphore()
    bits = range(1, dps.bit_length() - 1)
    for bit in bits:
        pl.semaphore_signal(barrier, inc=1, device_id={"dp": flipped(place, bit)})
    pl.semaphore_signal(barrier, inc=1, device_id={"dp": flipped(place, 0)})
    for step in range(1, tps):
        other = lax.rem(level + step, tps)
        pl.semaphore_signal(barrier, inc=1, device_id={"tensor": other})
        pl.semaphore_signal(barrier, inc=1, device_id={"dp": flipped(place, 0), "tensor": other})
    pl.semaphore_wait(barrier, len(bits) + 2 * tps - 1)


def seat(place, level):
    core = lax.rem(place, 2)
    group = level // 2
    gate = lax.rem((level + 1) // 2, 2)
    mate = level + 1 - 2 * lax.rem(level, 2)
    near, far = 2 - group, 3 - 3 * group
    heads = lax.rem(level + 2 * core, 4)
    return core, group, gate, mate, near, far, heads


def ordered(level, step):
    group = level // 2
    gate = lax.rem((level + 1) // 2, 2)
    turned = step + gate * (step // 2) * (5 - 2 * step)
    return (1 - group) * (3 - turned) + group * turned


def forward_kernel(
    dps,
    tps,
    tok_ref,
    pack_ref,
    mine_ref,
    rows_ref,
    packs_ref,
    qkv_ref,
    att_ref,
    lse_ref,
    cross_ref,
    gath_ref,
    weight_s,
    away_sem,
    mate_sem,
    core_sem,
    land_sem,
    pack_send,
    pack_land,
    local_sem,
    level_send,
    near_send,
    level_land,
    plane_send,
    plane_land,
    cross_send,
    cross_land,
):
    place, level = lax.axis_index("dp"), lax.axis_index("tensor")
    rows, model = tok_ref.shape
    piece = model // dps
    width = pack_ref.shape[1] // 3
    pairs = width // PAIR
    cut = rows // CUTS
    count = mine_ref.shape[0]
    middle_row = count // (2 * PAD) * PAD
    spans = (pl.ds(0, middle_row), pl.ds(middle_row, count - middle_row))
    bits = tuple(range(1, dps.bit_length() - 1))
    orders = (bits, bits[::-1])
    core, group, gate, mate, near, far, heads = seat(place, level)
    lead = core == group
    partner = flipped(place, 0)
    own = pltpu.make_async_copy(tok_ref, rows_ref.at[level], local_sem.at[0])
    own_pack = pltpu.make_async_copy(pack_ref, packs_ref.at[place], local_sem.at[1])
    own_block = pltpu.make_async_copy(mine_ref, gath_ref.at[place, level], local_sem.at[2])
    own_block.start()

    @pl.when(lead)
    def _():
        own.start()

    @pl.when(core == 0)
    def _():
        own_pack.start()

    greet(dps, tps)

    def away(chunk):
        span = pl.ds(chunk * cut, cut)
        return pltpu.make_async_remote_copy(
            src_ref=tok_ref.at[span],
            dst_ref=rows_ref.at[level, span],
            send_sem=away_sem.at[chunk],
            recv_sem=land_sem.at[level, chunk],
            device_id={"tensor": near},
        )

    def to_mate(block, chunk, first=False):
        span = pl.ds(chunk * cut, cut)
        return pltpu.make_async_remote_copy(
            src_ref=tok_ref.at[span] if first else rows_ref.at[block, span],
            dst_ref=rows_ref.at[block, span],
            send_sem=mate_sem.at[block, chunk],
            recv_sem=land_sem.at[block, chunk],
            device_id={"tensor": mate},
        )

    def to_core(block, chunk, first=False):
        span = pl.ds(chunk * cut, cut)
        return pltpu.make_async_remote_copy(
            src_ref=tok_ref.at[span] if first else rows_ref.at[block, span],
            dst_ref=rows_ref.at[block, span],
            send_sem=core_sem.at[block, chunk],
            recv_sem=land_sem.at[block, chunk],
            device_id={"dp": partner},
        )

    line = (level, mate, near, far)

    def level_hop(at, half, inward, mine=False):
        return pltpu.make_async_remote_copy(
            src_ref=mine_ref.at[spans[half]] if mine else gath_ref.at[place, at, spans[half]],
            dst_ref=gath_ref.at[place, at, spans[half]],
            send_sem=(near_send if inward else level_send).at[at, half],
            recv_sem=level_land.at[at, half],
            device_id={"tensor": near if inward else mate},
        )

    def in_plane(block, step, half, bit, number, mine=False):
        at = line[step]
        return pltpu.make_async_remote_copy(
            src_ref=mine_ref.at[spans[half]] if mine else gath_ref.at[block, at, spans[half]],
            dst_ref=gath_ref.at[block, at, spans[half]],
            send_sem=plane_send.at[number, step, half],
            recv_sem=plane_land.at[block, step, half],
            device_id={"dp": flipped(place, bit)},
        )

    def held(half, stage):
        blocks = [place]
        for bit in orders[half][:stage]:
            blocks = blocks + [flipped(block, bit) for block in blocks]
        return blocks

    def numbered(half):
        found, at = [], 0
        for stage in range(len(bits) + 1):
            for block in held(half, stage)[(1 << stage) // 2 if stage else 0 :]:
                targets = list(orders[half][stage:]) + [0]
                found.append((stage, block, [(bit, at + i) for i, bit in enumerate(targets)]))
                at += len(targets)
        return found

    tables = (numbered(0), numbered(1))

    def pass_on(step, stage):
        for half in range(2):
            for came, block, targets in tables[half]:
                if came != stage:
                    continue
                if stage:
                    in_plane(block, step, half, 0, 0).wait_recv()
                for bit, number in targets:
                    in_plane(block, step, half, bit, number, step == 0 and stage == 0).start()

    def level_in(step):
        for half in range(2):
            level_hop(line[step], half, False).wait_recv()

            @pl.when(gate == 1)
            def _():
                level_hop(line[step], half, step == 1).start()

    even = place - core
    opposite = lax.rem(level + 2, tps)

    def pack_to(index, block, device):
        return pltpu.make_async_remote_copy(
            src_ref=pack_ref,
            dst_ref=packs_ref.at[block],
            send_sem=pack_send.at[index],
            recv_sem=pack_land.at[block],
            device_id=device,
        )

    pack_to(0, place, {"dp": even + 1, "tensor": opposite}).start()
    for half in range(2):
        level_hop(level, half, False, True).start()

        @pl.when(gate == 1)
        def _():
            level_hop(level, half, True, True).start()

    for chunk in range(CUTS):

        @pl.when(lead)
        def _():
            to_mate(level, chunk, True).start()
            to_core(level, chunk, True).start()

        @pl.when(core != group)
        def _():
            away(chunk).start()

    pass_on(0, 0)

    @pl.when(core == 1)
    def _():
        pack_to(1, place, {"dp": even}).start()
        pack_to(0, even, {"dp": even}).wait_recv()

    @pl.when(core == 0)
    def _():
        own_pack.wait()

    pack_to(0, even + 1, {"dp": even}).wait_recv()

    def pack_on(block, index, bit):
        return pltpu.make_async_remote_copy(
            src_ref=packs_ref.at[block],
            dst_ref=packs_ref.at[block],
            send_sem=pack_send.at[index],
            recv_sem=pack_land.at[block],
            device_id={"dp": flipped(place, bit)},
        )

    known = [even, even + 1]
    sent = 2
    pack_sends = []
    for bit in bits:
        for block in known:
            pack_on(block, sent, bit).start()
            pack_sends.append((block, sent, bit))
            sent += 1
        more = [flipped(block, bit) for block in known]
        for block in more:
            pack_on(block, 0, bit).wait_recv()
        known = known + more
    weight_s[...] = packs_ref[:, :piece].reshape(weight_s.shape)
    bias = jnp.sum(packs_ref[:, piece : piece + PAD].astype(F32), axis=0)[0:1]

    def project(block):
        qkv_ref[block] = (contract(rows_ref[block], weight_s[...], 1, 0) + bias).astype(BF)

    def advance(step, stage):
        if step and stage == 0:
            level_in(step)
        pass_on(step, stage)

    @pl.when(lead)
    def _():
        own.wait()

    for index, block in enumerate((level, mate, near, far)):
        for chunk in range(CUTS):
            if index:

                @pl.when(lead)
                def _():
                    to_core(block, chunk).wait_recv()

                if index > 1:

                    @pl.when(lead & (gate == 1))
                    def _():
                        to_mate(block, chunk).start()

                @pl.when(lead)
                def _():
                    to_core(block, chunk).start()

            @pl.when(core != group)
            def _():
                to_core(block, chunk).wait_recv()

        project(block)
        for step, stage in (((0, 1),), ((1, 0),), ((0, 2), (2, 0)), ((1, 1),))[index]:
            advance(step, stage)
    for stage in range(3, len(bits) + 1):
        pass_on(0, stage)

    half_rows = rows // 2

    def cross(target, half):
        span = pl.ds(half * half_rows, half_rows)
        return pltpu.make_async_remote_copy(
            src_ref=att_ref.at[target, span],
            dst_ref=cross_ref.at[heads, span],
            send_sem=cross_send.at[target, half],
            recv_sem=cross_land.at[heads, half],
            device_id={"dp": even + group, "tensor": target},
        )

    turns = 2 * pairs * tps

    def attend(turn, carry):
        pair = lax.rem(turn, pairs)
        half = lax.rem(turn // pairs, 2)
        target = ordered(level, turn // (2 * pairs))
        span = pl.ds(pl.multiple_of(half * half_rows, half_rows), half_rows)
        lanes = pl.ds(pl.multiple_of(pair * PAIR, PAIR), PAIR)
        query = qkv_ref[target, span, lanes] * jnp.asarray(0.125, BF)
        key = qkv_ref[:, :, pl.ds(pl.multiple_of(width + pair * PAIR, PAIR), PAIR)]
        value = qkv_ref[:, :, pl.ds(pl.multiple_of(2 * width + pair * PAIR, PAIR), PAIR)]
        key, value = key.reshape(tps * rows, PAIR), value.reshape(tps * rows, PAIR)
        total, columns = None, []
        for head in range(2):
            scores = contract(query, one_head(key, head), 1, 1)
            highest = jnp.max(scores, axis=1, keepdims=True)
            expons = jnp.exp(scores - highest)
            mass = jnp.sum(expons, axis=1, keepdims=True)
            part = contract(expons.astype(BF), one_head(value, head), 1, 0) / mass
            total = part if total is None else total + part
            columns.append(jnp.broadcast_to(highest + jnp.log(mass), (half_rows, PAIR)))
        att_ref[target, span, lanes] = total.astype(BF)
        where = pl.ds(pl.multiple_of(target * rows + half * half_rows, half_rows), half_rows)
        lse_ref[pair, :, where] = jnp.concatenate(
            [jnp.transpose(column)[:4] for column in columns], axis=0
        )

        @pl.when((pair == pairs - 1) & ((turn < 2 * pairs * (tps - 1)) | (core != group)))
        def _():
            cross(target, half).start()

        for at, batch in events.items():

            @pl.when(turn == at)
            def _():
                for step, stage in batch:
                    advance(step, stage)

        return carry

    events = {1: [(2, 1)], turns // 4: [(1, 2), (3, 0)], turns // 2: [(2, 2)], turns - 4: [(3, 1)], turns - 1: [(3, 2)]}
    early = [item for batch in events.values() for item in batch]
    early = early + [item for batch in (((0, 1),), ((1, 0),), ((0, 2), (2, 0)), ((1, 1),)) for item in batch]
    late = [
        (step, stage)
        for step in range(1, tps)
        for stage in range(len(bits) + 1)
        if (step, stage) not in early
    ]
    lax.fori_loop(0, turns, attend, 0)
    own_cross = pltpu.make_async_copy(att_ref.at[level], cross_ref.at[heads], local_sem.at[3])

    @pl.when(lead)
    def _():
        own_cross.start()

    for step, stage in sorted(late, key=lambda item: (item[0] + item[1], item[0])):
        advance(step, stage)
    for index in range(tps):
        for half in range(2):

            @pl.when((core != group) | (index != heads))
            def _():
                pltpu.make_async_remote_copy(
                    src_ref=att_ref.at[level, pl.ds(half * half_rows, half_rows)],
                    dst_ref=cross_ref.at[index, pl.ds(half * half_rows, half_rows)],
                    send_sem=cross_send.at[index, half],
                    recv_sem=cross_land.at[index, half],
                    device_id={"tensor": mate},
                ).wait_recv()

            @pl.when((core != group) | (index != level))
            def _():
                cross(index, half).wait_send()

    for step in range(tps):
        for half in range(2):
            for stage, block, targets in tables[half]:
                in_plane(flipped(block, 0), step, half, 0, 0).wait_recv()
                for bit, number in targets:
                    in_plane(block, step, half, bit, number).wait_send()
    for half in range(2):
        level_hop(level, half, False).wait_send()

        @pl.when(gate == 1)
        def _():
            level_hop(level, half, True).wait_send()
            level_hop(mate, half, True).wait_send()
            level_hop(near, half, False).wait_send()
            level_hop(far, half, False).wait_send()

    own_block.wait()
    pack_to(0, place, {"dp": even + 1, "tensor": opposite}).wait_send()

    @pl.when(core == 1)
    def _():
        pack_to(1, place, {"dp": even}).wait_send()

    for block, index, bit in pack_sends:
        pack_on(block, index, bit).wait_send()

    @pl.when(lead)
    def _():
        own_cross.wait()

    for chunk in range(CUTS):

        @pl.when(core != group)
        def _():
            away(chunk).wait_send()

        for index, block in enumerate((level, mate, near, far)):

            @pl.when(lead)
            def _():
                to_core(block, chunk).wait_send()

            if index == 0:

                @pl.when(lead)
                def _():
                    to_mate(block, chunk).wait_send()

            if index > 1:

                @pl.when(lead & (gate == 1))
                def _():
                    to_mate(block, chunk).wait_send()


def forward(tokens, pack, mine, dps, tps):
    rows, model = tokens.shape
    columns = pack.shape[1]
    width = columns // 3
    vmem = pl.BlockSpec(memory_space=pltpu.VMEM)
    hbm = pl.BlockSpec(memory_space=pl.ANY)
    dma = pltpu.SemaphoreType.DMA
    return pl.pallas_call(
        lambda *refs: forward_kernel(dps, tps, *refs),
        in_specs=[vmem, vmem, hbm],
        out_specs=[vmem] * 5 + [hbm] * 2,
        out_shape=[
            jax.ShapeDtypeStruct((tps, rows, model), BF),
            jax.ShapeDtypeStruct((dps,) + pack.shape, BF),
            jax.ShapeDtypeStruct((tps, rows, columns), BF),
            jax.ShapeDtypeStruct((tps, rows, width), BF),
            jax.ShapeDtypeStruct((width // PAIR, 8, tps * rows), F32),
            jax.ShapeDtypeStruct((tps, rows, width), BF),
            jax.ShapeDtypeStruct((dps, tps) + mine.shape, BF),
        ],
        scratch_shapes=[
            pltpu.VMEM((model, columns), BF),
            dma((CUTS,)),
            dma((tps, CUTS)),
            dma((tps, CUTS)),
            dma((tps, CUTS)),
            dma((dps,)),
            dma((dps,)),
            dma((4,)),
            dma((tps, 2)),
            dma((tps, 2)),
            dma((tps, 2)),
            dma((dps - 1, tps, 2)),
            dma((dps, tps, 2)),
            dma((tps, 2)),
            dma((tps, 2)),
        ],
        cost_estimate=pl.CostEstimate(
            flops=2 * tps * rows * model * columns, bytes_accessed=200 << 20, transcendentals=0
        ),
        compiler_params=pltpu.CompilerParams(
            vmem_limit_bytes=50 << 20, collective_id=1, has_side_effects=True
        ),
        name="forward",
    )(tokens, pack, mine)


def backward_kernel(
    dps,
    tps,
    scatter,
    cross_ref,
    packed_ref,
    qkv_ref,
    att_ref,
    lse_ref,
    rows_ref,
    packs_ref,
    gsum_ref,
    tok_out,
    pack_out,
    feed_out,
    grad_s,
    weight_s,
    dq_s,
    dk_s,
    dv_s,
    land_s,
    other_s,
    mine_s,
    theirs_s,
    gsum_s,
    kept_s,
    stage_s,
    one_a,
    one_b,
    two_a,
    two_b,
    level_s,
    local_sem,
    grad_send,
    grad_land,
    core_send,
    core_land,
    hop_send,
    hop_land,
    pack_send,
    pack_land,
    chip_send,
    chip_land,
    stage_sem,
    one_send,
    one_land,
    two_send,
    two_land,
    level_send,
    level_land,
):
    place, level = lax.axis_index("dp"), lax.axis_index("tensor")
    rows, model = gsum_ref.shape
    piece = model // dps
    width = att_ref.shape[2]
    pairs = width // PAIR
    cut = rows // CUTS
    half_rows = rows // 2
    count = packed_ref.shape[2]
    middle_row = count // (2 * PAD) * PAD
    spans = (pl.ds(0, middle_row), pl.ds(middle_row, count - middle_row))

    load_weight = pltpu.make_async_copy(
        packs_ref.at[:, pl.ds(0, piece)], weight_s, local_sem.at[0]
    )
    load_sum = pltpu.make_async_copy(gsum_ref, gsum_s, local_sem.at[1])
    core, group, gate, mate, near, far, heads = seat(place, level)
    lead = core == group
    even = place - core
    opposite = lax.rem(level + 2, tps)
    own_grad = pltpu.make_async_copy(cross_ref.at[heads], grad_s.at[level], local_sem.at[2])
    load_weight.start()
    load_sum.start()

    @pl.when(lead)
    def _():
        own_grad.start()

    greet(dps, tps)

    def cross(index):
        other = lax.rem(index // 2 + core, 2)
        return pltpu.make_async_remote_copy(
            src_ref=cross_ref.at[index],
            dst_ref=grad_s.at[level],
            send_sem=grad_send.at[index],
            recv_sem=grad_land.at[level],
            device_id={"dp": even + other, "tensor": lax.rem(index + 2 * other, tps)},
        )

    def crossed(block):
        return pltpu.make_async_remote_copy(
            src_ref=cross_ref.at[block],
            dst_ref=grad_s.at[block],
            send_sem=grad_send.at[block],
            recv_sem=grad_land.at[block],
            device_id={"tensor": mate},
        )

    for index in range(tps):

        @pl.when((core != group) | (index != heads))
        def _():
            cross(index).start()

    def block_of(kind):
        block = place
        if kind in (0, 2):
            block = flipped(block, 1)
        if kind in (0, 1):
            block = flipped(block, 2)
        return block

    def level_of(turn):
        return ordered(level, turn)

    def chip(kind, turn):
        return pltpu.make_async_remote_copy(
            src_ref=packed_ref.at[flipped(block_of(kind), 0), level_of(turn)],
            dst_ref=kept_s.at[turn * 4 + kind],
            send_sem=chip_send.at[turn * 4 + kind],
            recv_sem=chip_land.at[turn * 4 + kind],
            device_id={"dp": flipped(place, 0)},
        )

    def load(kind, turn, slot):
        return pltpu.make_async_copy(
            packed_ref.at[block_of(kind), level_of(turn)], stage_s.at[slot], stage_sem.at[slot]
        )

    def plane_one(kind, turn, half):
        bit = 2 - half
        target = one_b if half else one_a
        at = turn * 2 + (0 if kind == 0 else 1)
        return pltpu.make_async_remote_copy(
            src_ref=kept_s.at[turn * 4 + kind, spans[half]],
            dst_ref=target.at[at],
            send_sem=one_send.at[at, half],
            recv_sem=one_land.at[at, half],
            device_id={"dp": flipped(place, bit)},
        )

    def plane_two(turn, half):
        bit = 1 + half
        target = two_b if half else two_a
        return pltpu.make_async_remote_copy(
            src_ref=kept_s.at[turn * 4 + 2 - half, spans[half]],
            dst_ref=target.at[turn],
            send_sem=two_send.at[turn, half],
            recv_sem=two_land.at[turn, half],
            device_id={"dp": flipped(place, bit)},
        )

    def along_z(turn, slot, device):
        return pltpu.make_async_remote_copy(
            src_ref=kept_s.at[turn * 4 + 3],
            dst_ref=level_s.at[slot],
            send_sem=level_send.at[turn],
            recv_sem=level_land.at[slot],
            device_id={"tensor": device},
        )

    def through_z(turn):
        @pl.when(gate == 1)
        def _():
            along_z(turn, turn, mate).wait_recv()
            at = turn * 4 + 3
            kept_s[at] = (kept_s[at].astype(F32) + level_s[turn].astype(F32)).astype(BF)
            if turn == 2:
                along_z(turn, 3, mate).start()
            else:
                along_z(turn, 2 + turn, near).start()

    def add_to(slot, half, source):
        kept_s[slot, spans[half]] = (
            kept_s[slot, spans[half]].astype(F32) + source.astype(F32)
        ).astype(BF)

    def chip_in(kind, turn):
        slot = kind % 2
        load(kind, turn, slot).wait()
        chip(kind, turn).wait_recv()
        at = turn * 4 + kind
        kept_s[at] = (kept_s[at].astype(F32) + stage_s[slot].astype(F32)).astype(BF)
        if kind in (0, 1):
            plane_one(kind, turn, 0).start()
        if kind in (0, 2):
            plane_one(kind, turn, 1).start()

    def one_in(turn):
        plane_one(0, turn, 0).wait_recv()
        add_to(turn * 4 + 2, 0, one_a[turn * 2])
        plane_two(turn, 0).start()
        plane_one(0, turn, 1).wait_recv()
        add_to(turn * 4 + 1, 1, one_b[turn * 2])
        plane_two(turn, 1).start()
        plane_one(1, turn, 0).wait_recv()
        add_to(turn * 4 + 3, 0, one_a[turn * 2 + 1])
        plane_one(2, turn, 1).wait_recv()
        add_to(turn * 4 + 3, 1, one_b[turn * 2 + 1])

    def two_in(turn):
        plane_two(turn, 0).wait_recv()
        add_to(turn * 4 + 3, 0, two_a[turn])
        plane_two(turn, 1).wait_recv()
        add_to(turn * 4 + 3, 1, two_b[turn])
        if turn < tps - 1:

            @pl.when(gate == 0)
            def _():
                along_z(turn, 4 if turn == 2 else turn, mate).start()

    if scatter:
        load(0, 0, 0).start()
        for turn in range(tps):
            for kind in range(4):
                chip(kind, turn).start()

    dk_s[...] = jnp.zeros_like(dk_s)
    dv_s[...] = jnp.zeros_like(dv_s)

    @pl.when(lead)
    def _():
        own_grad.wait()

    def attend(turn, carry):
        pair = lax.rem(turn, pairs)
        half = lax.rem(turn // pairs, 2)
        step = turn // (2 * pairs)
        target = ordered(level, tps - 1 - step)

        @pl.when((lax.rem(turn, 2 * pairs) == 0) & ((step > 0) | (core != group)))
        def _():
            crossed(target).wait_recv()

        span = pl.ds(pl.multiple_of(half * half_rows, half_rows), half_rows)
        lanes = pl.ds(pl.multiple_of(pair * PAIR, PAIR), PAIR)
        query = qkv_ref[target, span, lanes] * jnp.asarray(0.125, BF)
        key = qkv_ref[:, :, pl.ds(pl.multiple_of(width + pair * PAIR, PAIR), PAIR)]
        value = qkv_ref[:, :, pl.ds(pl.multiple_of(2 * width + pair * PAIR, PAIR), PAIR)]
        key, value = key.reshape(tps * rows, PAIR), value.reshape(tps * rows, PAIR)
        grad = grad_s[target, span, lanes]
        products = jnp.transpose(grad.astype(F32) * att_ref[target, span, lanes].astype(F32))
        where = pl.ds(pl.multiple_of(target * rows + half * half_rows, half_rows), half_rows)
        logsums = lse_ref[pair, :, where]
        grad_query = None
        for head in range(2):
            key_head, value_head = one_head(key, head), one_head(value, head)
            inner = jnp.sum(products[HD * head : HD * head + HD], axis=0, keepdims=True)
            logsum = logsums[4 * head : 4 * head + 1]
            probs = jnp.exp(contract(key_head, query, 1, 1) - logsum)
            grad_probs = contract(value_head, grad, 1, 1)
            grad_scores = (probs * (grad_probs - inner)).astype(BF)
            dv_s[:, lanes] += contract(probs.astype(BF), one_head(grad, head), 1, 0)
            dk_s[:, lanes] += contract(grad_scores, one_head(query, head), 1, 0)
            part = contract(grad_scores, key_head, 0, 0)
            grad_query = part if grad_query is None else grad_query + part
        dq_s[where, lanes] = (grad_query * 0.125).astype(BF)

        if scatter:
            for kind in range(4):

                @pl.when(lax.rem(turn, 4) == kind)
                def _():
                    if kind < 3:
                        load(kind + 1, turn // 4, (kind + 1) % 2).start()
                    else:

                        @pl.when(turn // 4 < tps - 1)
                        def _():
                            load(0, turn // 4 + 1, 0).start()

                    chip_in(kind, turn // 4)

            @pl.when(turn == 9)
            def _():
                one_in(0)

            @pl.when(turn == 13)
            def _():
                two_in(0)

            @pl.when(turn == 15)
            def _():
                one_in(1)

        return carry

    lax.fori_loop(0, 2 * pairs * tps, attend, 0)
    load_weight.wait()
    refs = (dq_s, dk_s, dv_s)

    def rows_of(block):
        span = pl.ds(pl.multiple_of(block * rows, rows), rows)
        total = None
        for index, ref in enumerate(refs):
            weight = weight_s[:, :, index * width : (index + 1) * width].reshape(model, width)
            part = contract(ref[span].astype(BF), weight, 1, 1)
            total = part if total is None else total + part
        return total

    def to_core(block, chunk):
        span = pl.ds(chunk * cut, cut)
        return pltpu.make_async_remote_copy(
            src_ref=land_s.at[block, span],
            dst_ref=land_s.at[block, span],
            send_sem=core_send.at[block, chunk],
            recv_sem=core_land.at[block, chunk],
            device_id={"dp": flipped(place, 0)},
        )

    def onward(block, chunk, slot, device):
        span = pl.ds(chunk * cut, cut)
        return pltpu.make_async_remote_copy(
            src_ref=land_s.at[block, span],
            dst_ref=other_s.at[slot, span],
            send_sem=hop_send.at[block, chunk],
            recv_sem=hop_land.at[slot, chunk],
            device_id={"tensor": device},
        )

    order_of = (far, near, mate, level)

    def part_out(index, carry):
        block = ordered(level, index)
        land_s[block] = rows_of(block).astype(BF)
        for chunk in range(CUTS):
            to_core(block, chunk).start()
        return carry

    def chip_total(block, chunk, own):
        to_core(block, chunk).wait_recv()
        span = pl.ds(chunk * cut, cut)
        return land_s[block, span].astype(F32) + own[chunk * cut : (chunk + 1) * cut]

    def part_on(index, carry):
        block = ordered(level, index)
        own = rows_of(block)
        for chunk in range(CUTS):
            land_s[block, pl.ds(chunk * cut, cut)] = chip_total(block, chunk, own).astype(BF)
            onward(block, chunk, index, mate).start()
        return carry

    def part_through(index, carry):
        block = ordered(level, index)
        own = rows_of(block)
        for chunk in range(CUTS):
            span = pl.ds(chunk * cut, cut)
            total = chip_total(block, chunk, own)
            onward(block, chunk, index, block).wait_recv()
            land_s[block, span] = (total + other_s[index, span].astype(F32)).astype(BF)
            onward(block, chunk, 2, block).start()
        return carry

    def part_own():
        own = rows_of(level)
        for chunk in range(CUTS):
            land_s[level, pl.ds(chunk * cut, cut)] = chip_total(level, chunk, own).astype(BF)

    inner = lead & (gate == 1)

    @pl.when(core != group)
    def _():
        lax.fori_loop(0, tps, part_out, 0)

    @pl.when(lead)
    def _():
        lax.fori_loop(2 * gate, 3, part_on, 0)

    tail = jnp.concatenate(
        [jnp.sum(ref[...].astype(BF).astype(F32), axis=0, keepdims=True) for ref in refs], axis=1
    )
    tokens = rows_ref.reshape(tps * rows, model)
    for index, ref in enumerate(refs):
        grad = contract(tokens[...], ref[...].astype(BF), 0, 0).astype(BF)
        mine_s[:, :piece, index * width : (index + 1) * width] = grad.reshape(dps, piece, width)
    mine_s[:, piece:] = jnp.broadcast_to(tail.astype(BF)[None], (dps, PAD, 3 * width))

    def exchange(index, bit, other):
        return pltpu.make_async_remote_copy(
            src_ref=mine_s.at[other],
            dst_ref=theirs_s.at[index],
            send_sem=pack_send.at[index],
            recv_sem=pack_land.at[index],
            device_id={"dp": flipped(place, bit)},
        )

    plane = tuple(range(1, dps.bit_length() - 1))[::-1]

    def kept(done):
        blocks = [even, even + 1]
        for bit in plane[done:][::-1]:
            blocks = blocks + [flipped(block, bit) for block in blocks]
        return blocks

    starts, at = [], 0
    for done in range(len(plane)):
        starts.append(at)
        at += dps >> (done + 1)

    def pack_start(done):
        for index, block in enumerate(kept(done + 1)):
            exchange(starts[done] + index, plane[done], flipped(block, plane[done])).start()

    def pack_finish(done):
        for index, block in enumerate(kept(done + 1)):
            exchange(starts[done] + index, plane[done], block).wait()
            mine_s[block] = (
                mine_s[block].astype(F32) + theirs_s[starts[done] + index].astype(F32)
            ).astype(BF)

    def pack_home(block, slot, device):
        return pltpu.make_async_remote_copy(
            src_ref=mine_s.at[block],
            dst_ref=theirs_s.at[slot],
            send_sem=pack_send.at[lax.rem(block, 2) + dps - 2],
            recv_sem=pack_land.at[slot],
            device_id=device,
        )

    def homeward():
        @pl.when(core == 0)
        def _():
            pack_home(even + 1, dps - 1, {"dp": even + 1}).start()

        @pl.when(core == 1)
        def _():
            pack_home(even, dps - 2, {"dp": even, "tensor": opposite}).start()
            pack_home(even + 1, dps - 2, {"tensor": opposite}).start()

    pack_start(0)
    if scatter:
        through_z(0)
        two_in(1)
        one_in(2)

    @pl.when(inner)
    def _():
        lax.fori_loop(0, 2, part_through, 0)

    @pl.when(lead)
    def _():
        part_own()

    if scatter:
        through_z(1)
        one_in(3)
        two_in(2)
        through_z(2)
        two_in(3)

    stages = len(plane)
    for turn in range(stages):
        pack_finish(turn)
        if turn + 1 < stages:
            pack_start(turn + 1)
        else:
            homeward()
    pack_home(even, dps - 2, {"dp": even}).wait_recv()

    @pl.when(core == 0)
    def _():
        pack_out[...] = mine_s[even].astype(F32) + theirs_s[dps - 2].astype(F32)
        pack_home(even + 1, dps - 1, {"dp": even + 1}).wait_send()

    @pl.when(core == 1)
    def _():
        pack_home(even, dps - 1, {"dp": even}).wait_recv()
        pack_out[...] = theirs_s[dps - 1].astype(F32) + theirs_s[dps - 2].astype(F32)
        pack_home(even, dps - 2, {"dp": even, "tensor": opposite}).wait_send()
        pack_home(even + 1, dps - 2, {"tensor": opposite}).wait_send()

    load_sum.wait()
    if scatter:
        along_z(0, 3, mate).wait_recv()
        feed_out[...] = kept_s[(tps - 1) * 4 + 3].astype(F32) + level_s[3].astype(F32)

        @pl.when(gate == 1)
        def _():
            along_z(0, 4, mate).wait_recv()
            feed_out[...] += level_s[4].astype(F32)

    for chunk in range(CUTS):
        onward(level, chunk, 2, mate).wait_recv()
    total = gsum_s[...] + other_s[2].astype(F32)
    tok_out[...] = (total + jnp.where(lead, land_s[level].astype(F32), 0.0)).astype(BF)
    for index, block in enumerate(order_of):

        @pl.when((core != group) | (index != heads))
        def _():
            cross(index).wait_send()

        for chunk in range(CUTS):

            @pl.when(core != group)
            def _():
                to_core(block, chunk).wait_send()

            if index < 3:

                @pl.when(lead)
                def _():
                    onward(block, chunk, 2, mate).wait_send()

    if scatter:
        for turn in range(tps):
            for kind in range(4):
                chip(kind, turn).wait_send()
            plane_one(0, turn, 0).wait_send()
            plane_one(1, turn, 0).wait_send()
            plane_one(0, turn, 1).wait_send()
            plane_one(2, turn, 1).wait_send()
            plane_two(turn, 0).wait_send()
            plane_two(turn, 1).wait_send()
            if turn < tps - 1:
                along_z(turn, turn, mate).wait_send()
    else:
        feed_out[...] = jnp.zeros_like(feed_out)


def backward(grad_cross, packed, qkv, attended, logsum, rows_full, packs, grad_sum, scatter):
    rows, model = grad_sum.shape
    tps = rows_full.shape[0]
    dps, pack_rows, columns = packs.shape
    width = columns // 3
    count = packed.shape[2]
    middle_row = count // (2 * PAD) * PAD
    vmem = pl.BlockSpec(memory_space=pltpu.VMEM)
    hbm = pl.BlockSpec(memory_space=pl.ANY)
    dma = pltpu.SemaphoreType.DMA
    slots = 4 * tps if scatter else 1

    def buffer(*shape):
        return pltpu.VMEM(shape if scatter else (1, 16, model), BF)

    return pl.pallas_call(
        lambda *refs: backward_kernel(dps, tps, scatter, *refs),
        in_specs=[hbm, hbm, vmem, vmem, vmem, vmem, hbm, hbm],
        out_specs=[vmem] * 3,
        out_shape=[
            jax.ShapeDtypeStruct((rows, model), BF),
            jax.ShapeDtypeStruct((pack_rows, columns), F32),
            jax.ShapeDtypeStruct((count, model), F32),
        ],
        scratch_shapes=[
            pltpu.VMEM((tps, rows, width), BF),
            pltpu.VMEM((dps, model // dps, columns), BF),
            pltpu.VMEM((tps * rows, width), BF),
            pltpu.VMEM((tps * rows, width), F32),
            pltpu.VMEM((tps * rows, width), F32),
            pltpu.VMEM((tps, rows, model), BF),
            pltpu.VMEM((3, rows, model), BF),
            pltpu.VMEM(packs.shape, BF),
            pltpu.VMEM(packs.shape, BF),
            pltpu.VMEM((rows, model), F32),
            buffer(slots, count, model),
            buffer(2, count, model),
            buffer(2 * tps, middle_row, model),
            buffer(2 * tps, count - middle_row, model),
            buffer(tps, middle_row, model),
            buffer(tps, count - middle_row, model),
            buffer(tps + 1, count, model),
            dma((3,)),
            dma((tps,)),
            dma((tps,)),
            dma((tps, CUTS)),
            dma((tps, CUTS)),
            dma((tps, CUTS)),
            dma((3, CUTS)),
            dma((dps,)),
            dma((dps,)),
            dma((slots,)),
            dma((slots,)),
            dma((2,)),
            dma((2 * tps, 2)),
            dma((2 * tps, 2)),
            dma((tps, 2)),
            dma((tps, 2)),
            dma((tps - 1,)),
            dma((tps + 1,)),
        ],
        cost_estimate=pl.CostEstimate(
            flops=4 * tps * rows * model * columns, bytes_accessed=200 << 20, transcendentals=0
        ),
        compiler_params=pltpu.CompilerParams(
            vmem_limit_bytes=63 << 20, collective_id=2, has_side_effects=True
        ),
        name="backward",
    )(grad_cross, packed, qkv, attended, logsum, rows_full, packs, grad_sum)


def pack_kernel(hidden_ref, down_ref, out_ref, vec_ref, packed_ref):
    piece, wide = hidden_ref.shape
    width = out_ref.shape[0]
    chunks = min(wide // width, piece // PAD)
    part = piece // chunks
    packed_ref[:piece] = hidden_ref[...]
    packed_ref[piece : 2 * piece] = jnp.transpose(down_ref[...])
    turned = jnp.transpose(out_ref[...])
    for chunk in range(chunks):
        packed_ref[2 * piece : 2 * piece + part, chunk * width : (chunk + 1) * width] = turned[
            chunk * part : (chunk + 1) * part
        ]
    if chunks * width < wide:
        packed_ref[2 * piece : 2 * piece + part, chunks * width :] = jnp.zeros(
            (part, wide - chunks * width), BF
        )
    packed_ref[2 * piece + part :] = vec_ref[...]


def pack_weights(hidden, down, out, vec):
    piece, wide = hidden.shape
    chunks = min(wide // out.shape[0], piece // PAD)
    return pl.pallas_call(
        pack_kernel,
        out_shape=jax.ShapeDtypeStruct((2 * piece + piece // chunks + PAD, wide), BF),
        name="pack",
    )(hidden, down, out, vec)


def row_mean(values):
    return jnp.mean(values, axis=1, keepdims=True)


def column_sum(values):
    return jnp.sum(values, axis=0, keepdims=True)


def middle_kernel(
    sizes,
    att_ref,
    tok_ref,
    cot_ref,
    all_ref,
    feed_ref,
    out_ref,
    gsum_ref,
    gatt_ref,
    pack_ref,
    first_s,
    norm_s,
    down_s,
    inv_s,
    low_s,
    low_t,
    gdown_s,
    gdown_t,
    hidden_s,
    slope_s,
    stage_s,
    tail_s,
    extra_s,
    wout_s,
    vec_s,
    sems,
    extra_sem,
):
    dps, tps, piece, chunks = sizes
    step = pl.program_id(0)
    model = tok_ref.shape[1]
    feed_rows = 2 * piece
    part = piece // chunks
    width = att_ref.shape[2]

    def norm_parts(values):
        centered = values - row_mean(values)
        inverse = lax.rsqrt(row_mean(centered * centered) + 1e-05)
        return centered * inverse, inverse

    def norm_back(grad, scale, normed, inverse):
        scaled = grad * scale
        return inverse * (scaled - row_mean(scaled) - normed * row_mean(scaled * normed))

    def send(slot, block):
        return pltpu.make_async_copy(
            stage_s.at[slot], pack_ref.at[:, block, pl.ds(0, feed_rows)], sems.at[slot]
        )

    @pl.when(step == 0)
    def _():
        def fetch(t):
            return pltpu.make_async_copy(
                all_ref.at[:, t, pl.ds(feed_rows, part + PAD)], extra_s.at[t % 2], extra_sem.at[t % 2]
            )

        fetch(0).start()
        for t in range(tps):
            if t + 1 < tps:
                fetch(t + 1).start()
            fetch(t).wait()
            extra = extra_s.at[t % 2]
            placed = jnp.sum(extra[:, part:].astype(F32), axis=0)
            if t == 0:
                vec_s[0:8] = placed[0:8]
            vec_s[8 + t : 9 + t] = placed[6:7]
            turned = jnp.concatenate(
                [extra[:, :part, c * width : (c + 1) * width] for c in range(chunks)], axis=1
            )
            wout_s[t] = turned.reshape(model, width)
        branch = None
        for t in range(tps):
            term = contract(att_ref[t], wout_s[t], 1, 1)
            branch = term if branch is None else branch + term
        normed, inverse = norm_parts(tok_ref[...].astype(F32) + branch + vec_s[0:1])
        first = normed * vec_s[1:2] + vec_s[2:3]
        norm_s[...] = normed
        inv_s[...] = jnp.broadcast_to(inverse, inv_s.shape)
        first_s[...] = first
        low = first.astype(BF)
        low_s[...] = low
        low_t[...] = jnp.transpose(low)
        down_s[...] = jnp.zeros_like(down_s)

    @pl.when(step < tps)
    def _():
        weight = feed_ref[:, 0, :piece].reshape(model, -1)
        pre = contract(low_s[...], weight, 1, 0) + vec_s[pl.ds(8 + step, 1)]
        share = 0.5 + 0.5 * lax.erf(pre * 0.7071067811865476)
        hidden = (pre * share).astype(BF)
        hidden_s[step] = hidden
        slope_s[step] = (share + pre * (0.3989422804014327 * jnp.exp(-0.5 * pre * pre))).astype(BF)
        down_s[...] += contract(hidden, feed_ref[:, 0, piece:].reshape(model, -1), 1, 1)

    @pl.when(step == tps)
    def _():
        normed, inverse = norm_parts(first_s[...] + down_s[...] + vec_s[3:4])
        out_ref[...] = (normed * vec_s[4:5] + vec_s[5:6]).astype(BF)
        grad = cot_ref[...].astype(F32)
        tail_s[0:1] = column_sum(grad * normed)
        tail_s[1:2] = column_sum(grad)
        grad_mid = norm_back(grad, vec_s[4:5], normed, inverse)
        gsum_ref[...] = grad_mid
        tail_s[2:3] = column_sum(grad_mid)
        grad_down = grad_mid.astype(BF)
        gdown_s[...] = grad_down
        gdown_t[...] = jnp.transpose(grad_down)
        down_s[...] = jnp.zeros_like(down_s)

    @pl.when(step >= tps)
    def _():
        block = 2 * tps - 1 - step
        slot = lax.rem(step, 2)

        @pl.when(step >= tps + 2)
        def _():
            send(slot, block + 2).wait()

        grad_hidden = contract(gdown_s[...], feed_ref[:, 0, piece:].reshape(model, -1), 1, 0)
        grad_pre = grad_hidden * slope_s[block].astype(F32)
        grad_low = grad_pre.astype(BF)
        tail_s[pl.ds(8 + block, 1)] = column_sum(grad_low.astype(F32))
        down_s[...] += contract(grad_low, feed_ref[:, 0, :piece].reshape(model, -1), 1, 1)
        stage_s[slot, :, :piece] = (
            contract(low_t[...], grad_low, 1, 0).astype(BF).reshape(dps, piece, -1)
        )
        stage_s[slot, :, piece:] = (
            contract(gdown_t[...], hidden_s[block], 1, 0).astype(BF).reshape(dps, piece, -1)
        )
        send(slot, block).start()

    @pl.when(step == 2 * tps - 1)
    def _():
        grad = gsum_ref[...] + down_s[...]
        normed = norm_s[...]
        grad_scale, grad_shift = column_sum(grad * normed), column_sum(grad)
        grad_sum = norm_back(grad, vec_s[1:2], normed, inv_s[:, 0:1])
        gsum_ref[...] = grad_sum
        grad_bias = column_sum(grad_sum)
        low = grad_sum.astype(BF)
        low_t[...] = jnp.transpose(low)
        for t in range(tps):
            gatt_ref[t] = contract(low, wout_s[t], 1, 0).astype(BF)
        send(lax.rem(step + 1, 2), 1).wait()
        send(lax.rem(step, 2), 0).wait()
        six = jnp.concatenate(
            [grad_bias, grad_scale, grad_shift, tail_s[2:3], tail_s[0:1], tail_s[1:2]], axis=0
        )
        for t in range(tps):
            gout = contract(low_t[...], att_ref[t], 1, 0).reshape(dps, piece, width)
            wide = [gout[:, c * part : (c + 1) * part] for c in range(chunks)]
            if chunks * width < model:
                wide.append(jnp.zeros((dps, part, model - chunks * width), F32))
            stage_s[0, :, :part] = jnp.concatenate(wide, axis=2).astype(BF)
            rows = jnp.concatenate(
                [six, tail_s[8 + t : 9 + t], jnp.zeros((PAD - 7, model), F32)], axis=0
            ).astype(BF)
            stage_s[0, :, part : part + PAD] = jnp.broadcast_to(rows[None], (dps, PAD, model))
            copy = pltpu.make_async_copy(
                stage_s.at[0, :, pl.ds(0, part + PAD)],
                pack_ref.at[:, t, pl.ds(feed_rows, part + PAD)],
                sems.at[0],
            )
            copy.start()
            copy.wait()


def middle(att, tokens, cotangent, gathered):
    tps, rows, width = att.shape
    model = tokens.shape[1]
    dps, wide = gathered.shape[0], gathered.shape[3]
    piece = model // dps
    chunks = min(model // width, piece // PAD)
    pack_rows = 2 * piece + piece // chunks + PAD

    def fixed(array):
        rank = len(array.shape)
        return pl.BlockSpec(
            array.shape, lambda i: (0,) * rank, pipeline_mode=pl.Buffered(buffer_count=1)
        )

    def feed_at(i):
        return (0, jnp.minimum(i, 2 * tps - 1 - i), 0, 0)

    outs = [
        jax.ShapeDtypeStruct((rows, model), BF),
        jax.ShapeDtypeStruct((rows, model), F32),
        jax.ShapeDtypeStruct(att.shape, BF),
        jax.ShapeDtypeStruct((dps, tps, pack_rows, model), BF),
    ]
    return pl.pallas_call(
        lambda *refs: middle_kernel((dps, tps, piece, chunks), *refs),
        grid=(2 * tps,),
        in_specs=[fixed(a) for a in (att, tokens, cotangent)]
        + [
            pl.BlockSpec(memory_space=pl.ANY),
            pl.BlockSpec((dps, 1, 2 * piece, wide), feed_at),
        ],
        out_specs=[fixed(a) for a in outs[:3]] + [pl.BlockSpec(memory_space=pl.ANY)],
        out_shape=outs,
        scratch_shapes=[
            pltpu.VMEM((rows, model), F32),
            pltpu.VMEM((rows, model), F32),
            pltpu.VMEM((rows, model), F32),
            pltpu.VMEM((rows, 128), F32),
            pltpu.VMEM((rows, model), BF),
            pltpu.VMEM((model, rows), BF),
            pltpu.VMEM((rows, model), BF),
            pltpu.VMEM((model, rows), BF),
            pltpu.VMEM((tps, rows, wide), BF),
            pltpu.VMEM((tps, rows, wide), BF),
            pltpu.VMEM((2, dps, 2 * piece, model), BF),
            pltpu.VMEM((16, model), F32),
            pltpu.VMEM((2, dps, piece // chunks + PAD, wide), BF),
            pltpu.VMEM((tps, model, width), BF),
            pltpu.VMEM((16, model), F32),
            pltpu.SemaphoreType.DMA((2,)),
            pltpu.SemaphoreType.DMA((2,)),
        ],
        cost_estimate=pl.CostEstimate(
            flops=6 * rows * model * model * (2 * tps + 1),
            bytes_accessed=60 << 20,
            transcendentals=0,
        ),
        compiler_params=pltpu.CompilerParams(vmem_limit_bytes=62 << 20),
        name="middle",
    )(att, tokens, cotangent, gathered, gathered)


def on_device(
    tokens,
    weight_query,
    weight_key,
    weight_value,
    weight_out,
    bias_query,
    bias_value,
    bias_out,
    first_scale,
    first_shift,
    weight_hidden,
    bias_hidden,
    weight_down,
    bias_down,
    second_scale,
    second_shift,
    cotangent,
):
    dps, tps = lax.axis_size("dp"), lax.axis_size("tensor")
    rows, model = tokens.shape
    piece = weight_hidden.shape[0]
    width = weight_query.shape[1]
    small = bias_query.shape[0]

    place = lax.axis_index("dp")

    def placed(pieces, length):
        zeros = jnp.zeros((pieces.shape[0], length), BF)
        return lax.dynamic_update_slice_in_dim(zeros, pieces, place * pieces.shape[1], 1)

    vec_rows = placed(
        jnp.stack(
            [bias_out, first_scale, first_shift, bias_down, second_scale, second_shift, bias_hidden]
        ),
        model,
    )
    packed_weights = pack_weights(
        weight_hidden, weight_down, weight_out, jnp.pad(vec_rows, ((0, PAD - 7), (0, 0)))
    )
    bias_rows = placed(jnp.stack([bias_query, bias_value]), width)
    bias_row = jnp.concatenate([bias_rows[0:1], jnp.zeros((1, width), BF), bias_rows[1:2]], axis=1)
    attn_pack = jnp.concatenate(
        [
            jnp.concatenate([weight_query, weight_key, weight_value], axis=1),
            jnp.pad(bias_row, ((0, PAD - 1), (0, 0))),
        ],
        axis=0,
    )
    rows_full, packs, qkv, attended, logsum, crossed, gathered = forward(
        tokens, attn_pack, packed_weights, dps, tps
    )
    output, grad_sum, grad_cross, packed = middle(crossed, tokens, cotangent, gathered)
    scatter = dps == 8 and tps == 4 and width == 2 * PAIR
    grad_tokens, attn_grads, summed = backward(
        grad_cross, packed, qkv, attended, logsum, rows_full, packs, grad_sum, scatter
    )
    if scatter:
        packed = summed
    else:
        packed = lax.psum_scatter(packed, "dp", scatter_dimension=0, tiled=False)
        packed = lax.psum_scatter(packed, "tensor", scatter_dimension=0, tiled=False).astype(F32)

    def share(values, count):
        return lax.dynamic_slice_in_dim(values, place * count, count, 0)

    chunks = min(model // width, piece // PAD)
    part = piece // chunks
    out_grad = packed[2 * piece : 2 * piece + part, : chunks * width]
    out_grad = out_grad.reshape(part, chunks, width).transpose(2, 1, 0).reshape(width, piece)
    vec_grads = [share(packed[2 * piece + part + i], piece) for i in range(6)]
    hidden_grad = share(packed[2 * piece + part + 6], bias_hidden.shape[0])
    return (
        output,
        grad_tokens,
        attn_grads[:piece, :width],
        attn_grads[:piece, width : 2 * width],
        attn_grads[:piece, 2 * width :],
        out_grad,
        share(attn_grads[piece, :width], small),
        share(attn_grads[piece, 2 * width :], small),
        vec_grads[0],
        vec_grads[1],
        vec_grads[2],
        packed[:piece],
        hidden_grad,
        packed[piece : 2 * piece].T,
        vec_grads[3],
        vec_grads[4],
        vec_grads[5],
    )


def solution(mesh):
    placed = (
        P(("dp", "tensor"), None),
        P("dp", "tensor"),
        P("dp", "tensor"),
        P("dp", "tensor"),
        P("tensor", "dp"),
        P(("tensor", "dp")),
        P(("tensor", "dp")),
        P("dp"),
        P("dp"),
        P("dp"),
        P("dp", "tensor"),
        P(("tensor", "dp")),
        P("tensor", "dp"),
        P("dp"),
        P("dp"),
        P("dp"),
        P(("dp", "tensor"), None),
    )
    return jax.shard_map(
        on_device,
        mesh=mesh,
        in_specs=placed,
        out_specs=(
            P(("dp", "tensor"), None),
            P(("dp", "tensor"), None),
            P("dp", "tensor"),
            P("dp", "tensor"),
            P("dp", "tensor"),
            P("tensor", "dp"),
            P(("tensor", "dp")),
            P(("tensor", "dp")),
            P("dp"),
            P("dp"),
            P("dp"),
            P("dp", "tensor"),
            P(("tensor", "dp")),
            P("tensor", "dp"),
            P("dp"),
            P("dp"),
            P("dp"),
        ),
        check_vma=False,
    )
```

```python
import jax
import jax.numpy as jnp
from jax import lax
from jax.experimental import pallas as pl
from jax.experimental.pallas import tpu as pltpu
from jax.sharding import PartitionSpec as P

HD = 64
PAIR = 2 * HD
PAD = 16
F32 = jnp.float32
BF = jnp.bfloat16


def contract(left, right, left_dim, right_dim):
    return lax.dot_general(
        left, right, (((left_dim,), (right_dim,)), ((), ())), preferred_element_type=F32
    )


def one_head(pair, head):
    lane = lax.broadcasted_iota(jnp.int32, pair.shape, 1)
    keep = lane < HD if head == 0 else lane >= HD
    return jnp.where(keep, pair, jnp.zeros_like(pair))


CUTS = 4


def flipped(index, bit):
    size = 1 << bit
    return index + size - 2 * size * lax.rem(index // size, 2)


def greet(dps, tps):
    place, level = lax.axis_index("dp"), lax.axis_index("tensor")
    barrier = pltpu.get_barrier_semaphore()
    bits = range(1, dps.bit_length() - 1)
    for bit in bits:
        pl.semaphore_signal(barrier, inc=1, device_id={"dp": flipped(place, bit)})
    pl.semaphore_signal(barrier, inc=1, device_id={"dp": flipped(place, 0)})
    for step in range(1, tps):
        other = lax.rem(level + step, tps)
        pl.semaphore_signal(barrier, inc=1, device_id={"tensor": other})
        pl.semaphore_signal(barrier, inc=1, device_id={"dp": flipped(place, 0), "tensor": other})
    pl.semaphore_wait(barrier, len(bits) + 2 * tps - 1)


def seat(place, level):
    core = lax.rem(place, 2)
    group = level // 2
    gate = lax.rem((level + 1) // 2, 2)
    mate = level + 1 - 2 * lax.rem(level, 2)
    near, far = 2 - group, 3 - 3 * group
    heads = lax.rem(level + 2 * core, 4)
    return core, group, gate, mate, near, far, heads


def ordered(level, step):
    group = level // 2
    gate = lax.rem((level + 1) // 2, 2)
    turned = step + gate * (step // 2) * (5 - 2 * step)
    return (1 - group) * (3 - turned) + group * turned


def forward_kernel(
    dps,
    tps,
    tok_ref,
    pack_ref,
    mine_ref,
    rows_ref,
    packs_ref,
    qkv_ref,
    att_ref,
    lse_ref,
    cross_ref,
    gath_ref,
    weight_s,
    away_sem,
    mate_sem,
    core_sem,
    land_sem,
    pack_send,
    pack_land,
    local_sem,
    level_send,
    near_send,
    level_land,
    plane_send,
    plane_land,
    cross_send,
    cross_land,
):
    place, level = lax.axis_index("dp"), lax.axis_index("tensor")
    rows, model = tok_ref.shape
    piece = model // dps
    width = pack_ref.shape[1] // 3
    pairs = width // PAIR
    cut = rows // CUTS
    count = mine_ref.shape[0]
    middle_row = count // (2 * PAD) * PAD
    spans = (pl.ds(0, middle_row), pl.ds(middle_row, count - middle_row))
    bits = tuple(range(1, dps.bit_length() - 1))
    orders = (bits, bits[::-1])
    core, group, gate, mate, near, far, heads = seat(place, level)
    lead = core == group
    partner = flipped(place, 0)
    own = pltpu.make_async_copy(tok_ref, rows_ref.at[level], local_sem.at[0])
    own_pack = pltpu.make_async_copy(pack_ref, packs_ref.at[place], local_sem.at[1])
    own_block = pltpu.make_async_copy(mine_ref, gath_ref.at[place, level], local_sem.at[2])
    own_block.start()

    @pl.when(lead)
    def _():
        own.start()

    @pl.when(core == 0)
    def _():
        own_pack.start()

    greet(dps, tps)

    def away(chunk):
        span = pl.ds(chunk * cut, cut)
        return pltpu.make_async_remote_copy(
            src_ref=tok_ref.at[span],
            dst_ref=rows_ref.at[level, span],
            send_sem=away_sem.at[chunk],
            recv_sem=land_sem.at[level, chunk],
            device_id={"tensor": near},
        )

    def to_mate(block, chunk, first=False):
        span = pl.ds(chunk * cut, cut)
        return pltpu.make_async_remote_copy(
            src_ref=tok_ref.at[span] if first else rows_ref.at[block, span],
            dst_ref=rows_ref.at[block, span],
            send_sem=mate_sem.at[block, chunk],
            recv_sem=land_sem.at[block, chunk],
            device_id={"tensor": mate},
        )

    def to_core(block, chunk, first=False):
        span = pl.ds(chunk * cut, cut)
        return pltpu.make_async_remote_copy(
            src_ref=tok_ref.at[span] if first else rows_ref.at[block, span],
            dst_ref=rows_ref.at[block, span],
            send_sem=core_sem.at[block, chunk],
            recv_sem=land_sem.at[block, chunk],
            device_id={"dp": partner},
        )

    line = (level, mate, near, far)

    def level_hop(at, half, inward, mine=False):
        return pltpu.make_async_remote_copy(
            src_ref=mine_ref.at[spans[half]] if mine else gath_ref.at[place, at, spans[half]],
            dst_ref=gath_ref.at[place, at, spans[half]],
            send_sem=(near_send if inward else level_send).at[at, half],
            recv_sem=level_land.at[at, half],
            device_id={"tensor": near if inward else mate},
        )

    def in_plane(block, step, half, bit, number, mine=False):
        at = line[step]
        return pltpu.make_async_remote_copy(
            src_ref=mine_ref.at[spans[half]] if mine else gath_ref.at[block, at, spans[half]],
            dst_ref=gath_ref.at[block, at, spans[half]],
            send_sem=plane_send.at[number, step, half],
            recv_sem=plane_land.at[block, step, half],
            device_id={"dp": flipped(place, bit)},
        )

    def held(half, stage):
        blocks = [place]
        for bit in orders[half][:stage]:
            blocks = blocks + [flipped(block, bit) for block in blocks]
        return blocks

    def numbered(half):
        found, at = [], 0
        for stage in range(len(bits) + 1):
            for block in held(half, stage)[(1 << stage) // 2 if stage else 0 :]:
                targets = list(orders[half][stage:]) + [0]
                found.append((stage, block, [(bit, at + i) for i, bit in enumerate(targets)]))
                at += len(targets)
        return found

    tables = (numbered(0), numbered(1))

    def pass_on(step, stage):
        for half in range(2):
            for came, block, targets in tables[half]:
                if came != stage:
                    continue
                if stage:
                    in_plane(block, step, half, 0, 0).wait_recv()
                for bit, number in targets:
                    in_plane(block, step, half, bit, number, step == 0 and stage == 0).start()

    def level_in(step):
        for half in range(2):
            level_hop(line[step], half, False).wait_recv()

            @pl.when(gate == 1)
            def _():
                level_hop(line[step], half, step == 1).start()

    even = place - core
    opposite = lax.rem(level + 2, tps)

    def pack_to(index, block, device):
        return pltpu.make_async_remote_copy(
            src_ref=pack_ref,
            dst_ref=packs_ref.at[block],
            send_sem=pack_send.at[index],
            recv_sem=pack_land.at[block],
            device_id=device,
        )

    pack_to(0, place, {"dp": even + 1, "tensor": opposite}).start()
    for half in range(2):
        level_hop(level, half, False, True).start()

        @pl.when(gate == 1)
        def _():
            level_hop(level, half, True, True).start()

    for chunk in range(CUTS):

        @pl.when(lead)
        def _():
            to_mate(level, chunk, True).start()
            to_core(level, chunk, True).start()

        @pl.when(core != group)
        def _():
            away(chunk).start()

    pass_on(0, 0)

    @pl.when(core == 1)
    def _():
        pack_to(1, place, {"dp": even}).start()
        pack_to(0, even, {"dp": even}).wait_recv()

    @pl.when(core == 0)
    def _():
        own_pack.wait()

    pack_to(0, even + 1, {"dp": even}).wait_recv()

    def pack_on(block, index, bit):
        return pltpu.make_async_remote_copy(
            src_ref=packs_ref.at[block],
            dst_ref=packs_ref.at[block],
            send_sem=pack_send.at[index],
            recv_sem=pack_land.at[block],
            device_id={"dp": flipped(place, bit)},
        )

    known = [even, even + 1]
    sent = 2
    pack_sends = []
    for bit in bits:
        for block in known:
            pack_on(block, sent, bit).start()
            pack_sends.append((block, sent, bit))
            sent += 1
        more = [flipped(block, bit) for block in known]
        for block in more:
            pack_on(block, 0, bit).wait_recv()
        known = known + more
    weight_s[...] = packs_ref[:, :piece].reshape(weight_s.shape)
    bias = jnp.sum(packs_ref[:, piece : piece + PAD].astype(F32), axis=0)[0:1]

    def project(block):
        qkv_ref[block] = (contract(rows_ref[block], weight_s[...], 1, 0) + bias).astype(BF)

    def advance(step, stage):
        if step and stage == 0:
            level_in(step)
        pass_on(step, stage)

    @pl.when(lead)
    def _():
        own.wait()

    def arrive(index, carry):
        block = ordered(level, tps - 1 - index)
        for chunk in range(CUTS):

            @pl.when((index > 0) | (core != group))
            def _():
                to_core(block, chunk).wait_recv()

            @pl.when(lead & (gate == 1) & (index > 1))
            def _():
                to_mate(block, chunk).start()

            @pl.when(lead & (index > 0))
            def _():
                to_core(block, chunk).start()

        project(block)
        for at, batch in enumerate((((0, 1),), ((1, 0),), ((0, 2), (2, 0)), ((1, 1),))):

            @pl.when(index == at)
            def _():
                for step, stage in batch:
                    advance(step, stage)

        return carry

    lax.fori_loop(0, tps, arrive, 0)
    for stage in range(3, len(bits) + 1):
        pass_on(0, stage)

    half_rows = rows // 2

    def cross(target, half):
        span = pl.ds(half * half_rows, half_rows)
        return pltpu.make_async_remote_copy(
            src_ref=att_ref.at[target, span],
            dst_ref=cross_ref.at[heads, span],
            send_sem=cross_send.at[target, half],
            recv_sem=cross_land.at[heads, half],
            device_id={"dp": even + group, "tensor": target},
        )

    turns = 2 * pairs * tps

    def attend(turn, carry):
        pair = lax.rem(turn, pairs)
        half = lax.rem(turn // pairs, 2)
        target = ordered(level, turn // (2 * pairs))
        span = pl.ds(pl.multiple_of(half * half_rows, half_rows), half_rows)
        lanes = pl.ds(pl.multiple_of(pair * PAIR, PAIR), PAIR)
        query = qkv_ref[target, span, lanes] * jnp.asarray(0.125, BF)
        key = qkv_ref[:, :, pl.ds(pl.multiple_of(width + pair * PAIR, PAIR), PAIR)]
        value = qkv_ref[:, :, pl.ds(pl.multiple_of(2 * width + pair * PAIR, PAIR), PAIR)]
        key, value = key.reshape(tps * rows, PAIR), value.reshape(tps * rows, PAIR)
        total, columns = None, []
        for head in range(2):
            scores = contract(query, one_head(key, head), 1, 1)
            highest = jnp.max(scores, axis=1, keepdims=True)
            expons = jnp.exp(scores - highest)
            mass = jnp.sum(expons, axis=1, keepdims=True)
            part = contract(expons.astype(BF), one_head(value, head), 1, 0) / mass
            total = part if total is None else total + part
            columns.append(jnp.broadcast_to(highest + jnp.log(mass), (half_rows, PAIR)))
        att_ref[target, span, lanes] = total.astype(BF)
        where = pl.ds(pl.multiple_of(target * rows + half * half_rows, half_rows), half_rows)
        lse_ref[pair, :, where] = jnp.concatenate(
            [jnp.transpose(column)[:4] for column in columns], axis=0
        )

        @pl.when((pair == pairs - 1) & ((turn < 2 * pairs * (tps - 1)) | (core != group)))
        def _():
            cross(target, half).start()

        for at, batch in events.items():

            @pl.when(turn == at)
            def _():
                for step, stage in batch:
                    advance(step, stage)

        return carry

    events = {1: [(2, 1)], turns // 4: [(1, 2), (3, 0)], turns // 2: [(2, 2)], turns - 4: [(3, 1)], turns - 1: [(3, 2)]}
    early = [item for batch in events.values() for item in batch]
    early = early + [item for batch in (((0, 1),), ((1, 0),), ((0, 2), (2, 0)), ((1, 1),)) for item in batch]
    late = [
        (step, stage)
        for step in range(1, tps)
        for stage in range(len(bits) + 1)
        if (step, stage) not in early
    ]
    lax.fori_loop(0, turns, attend, 0)
    own_cross = pltpu.make_async_copy(att_ref.at[level], cross_ref.at[heads], local_sem.at[3])

    @pl.when(lead)
    def _():
        own_cross.start()

    for step, stage in sorted(late, key=lambda item: (item[0] + item[1], item[0])):
        advance(step, stage)
    for index in range(tps):
        for half in range(2):

            @pl.when((core != group) | (index != heads))
            def _():
                pltpu.make_async_remote_copy(
                    src_ref=att_ref.at[level, pl.ds(half * half_rows, half_rows)],
                    dst_ref=cross_ref.at[index, pl.ds(half * half_rows, half_rows)],
                    send_sem=cross_send.at[index, half],
                    recv_sem=cross_land.at[index, half],
                    device_id={"tensor": mate},
                ).wait_recv()

            @pl.when((core != group) | (index != level))
            def _():
                cross(index, half).wait_send()

    for step in range(tps):
        for half in range(2):
            for stage, block, targets in tables[half]:
                in_plane(flipped(block, 0), step, half, 0, 0).wait_recv()
                for bit, number in targets:
                    in_plane(block, step, half, bit, number).wait_send()
    for half in range(2):
        level_hop(level, half, False).wait_send()

        @pl.when(gate == 1)
        def _():
            level_hop(level, half, True).wait_send()
            level_hop(mate, half, True).wait_send()
            level_hop(near, half, False).wait_send()
            level_hop(far, half, False).wait_send()

    own_block.wait()
    pack_to(0, place, {"dp": even + 1, "tensor": opposite}).wait_send()

    @pl.when(core == 1)
    def _():
        pack_to(1, place, {"dp": even}).wait_send()

    for block, index, bit in pack_sends:
        pack_on(block, index, bit).wait_send()

    @pl.when(lead)
    def _():
        own_cross.wait()

    for chunk in range(CUTS):

        @pl.when(core != group)
        def _():
            away(chunk).wait_send()

        for index, block in enumerate((level, mate, near, far)):

            @pl.when(lead)
            def _():
                to_core(block, chunk).wait_send()

            if index == 0:

                @pl.when(lead)
                def _():
                    to_mate(block, chunk).wait_send()

            if index > 1:

                @pl.when(lead & (gate == 1))
                def _():
                    to_mate(block, chunk).wait_send()


def forward(tokens, pack, mine, dps, tps):
    rows, model = tokens.shape
    columns = pack.shape[1]
    width = columns // 3
    vmem = pl.BlockSpec(memory_space=pltpu.VMEM)
    hbm = pl.BlockSpec(memory_space=pl.ANY)
    dma = pltpu.SemaphoreType.DMA
    return pl.pallas_call(
        lambda *refs: forward_kernel(dps, tps, *refs),
        in_specs=[vmem, vmem, hbm],
        out_specs=[vmem] * 5 + [hbm] * 2,
        out_shape=[
            jax.ShapeDtypeStruct((tps, rows, model), BF),
            jax.ShapeDtypeStruct((dps,) + pack.shape, BF),
            jax.ShapeDtypeStruct((tps, rows, columns), BF),
            jax.ShapeDtypeStruct((tps, rows, width), BF),
            jax.ShapeDtypeStruct((width // PAIR, 8, tps * rows), F32),
            jax.ShapeDtypeStruct((tps, rows, width), BF),
            jax.ShapeDtypeStruct((dps, tps) + mine.shape, BF),
        ],
        scratch_shapes=[
            pltpu.VMEM((model, columns), BF),
            dma((CUTS,)),
            dma((tps, CUTS)),
            dma((tps, CUTS)),
            dma((tps, CUTS)),
            dma((dps,)),
            dma((dps,)),
            dma((4,)),
            dma((tps, 2)),
            dma((tps, 2)),
            dma((tps, 2)),
            dma((dps - 1, tps, 2)),
            dma((dps, tps, 2)),
            dma((tps, 2)),
            dma((tps, 2)),
        ],
        cost_estimate=pl.CostEstimate(
            flops=2 * tps * rows * model * columns, bytes_accessed=200 << 20, transcendentals=0
        ),
        compiler_params=pltpu.CompilerParams(
            vmem_limit_bytes=50 << 20, collective_id=1, has_side_effects=True
        ),
        name="forward",
    )(tokens, pack, mine)


def backward_kernel(
    dps,
    tps,
    scatter,
    cross_ref,
    packed_ref,
    qkv_ref,
    att_ref,
    lse_ref,
    rows_ref,
    packs_ref,
    gsum_ref,
    tok_out,
    pack_out,
    feed_out,
    grad_s,
    weight_s,
    dq_s,
    dk_s,
    dv_s,
    land_s,
    other_s,
    mine_s,
    theirs_s,
    gsum_s,
    kept_s,
    stage_s,
    one_a,
    one_b,
    two_a,
    two_b,
    level_s,
    local_sem,
    grad_send,
    grad_land,
    core_send,
    core_land,
    hop_send,
    hop_land,
    pack_send,
    pack_land,
    chip_send,
    chip_land,
    stage_sem,
    one_send,
    one_land,
    two_send,
    two_land,
    level_send,
    level_land,
):
    place, level = lax.axis_index("dp"), lax.axis_index("tensor")
    rows, model = gsum_ref.shape
    piece = model // dps
    width = att_ref.shape[2]
    pairs = width // PAIR
    cut = rows // CUTS
    half_rows = rows // 2
    count = packed_ref.shape[2]
    middle_row = count // (2 * PAD) * PAD
    spans = (pl.ds(0, middle_row), pl.ds(middle_row, count - middle_row))

    load_weight = pltpu.make_async_copy(
        packs_ref.at[:, pl.ds(0, piece)], weight_s, local_sem.at[0]
    )
    load_sum = pltpu.make_async_copy(gsum_ref, gsum_s, local_sem.at[1])
    core, group, gate, mate, near, far, heads = seat(place, level)
    lead = core == group
    even = place - core
    opposite = lax.rem(level + 2, tps)
    own_grad = pltpu.make_async_copy(cross_ref.at[heads], grad_s.at[level], local_sem.at[2])
    load_weight.start()
    load_sum.start()

    @pl.when(lead)
    def _():
        own_grad.start()

    greet(dps, tps)

    def cross(index):
        other = lax.rem(index // 2 + core, 2)
        return pltpu.make_async_remote_copy(
            src_ref=cross_ref.at[index],
            dst_ref=grad_s.at[level],
            send_sem=grad_send.at[index],
            recv_sem=grad_land.at[level],
            device_id={"dp": even + other, "tensor": lax.rem(index + 2 * other, tps)},
        )

    def crossed(block):
        return pltpu.make_async_remote_copy(
            src_ref=cross_ref.at[block],
            dst_ref=grad_s.at[block],
            send_sem=grad_send.at[block],
            recv_sem=grad_land.at[block],
            device_id={"tensor": mate},
        )

    for index in range(tps):

        @pl.when((core != group) | (index != heads))
        def _():
            cross(index).start()

    def block_of(kind):
        block = place
        if kind in (0, 2):
            block = flipped(block, 1)
        if kind in (0, 1):
            block = flipped(block, 2)
        return block

    def level_of(turn):
        return ordered(level, turn)

    def chip(kind, turn):
        return pltpu.make_async_remote_copy(
            src_ref=packed_ref.at[flipped(block_of(kind), 0), level_of(turn)],
            dst_ref=kept_s.at[turn * 4 + kind],
            send_sem=chip_send.at[turn * 4 + kind],
            recv_sem=chip_land.at[turn * 4 + kind],
            device_id={"dp": flipped(place, 0)},
        )

    def load(kind, turn, slot):
        return pltpu.make_async_copy(
            packed_ref.at[block_of(kind), level_of(turn)], stage_s.at[slot], stage_sem.at[slot]
        )

    def plane_one(kind, turn, half):
        bit = 2 - half
        target = one_b if half else one_a
        at = turn * 2 + (0 if kind == 0 else 1)
        return pltpu.make_async_remote_copy(
            src_ref=kept_s.at[turn * 4 + kind, spans[half]],
            dst_ref=target.at[at],
            send_sem=one_send.at[at, half],
            recv_sem=one_land.at[at, half],
            device_id={"dp": flipped(place, bit)},
        )

    def plane_two(turn, half):
        bit = 1 + half
        target = two_b if half else two_a
        return pltpu.make_async_remote_copy(
            src_ref=kept_s.at[turn * 4 + 2 - half, spans[half]],
            dst_ref=target.at[turn],
            send_sem=two_send.at[turn, half],
            recv_sem=two_land.at[turn, half],
            device_id={"dp": flipped(place, bit)},
        )

    def along_z(turn, slot, device):
        return pltpu.make_async_remote_copy(
            src_ref=kept_s.at[turn * 4 + 3],
            dst_ref=level_s.at[slot],
            send_sem=level_send.at[turn],
            recv_sem=level_land.at[slot],
            device_id={"tensor": device},
        )

    def through_z(turn):
        @pl.when(gate == 1)
        def _():
            along_z(turn, turn, mate).wait_recv()
            at = turn * 4 + 3
            kept_s[at] = (kept_s[at].astype(F32) + level_s[turn].astype(F32)).astype(BF)
            if turn == 2:
                along_z(turn, 3, mate).start()
            else:
                along_z(turn, 2 + turn, near).start()

    def add_to(slot, half, source):
        kept_s[slot, spans[half]] = (
            kept_s[slot, spans[half]].astype(F32) + source.astype(F32)
        ).astype(BF)

    def chip_in(kind, turn):
        slot = kind % 2
        load(kind, turn, slot).wait()
        chip(kind, turn).wait_recv()
        at = turn * 4 + kind
        kept_s[at] = (kept_s[at].astype(F32) + stage_s[slot].astype(F32)).astype(BF)
        if kind in (0, 1):
            plane_one(kind, turn, 0).start()
        if kind in (0, 2):
            plane_one(kind, turn, 1).start()

    def one_in(turn):
        plane_one(0, turn, 0).wait_recv()
        add_to(turn * 4 + 2, 0, one_a[turn * 2])
        plane_two(turn, 0).start()
        plane_one(0, turn, 1).wait_recv()
        add_to(turn * 4 + 1, 1, one_b[turn * 2])
        plane_two(turn, 1).start()
        plane_one(1, turn, 0).wait_recv()
        add_to(turn * 4 + 3, 0, one_a[turn * 2 + 1])
        plane_one(2, turn, 1).wait_recv()
        add_to(turn * 4 + 3, 1, one_b[turn * 2 + 1])

    def two_in(turn):
        plane_two(turn, 0).wait_recv()
        add_to(turn * 4 + 3, 0, two_a[turn])
        plane_two(turn, 1).wait_recv()
        add_to(turn * 4 + 3, 1, two_b[turn])
        if turn < tps - 1:

            @pl.when(gate == 0)
            def _():
                along_z(turn, 4 if turn == 2 else turn, mate).start()

    if scatter:
        load(0, 0, 0).start()
        for turn in range(tps):
            for kind in range(4):
                chip(kind, turn).start()

    dk_s[...] = jnp.zeros_like(dk_s)
    dv_s[...] = jnp.zeros_like(dv_s)

    @pl.when(lead)
    def _():
        own_grad.wait()

    def attend(turn, carry):
        pair = lax.rem(turn, pairs)
        half = lax.rem(turn // pairs, 2)
        step = turn // (2 * pairs)
        target = ordered(level, tps - 1 - step)

        @pl.when((lax.rem(turn, 2 * pairs) == 0) & ((step > 0) | (core != group)))
        def _():
            crossed(target).wait_recv()

        span = pl.ds(pl.multiple_of(half * half_rows, half_rows), half_rows)
        lanes = pl.ds(pl.multiple_of(pair * PAIR, PAIR), PAIR)
        query = qkv_ref[target, span, lanes] * jnp.asarray(0.125, BF)
        key = qkv_ref[:, :, pl.ds(pl.multiple_of(width + pair * PAIR, PAIR), PAIR)]
        value = qkv_ref[:, :, pl.ds(pl.multiple_of(2 * width + pair * PAIR, PAIR), PAIR)]
        key, value = key.reshape(tps * rows, PAIR), value.reshape(tps * rows, PAIR)
        grad = grad_s[target, span, lanes]
        products = jnp.transpose(grad.astype(F32) * att_ref[target, span, lanes].astype(F32))
        where = pl.ds(pl.multiple_of(target * rows + half * half_rows, half_rows), half_rows)
        logsums = lse_ref[pair, :, where]
        grad_query = None
        for head in range(2):
            key_head, value_head = one_head(key, head), one_head(value, head)
            inner = jnp.sum(products[HD * head : HD * head + HD], axis=0, keepdims=True)
            logsum = logsums[4 * head : 4 * head + 1]
            probs = jnp.exp(contract(key_head, query, 1, 1) - logsum)
            grad_probs = contract(value_head, grad, 1, 1)
            grad_scores = (probs * (grad_probs - inner)).astype(BF)
            dv_s[:, lanes] += contract(probs.astype(BF), one_head(grad, head), 1, 0)
            dk_s[:, lanes] += contract(grad_scores, one_head(query, head), 1, 0)
            part = contract(grad_scores, key_head, 0, 0)
            grad_query = part if grad_query is None else grad_query + part
        dq_s[where, lanes] = (grad_query * 0.125).astype(BF)

        if scatter:
            for kind in range(4):

                @pl.when(lax.rem(turn, 4) == kind)
                def _():
                    if kind < 3:
                        load(kind + 1, turn // 4, (kind + 1) % 2).start()
                    else:

                        @pl.when(turn // 4 < tps - 1)
                        def _():
                            load(0, turn // 4 + 1, 0).start()

                    chip_in(kind, turn // 4)

            @pl.when(turn == 9)
            def _():
                one_in(0)

            @pl.when(turn == 13)
            def _():
                two_in(0)

            @pl.when(turn == 15)
            def _():
                one_in(1)

        return carry

    lax.fori_loop(0, 2 * pairs * tps, attend, 0)
    load_weight.wait()
    refs = (dq_s, dk_s, dv_s)

    def rows_of(block):
        span = pl.ds(pl.multiple_of(block * rows, rows), rows)
        total = None
        for index, ref in enumerate(refs):
            weight = weight_s[:, :, index * width : (index + 1) * width].reshape(model, width)
            part = contract(ref[span].astype(BF), weight, 1, 1)
            total = part if total is None else total + part
        return total

    def to_core(block, chunk):
        span = pl.ds(chunk * cut, cut)
        return pltpu.make_async_remote_copy(
            src_ref=land_s.at[block, span],
            dst_ref=land_s.at[block, span],
            send_sem=core_send.at[block, chunk],
            recv_sem=core_land.at[block, chunk],
            device_id={"dp": flipped(place, 0)},
        )

    def onward(block, chunk, slot, device):
        span = pl.ds(chunk * cut, cut)
        return pltpu.make_async_remote_copy(
            src_ref=land_s.at[block, span],
            dst_ref=other_s.at[slot, span],
            send_sem=hop_send.at[block, chunk],
            recv_sem=hop_land.at[slot, chunk],
            device_id={"tensor": device},
        )

    order_of = (far, near, mate, level)

    def part_out(index, carry):
        block = ordered(level, index)
        land_s[block] = rows_of(block).astype(BF)
        for chunk in range(CUTS):
            to_core(block, chunk).start()
        return carry

    def chip_total(block, chunk, own):
        to_core(block, chunk).wait_recv()
        span = pl.ds(chunk * cut, cut)
        return land_s[block, span].astype(F32) + own[chunk * cut : (chunk + 1) * cut]

    def part_on(index, carry):
        block = ordered(level, index)
        own = rows_of(block)
        for chunk in range(CUTS):
            land_s[block, pl.ds(chunk * cut, cut)] = chip_total(block, chunk, own).astype(BF)
            onward(block, chunk, index, mate).start()
        return carry

    def part_through(index, carry):
        block = ordered(level, index)
        own = rows_of(block)
        for chunk in range(CUTS):
            span = pl.ds(chunk * cut, cut)
            total = chip_total(block, chunk, own)
            onward(block, chunk, index, block).wait_recv()
            land_s[block, span] = (total + other_s[index, span].astype(F32)).astype(BF)
            onward(block, chunk, 2, block).start()
        return carry

    def part_own():
        own = rows_of(level)
        for chunk in range(CUTS):
            land_s[level, pl.ds(chunk * cut, cut)] = chip_total(level, chunk, own).astype(BF)

    inner = lead & (gate == 1)

    @pl.when(core != group)
    def _():
        lax.fori_loop(0, tps, part_out, 0)

    @pl.when(lead)
    def _():
        lax.fori_loop(2 * gate, 3, part_on, 0)

    tail = jnp.concatenate(
        [jnp.sum(ref[...].astype(BF).astype(F32), axis=0, keepdims=True) for ref in refs], axis=1
    )
    tokens = rows_ref.reshape(tps * rows, model)
    for index, ref in enumerate(refs):
        grad = contract(tokens[...], ref[...].astype(BF), 0, 0).astype(BF)
        mine_s[:, :piece, index * width : (index + 1) * width] = grad.reshape(dps, piece, width)
    mine_s[:, piece:] = jnp.broadcast_to(tail.astype(BF)[None], (dps, PAD, 3 * width))

    def exchange(index, bit, other):
        return pltpu.make_async_remote_copy(
            src_ref=mine_s.at[other],
            dst_ref=theirs_s.at[index],
            send_sem=pack_send.at[index],
            recv_sem=pack_land.at[index],
            device_id={"dp": flipped(place, bit)},
        )

    plane = tuple(range(1, dps.bit_length() - 1))[::-1]

    def kept(done):
        blocks = [even, even + 1]
        for bit in plane[done:][::-1]:
            blocks = blocks + [flipped(block, bit) for block in blocks]
        return blocks

    starts, at = [], 0
    for done in range(len(plane)):
        starts.append(at)
        at += dps >> (done + 1)

    def pack_start(done):
        for index, block in enumerate(kept(done + 1)):
            exchange(starts[done] + index, plane[done], flipped(block, plane[done])).start()

    def pack_finish(done):
        for index, block in enumerate(kept(done + 1)):
            exchange(starts[done] + index, plane[done], block).wait()
            mine_s[block] = (
                mine_s[block].astype(F32) + theirs_s[starts[done] + index].astype(F32)
            ).astype(BF)

    def pack_home(block, slot, device):
        return pltpu.make_async_remote_copy(
            src_ref=mine_s.at[block],
            dst_ref=theirs_s.at[slot],
            send_sem=pack_send.at[lax.rem(block, 2) + dps - 2],
            recv_sem=pack_land.at[slot],
            device_id=device,
        )

    def homeward():
        @pl.when(core == 0)
        def _():
            pack_home(even + 1, dps - 1, {"dp": even + 1}).start()

        @pl.when(core == 1)
        def _():
            pack_home(even, dps - 2, {"dp": even, "tensor": opposite}).start()
            pack_home(even + 1, dps - 2, {"tensor": opposite}).start()

    pack_start(0)
    if scatter:
        through_z(0)
        two_in(1)
        one_in(2)

    @pl.when(inner)
    def _():
        lax.fori_loop(0, 2, part_through, 0)

    @pl.when(lead)
    def _():
        part_own()

    if scatter:
        through_z(1)
        one_in(3)
        two_in(2)
        through_z(2)
        two_in(3)

    stages = len(plane)
    for turn in range(stages):
        pack_finish(turn)
        if turn + 1 < stages:
            pack_start(turn + 1)
        else:
            homeward()
    pack_home(even, dps - 2, {"dp": even}).wait_recv()

    @pl.when(core == 0)
    def _():
        pack_out[...] = mine_s[even].astype(F32) + theirs_s[dps - 2].astype(F32)
        pack_home(even + 1, dps - 1, {"dp": even + 1}).wait_send()

    @pl.when(core == 1)
    def _():
        pack_home(even, dps - 1, {"dp": even}).wait_recv()
        pack_out[...] = theirs_s[dps - 1].astype(F32) + theirs_s[dps - 2].astype(F32)
        pack_home(even, dps - 2, {"dp": even, "tensor": opposite}).wait_send()
        pack_home(even + 1, dps - 2, {"tensor": opposite}).wait_send()

    load_sum.wait()
    if scatter:
        along_z(0, 3, mate).wait_recv()
        feed_out[...] = kept_s[(tps - 1) * 4 + 3].astype(F32) + level_s[3].astype(F32)

        @pl.when(gate == 1)
        def _():
            along_z(0, 4, mate).wait_recv()
            feed_out[...] += level_s[4].astype(F32)

    for chunk in range(CUTS):
        onward(level, chunk, 2, mate).wait_recv()
    total = gsum_s[...] + other_s[2].astype(F32)
    tok_out[...] = (total + jnp.where(lead, land_s[level].astype(F32), 0.0)).astype(BF)
    for index, block in enumerate(order_of):

        @pl.when((core != group) | (index != heads))
        def _():
            cross(index).wait_send()

        for chunk in range(CUTS):

            @pl.when(core != group)
            def _():
                to_core(block, chunk).wait_send()

            if index < 3:

                @pl.when(lead)
                def _():
                    onward(block, chunk, 2, mate).wait_send()

    if scatter:
        for turn in range(tps):
            for kind in range(4):
                chip(kind, turn).wait_send()
            plane_one(0, turn, 0).wait_send()
            plane_one(1, turn, 0).wait_send()
            plane_one(0, turn, 1).wait_send()
            plane_one(2, turn, 1).wait_send()
            plane_two(turn, 0).wait_send()
            plane_two(turn, 1).wait_send()
            if turn < tps - 1:
                along_z(turn, turn, mate).wait_send()
    else:
        feed_out[...] = jnp.zeros_like(feed_out)


def backward(grad_cross, packed, qkv, attended, logsum, rows_full, packs, grad_sum, scatter):
    rows, model = grad_sum.shape
    tps = rows_full.shape[0]
    dps, pack_rows, columns = packs.shape
    width = columns // 3
    count = packed.shape[2]
    middle_row = count // (2 * PAD) * PAD
    vmem = pl.BlockSpec(memory_space=pltpu.VMEM)
    hbm = pl.BlockSpec(memory_space=pl.ANY)
    dma = pltpu.SemaphoreType.DMA
    slots = 4 * tps if scatter else 1

    def buffer(*shape):
        return pltpu.VMEM(shape if scatter else (1, 16, model), BF)

    return pl.pallas_call(
        lambda *refs: backward_kernel(dps, tps, scatter, *refs),
        in_specs=[hbm, hbm, vmem, vmem, vmem, vmem, hbm, hbm],
        out_specs=[vmem] * 3,
        out_shape=[
            jax.ShapeDtypeStruct((rows, model), BF),
            jax.ShapeDtypeStruct((pack_rows, columns), F32),
            jax.ShapeDtypeStruct((count, model), F32),
        ],
        scratch_shapes=[
            pltpu.VMEM((tps, rows, width), BF),
            pltpu.VMEM((dps, model // dps, columns), BF),
            pltpu.VMEM((tps * rows, width), BF),
            pltpu.VMEM((tps * rows, width), F32),
            pltpu.VMEM((tps * rows, width), F32),
            pltpu.VMEM((tps, rows, model), BF),
            pltpu.VMEM((3, rows, model), BF),
            pltpu.VMEM(packs.shape, BF),
            pltpu.VMEM(packs.shape, BF),
            pltpu.VMEM((rows, model), F32),
            buffer(slots, count, model),
            buffer(2, count, model),
            buffer(2 * tps, middle_row, model),
            buffer(2 * tps, count - middle_row, model),
            buffer(tps, middle_row, model),
            buffer(tps, count - middle_row, model),
            buffer(tps + 1, count, model),
            dma((3,)),
            dma((tps,)),
            dma((tps,)),
            dma((tps, CUTS)),
            dma((tps, CUTS)),
            dma((tps, CUTS)),
            dma((3, CUTS)),
            dma((dps,)),
            dma((dps,)),
            dma((slots,)),
            dma((slots,)),
            dma((2,)),
            dma((2 * tps, 2)),
            dma((2 * tps, 2)),
            dma((tps, 2)),
            dma((tps, 2)),
            dma((tps - 1,)),
            dma((tps + 1,)),
        ],
        cost_estimate=pl.CostEstimate(
            flops=4 * tps * rows * model * columns, bytes_accessed=200 << 20, transcendentals=0
        ),
        compiler_params=pltpu.CompilerParams(
            vmem_limit_bytes=63 << 20, collective_id=2, has_side_effects=True
        ),
        name="backward",
    )(grad_cross, packed, qkv, attended, logsum, rows_full, packs, grad_sum)


def pack_kernel(hidden_ref, down_ref, out_ref, vec_ref, packed_ref):
    piece, wide = hidden_ref.shape
    width = out_ref.shape[0]
    chunks = min(wide // width, piece // PAD)
    part = piece // chunks
    packed_ref[:piece] = hidden_ref[...]
    packed_ref[piece : 2 * piece] = jnp.transpose(down_ref[...])
    turned = jnp.transpose(out_ref[...])
    for chunk in range(chunks):
        packed_ref[2 * piece : 2 * piece + part, chunk * width : (chunk + 1) * width] = turned[
            chunk * part : (chunk + 1) * part
        ]
    if chunks * width < wide:
        packed_ref[2 * piece : 2 * piece + part, chunks * width :] = jnp.zeros(
            (part, wide - chunks * width), BF
        )
    packed_ref[2 * piece + part :] = vec_ref[...]


def pack_weights(hidden, down, out, vec):
    piece, wide = hidden.shape
    chunks = min(wide // out.shape[0], piece // PAD)
    return pl.pallas_call(
        pack_kernel,
        out_shape=jax.ShapeDtypeStruct((2 * piece + piece // chunks + PAD, wide), BF),
        name="pack",
    )(hidden, down, out, vec)


def row_mean(values):
    return jnp.mean(values, axis=1, keepdims=True)


def column_sum(values):
    return jnp.sum(values, axis=0, keepdims=True)


def middle_kernel(
    sizes,
    att_ref,
    tok_ref,
    cot_ref,
    all_ref,
    feed_ref,
    out_ref,
    gsum_ref,
    gatt_ref,
    pack_ref,
    first_s,
    norm_s,
    down_s,
    inv_s,
    low_s,
    low_t,
    gdown_s,
    gdown_t,
    hidden_s,
    slope_s,
    stage_s,
    tail_s,
    extra_s,
    wout_s,
    vec_s,
    sems,
    extra_sem,
):
    dps, tps, piece, chunks = sizes
    step = pl.program_id(0)
    model = tok_ref.shape[1]
    feed_rows = 2 * piece
    part = piece // chunks
    width = att_ref.shape[2]

    def norm_parts(values):
        centered = values - row_mean(values)
        inverse = lax.rsqrt(row_mean(centered * centered) + 1e-05)
        return centered * inverse, inverse

    def norm_back(grad, scale, normed, inverse):
        scaled = grad * scale
        return inverse * (scaled - row_mean(scaled) - normed * row_mean(scaled * normed))

    def send(slot, block):
        return pltpu.make_async_copy(
            stage_s.at[slot], pack_ref.at[:, block, pl.ds(0, feed_rows)], sems.at[slot]
        )

    @pl.when(step == 0)
    def _():
        def fetch(t):
            return pltpu.make_async_copy(
                all_ref.at[:, t, pl.ds(feed_rows, part + PAD)], extra_s.at[t % 2], extra_sem.at[t % 2]
            )

        fetch(0).start()
        for t in range(tps):
            if t + 1 < tps:
                fetch(t + 1).start()
            fetch(t).wait()
            extra = extra_s.at[t % 2]
            placed = jnp.sum(extra[:, part:].astype(F32), axis=0)
            if t == 0:
                vec_s[0:8] = placed[0:8]
            vec_s[8 + t : 9 + t] = placed[6:7]
            turned = jnp.concatenate(
                [extra[:, :part, c * width : (c + 1) * width] for c in range(chunks)], axis=1
            )
            wout_s[t] = turned.reshape(model, width)
        branch = None
        for t in range(tps):
            term = contract(att_ref[t], wout_s[t], 1, 1)
            branch = term if branch is None else branch + term
        normed, inverse = norm_parts(tok_ref[...].astype(F32) + branch + vec_s[0:1])
        first = normed * vec_s[1:2] + vec_s[2:3]
        norm_s[...] = normed
        inv_s[...] = jnp.broadcast_to(inverse, inv_s.shape)
        first_s[...] = first
        low = first.astype(BF)
        low_s[...] = low
        low_t[...] = jnp.transpose(low)
        down_s[...] = jnp.zeros_like(down_s)

    @pl.when(step < tps)
    def _():
        weight = feed_ref[:, 0, :piece].reshape(model, -1)
        pre = contract(low_s[...], weight, 1, 0) + vec_s[pl.ds(8 + step, 1)]
        share = 0.5 + 0.5 * lax.erf(pre * 0.7071067811865476)
        hidden = (pre * share).astype(BF)
        hidden_s[step] = hidden
        slope_s[step] = (share + pre * (0.3989422804014327 * jnp.exp(-0.5 * pre * pre))).astype(BF)
        down_s[...] += contract(hidden, feed_ref[:, 0, piece:].reshape(model, -1), 1, 1)

    @pl.when(step == tps)
    def _():
        normed, inverse = norm_parts(first_s[...] + down_s[...] + vec_s[3:4])
        out_ref[...] = (normed * vec_s[4:5] + vec_s[5:6]).astype(BF)
        grad = cot_ref[...].astype(F32)
        tail_s[0:1] = column_sum(grad * normed)
        tail_s[1:2] = column_sum(grad)
        grad_mid = norm_back(grad, vec_s[4:5], normed, inverse)
        gsum_ref[...] = grad_mid
        tail_s[2:3] = column_sum(grad_mid)
        grad_down = grad_mid.astype(BF)
        gdown_s[...] = grad_down
        gdown_t[...] = jnp.transpose(grad_down)
        down_s[...] = jnp.zeros_like(down_s)

    @pl.when(step >= tps)
    def _():
        block = 2 * tps - 1 - step
        slot = lax.rem(step, 2)

        @pl.when(step >= tps + 2)
        def _():
            send(slot, block + 2).wait()

        grad_hidden = contract(gdown_s[...], feed_ref[:, 0, piece:].reshape(model, -1), 1, 0)
        grad_pre = grad_hidden * slope_s[block].astype(F32)
        grad_low = grad_pre.astype(BF)
        tail_s[pl.ds(8 + block, 1)] = column_sum(grad_low.astype(F32))
        down_s[...] += contract(grad_low, feed_ref[:, 0, :piece].reshape(model, -1), 1, 1)
        stage_s[slot, :, :piece] = (
            contract(low_t[...], grad_low, 1, 0).astype(BF).reshape(dps, piece, -1)
        )
        stage_s[slot, :, piece:] = (
            contract(gdown_t[...], hidden_s[block], 1, 0).astype(BF).reshape(dps, piece, -1)
        )
        send(slot, block).start()

    @pl.when(step == 2 * tps - 1)
    def _():
        grad = gsum_ref[...] + down_s[...]
        normed = norm_s[...]
        grad_scale, grad_shift = column_sum(grad * normed), column_sum(grad)
        grad_sum = norm_back(grad, vec_s[1:2], normed, inv_s[:, 0:1])
        gsum_ref[...] = grad_sum
        grad_bias = column_sum(grad_sum)
        low = grad_sum.astype(BF)
        low_t[...] = jnp.transpose(low)
        for t in range(tps):
            gatt_ref[t] = contract(low, wout_s[t], 1, 0).astype(BF)
        send(lax.rem(step + 1, 2), 1).wait()
        send(lax.rem(step, 2), 0).wait()
        six = jnp.concatenate(
            [grad_bias, grad_scale, grad_shift, tail_s[2:3], tail_s[0:1], tail_s[1:2]], axis=0
        )
        for t in range(tps):
            gout = contract(low_t[...], att_ref[t], 1, 0).reshape(dps, piece, width)
            wide = [gout[:, c * part : (c + 1) * part] for c in range(chunks)]
            if chunks * width < model:
                wide.append(jnp.zeros((dps, part, model - chunks * width), F32))
            stage_s[0, :, :part] = jnp.concatenate(wide, axis=2).astype(BF)
            rows = jnp.concatenate(
                [six, tail_s[8 + t : 9 + t], jnp.zeros((PAD - 7, model), F32)], axis=0
            ).astype(BF)
            stage_s[0, :, part : part + PAD] = jnp.broadcast_to(rows[None], (dps, PAD, model))
            copy = pltpu.make_async_copy(
                stage_s.at[0, :, pl.ds(0, part + PAD)],
                pack_ref.at[:, t, pl.ds(feed_rows, part + PAD)],
                sems.at[0],
            )
            copy.start()
            copy.wait()


def middle(att, tokens, cotangent, gathered):
    tps, rows, width = att.shape
    model = tokens.shape[1]
    dps, wide = gathered.shape[0], gathered.shape[3]
    piece = model // dps
    chunks = min(model // width, piece // PAD)
    pack_rows = 2 * piece + piece // chunks + PAD

    def fixed(array):
        rank = len(array.shape)
        return pl.BlockSpec(
            array.shape, lambda i: (0,) * rank, pipeline_mode=pl.Buffered(buffer_count=1)
        )

    def feed_at(i):
        return (0, jnp.minimum(i, 2 * tps - 1 - i), 0, 0)

    outs = [
        jax.ShapeDtypeStruct((rows, model), BF),
        jax.ShapeDtypeStruct((rows, model), F32),
        jax.ShapeDtypeStruct(att.shape, BF),
        jax.ShapeDtypeStruct((dps, tps, pack_rows, model), BF),
    ]
    return pl.pallas_call(
        lambda *refs: middle_kernel((dps, tps, piece, chunks), *refs),
        grid=(2 * tps,),
        in_specs=[fixed(a) for a in (att, tokens, cotangent)]
        + [
            pl.BlockSpec(memory_space=pl.ANY),
            pl.BlockSpec((dps, 1, 2 * piece, wide), feed_at),
        ],
        out_specs=[fixed(a) for a in outs[:3]] + [pl.BlockSpec(memory_space=pl.ANY)],
        out_shape=outs,
        scratch_shapes=[
            pltpu.VMEM((rows, model), F32),
            pltpu.VMEM((rows, model), F32),
            pltpu.VMEM((rows, model), F32),
            pltpu.VMEM((rows, 128), F32),
            pltpu.VMEM((rows, model), BF),
            pltpu.VMEM((model, rows), BF),
            pltpu.VMEM((rows, model), BF),
            pltpu.VMEM((model, rows), BF),
            pltpu.VMEM((tps, rows, wide), BF),
            pltpu.VMEM((tps, rows, wide), BF),
            pltpu.VMEM((2, dps, 2 * piece, model), BF),
            pltpu.VMEM((16, model), F32),
            pltpu.VMEM((2, dps, piece // chunks + PAD, wide), BF),
            pltpu.VMEM((tps, model, width), BF),
            pltpu.VMEM((16, model), F32),
            pltpu.SemaphoreType.DMA((2,)),
            pltpu.SemaphoreType.DMA((2,)),
        ],
        cost_estimate=pl.CostEstimate(
            flops=6 * rows * model * model * (2 * tps + 1),
            bytes_accessed=60 << 20,
            transcendentals=0,
        ),
        compiler_params=pltpu.CompilerParams(vmem_limit_bytes=62 << 20),
        name="middle",
    )(att, tokens, cotangent, gathered, gathered)


def on_device(
    tokens,
    weight_query,
    weight_key,
    weight_value,
    weight_out,
    bias_query,
    bias_value,
    bias_out,
    first_scale,
    first_shift,
    weight_hidden,
    bias_hidden,
    weight_down,
    bias_down,
    second_scale,
    second_shift,
    cotangent,
):
    dps, tps = lax.axis_size("dp"), lax.axis_size("tensor")
    rows, model = tokens.shape
    piece = weight_hidden.shape[0]
    width = weight_query.shape[1]
    small = bias_query.shape[0]

    place = lax.axis_index("dp")

    def placed(pieces, length):
        zeros = jnp.zeros((pieces.shape[0], length), BF)
        return lax.dynamic_update_slice_in_dim(zeros, pieces, place * pieces.shape[1], 1)

    vec_rows = placed(
        jnp.stack(
            [bias_out, first_scale, first_shift, bias_down, second_scale, second_shift, bias_hidden]
        ),
        model,
    )
    packed_weights = pack_weights(
        weight_hidden, weight_down, weight_out, jnp.pad(vec_rows, ((0, PAD - 7), (0, 0)))
    )
    bias_rows = placed(jnp.stack([bias_query, bias_value]), width)
    bias_row = jnp.concatenate([bias_rows[0:1], jnp.zeros((1, width), BF), bias_rows[1:2]], axis=1)
    attn_pack = jnp.concatenate(
        [
            jnp.concatenate([weight_query, weight_key, weight_value], axis=1),
            jnp.pad(bias_row, ((0, PAD - 1), (0, 0))),
        ],
        axis=0,
    )
    rows_full, packs, qkv, attended, logsum, crossed, gathered = forward(
        tokens, attn_pack, packed_weights, dps, tps
    )
    output, grad_sum, grad_cross, packed = middle(crossed, tokens, cotangent, gathered)
    scatter = dps == 8 and tps == 4 and width == 2 * PAIR
    grad_tokens, attn_grads, summed = backward(
        grad_cross, packed, qkv, attended, logsum, rows_full, packs, grad_sum, scatter
    )
    if scatter:
        packed = summed
    else:
        packed = lax.psum_scatter(packed, "dp", scatter_dimension=0, tiled=False)
        packed = lax.psum_scatter(packed, "tensor", scatter_dimension=0, tiled=False).astype(F32)

    def share(values, count):
        return lax.dynamic_slice_in_dim(values, place * count, count, 0)

    chunks = min(model // width, piece // PAD)
    part = piece // chunks
    out_grad = packed[2 * piece : 2 * piece + part, : chunks * width]
    out_grad = out_grad.reshape(part, chunks, width).transpose(2, 1, 0).reshape(width, piece)
    vec_grads = [share(packed[2 * piece + part + i], piece) for i in range(6)]
    hidden_grad = share(packed[2 * piece + part + 6], bias_hidden.shape[0])
    return (
        output,
        grad_tokens,
        attn_grads[:piece, :width],
        attn_grads[:piece, width : 2 * width],
        attn_grads[:piece, 2 * width :],
        out_grad,
        share(attn_grads[piece, :width], small),
        share(attn_grads[piece, 2 * width :], small),
        vec_grads[0],
        vec_grads[1],
        vec_grads[2],
        packed[:piece],
        hidden_grad,
        packed[piece : 2 * piece].T,
        vec_grads[3],
        vec_grads[4],
        vec_grads[5],
    )


def solution(mesh):
    placed = (
        P(("dp", "tensor"), None),
        P("dp", "tensor"),
        P("dp", "tensor"),
        P("dp", "tensor"),
        P("tensor", "dp"),
        P(("tensor", "dp")),
        P(("tensor", "dp")),
        P("dp"),
        P("dp"),
        P("dp"),
        P("dp", "tensor"),
        P(("tensor", "dp")),
        P("tensor", "dp"),
        P("dp"),
        P("dp"),
        P("dp"),
        P(("dp", "tensor"), None),
    )
    return jax.shard_map(
        on_device,
        mesh=mesh,
        in_specs=placed,
        out_specs=(
            P(("dp", "tensor"), None),
            P(("dp", "tensor"), None),
            P("dp", "tensor"),
            P("dp", "tensor"),
            P("dp", "tensor"),
            P("tensor", "dp"),
            P(("tensor", "dp")),
            P(("tensor", "dp")),
            P("dp"),
            P("dp"),
            P("dp"),
            P("dp", "tensor"),
            P(("tensor", "dp")),
            P("tensor", "dp"),
            P("dp"),
            P("dp"),
            P("dp"),
        ),
        check_vma=False,
    )
```
